8 devices in a mesh: data: 1 (over z), chip: 2 (over y), dap: 4 (over x, core).
Axes of the slice: x: 2, y: 2, z: 1, core: 2. Of those that a mesh axis runs over, the one named last changes fastest.
Arguments:
- m: bfloat16 [256, 96, 256], P(('data', 'chip', 'dap'))
- z: bfloat16 [96, 96, 128], P(('data', 'chip', 'dap'))
- msa_mask: int32 [256, 96], P('data')
- res_mask: int32 [96], P('data')
- w_row_in: bfloat16 [256, 1024], replicated
- w_row_bias: bfloat16 [128, 8], replicated
- w_row_out: bfloat16 [256, 256], replicated
- w_col_in: bfloat16 [256, 1024], replicated
- w_col_out: bfloat16 [256, 256], replicated
- w_opm_in: bfloat16 [256, 64], replicated
- w_opm_out: bfloat16 [1024, 128], replicated
- w_start_in: bfloat16 [128, 512], replicated
- w_start_bias: bfloat16 [128, 4], replicated
- w_start_out: bfloat16 [128, 128], replicated
- w_end_in: bfloat16 [128, 512], replicated
- w_end_bias: bfloat16 [128, 4], replicated
- w_end_out: bfloat16 [128, 128], replicated
Outputs:
- output 1: bfloat16 [256, 96, 256], P(('data', 'chip', 'dap'))
- output 2: bfloat16 [96, 96, 128], P(('data', 'chip', 'dap'))
All inputs are finite; a program needn't handle non-finite values.
Results may differ from the reference program's by a relative error of at most 0.0151752.
Values are sent between devices in bfloat16 or wider.
A program may use at most 1 GiB of HBM per device.

```python
import jax
import jax.numpy as jnp
from jax import lax

NUM_SEQ = 256
NUM_RES = 96
C_M = 256
C_Z = 128
HEADS_M = 8
HEAD_M = 32
HEADS_T = 4
HEAD_T = 32
OPM = 32


def layer_norm(x):
    values = x.astype(jnp.float32)
    centred = values - jnp.mean(values, axis=-1, keepdims=True)
    variance = jnp.mean(centred * centred, axis=-1, keepdims=True)
    return (centred * lax.rsqrt(variance + 1e-5)).astype(jnp.bfloat16)


def project(x, weight):
    return jnp.dot(x, weight, preferred_element_type=jnp.float32).astype(jnp.bfloat16)


def add_residual(state, update):
    return (state.astype(jnp.float32) + update).astype(jnp.bfloat16)


def gated_rows(projected, head_bias, key_ok, heads, head_dim):
    length = projected.shape[0]
    split_proj = projected.reshape(length, 4, heads, head_dim).astype(jnp.float32)
    scores = jnp.einsum('ihd,jhd->hij', split_proj[:, 0], split_proj[:, 1]) * head_dim ** -0.5
    if head_bias is not None:
        scores = scores + head_bias.astype(jnp.float32)
    scores = jnp.where(key_ok[None, None, :], scores, -1e9)
    attn_prob = jax.nn.softmax(scores, axis=-1).astype(jnp.bfloat16).astype(jnp.float32)
    mixed = jnp.einsum('hij,jhd->ihd', attn_prob, split_proj[:, 2])
    gated = (mixed * jax.nn.sigmoid(split_proj[:, 3])).astype(jnp.bfloat16)
    return gated.reshape(length, heads * head_dim)


def draw_masks(mask_key):
    seq_key, res_key = jax.random.split(mask_key)
    seq_idx = jnp.arange(NUM_SEQ)[:, None]
    res_idx = jnp.arange(NUM_RES)
    msa_draw = jax.random.randint(seq_key, (NUM_SEQ, NUM_RES), 0, 4)
    msa_mask = ((msa_draw != 0) | (seq_idx == 0) | (res_idx[None, :] == 0)).astype(jnp.int32)
    res_draw = jax.random.randint(res_key, (NUM_RES,), 0, 4)
    res_mask = ((res_draw != 0) | (res_idx == 0)).astype(jnp.int32)
    return msa_mask, res_mask


def dense(weight_key, rows, cols, gain):
    draw = jax.random.normal(weight_key, (rows, cols), jnp.float32)
    return (draw * (gain * rows ** -0.5)).astype(jnp.bfloat16)


def attn_in(weight_key, rows, heads, head_dim):
    draw = jax.random.normal(weight_key, (rows, 4, heads * head_dim), jnp.float32)
    boost = jnp.array([1.5, 1.5, 1.0, 1.0], jnp.float32)[None, :, None]
    return (draw * boost * rows ** -0.5).reshape(rows, 4 * heads * head_dim).astype(jnp.bfloat16)


def setup_inputs(seed: int = 0, part: int = 0) -> dict:
    part_keys = jax.random.split(jax.random.fold_in(jax.random.key(seed), part), 4)
    weight_keys = jax.random.split(jax.random.key(seed + 1), 13)
    profile = jax.random.normal(part_keys[0], (1, NUM_RES, C_M), jnp.float32)
    noise = jax.random.normal(part_keys[1], (NUM_SEQ, NUM_RES, C_M), jnp.float32)
    pair = jax.random.normal(part_keys[2], (NUM_RES, NUM_RES, C_Z), jnp.float32)
    msa_mask, res_mask = draw_masks(part_keys[3])
    return {
        'm': (profile + noise).astype(jnp.bfloat16),
        'z': pair.astype(jnp.bfloat16),
        'msa_mask': msa_mask,
        'res_mask': res_mask,
        'w_row_in': attn_in(weight_keys[0], C_M, HEADS_M, HEAD_M),
        'w_row_bias': dense(weight_keys[1], C_Z, HEADS_M, 1.5),
        'w_row_out': dense(weight_keys[2], HEADS_M * HEAD_M, C_M, 1.0),
        'w_col_in': attn_in(weight_keys[3], C_M, HEADS_M, HEAD_M),
        'w_col_out': dense(weight_keys[4], HEADS_M * HEAD_M, C_M, 1.0),
        'w_opm_in': dense(weight_keys[5], C_M, 2 * OPM, 1.0),
        'w_opm_out': dense(weight_keys[6], OPM * OPM, C_Z, 1.0),
        'w_start_in': attn_in(weight_keys[7], C_Z, HEADS_T, HEAD_T),
        'w_start_bias': dense(weight_keys[8], C_Z, HEADS_T, 1.5),
        'w_start_out': dense(weight_keys[9], HEADS_T * HEAD_T, C_Z, 1.0),
        'w_end_in': attn_in(weight_keys[10], C_Z, HEADS_T, HEAD_T),
        'w_end_bias': dense(weight_keys[11], C_Z, HEADS_T, 1.5),
        'w_end_out': dense(weight_keys[12], HEADS_T * HEAD_T, C_Z, 1.0),
    }


def reference(m, z, msa_mask, res_mask, w_row_in, w_row_bias, w_row_out, w_col_in, w_col_out,
              w_opm_in, w_opm_out, w_start_in, w_start_bias, w_start_out, w_end_in, w_end_bias, w_end_out):
    msa_ok = msa_mask != 0
    res_ok = res_mask != 0

    row_bias = jnp.transpose(project(layer_norm(z), w_row_bias), (2, 0, 1))
    row_proj = project(layer_norm(m), w_row_in)

    def row_step(step_in):
        return gated_rows(step_in[0], row_bias, step_in[1], HEADS_M, HEAD_M)

    row_gated = lax.map(row_step, (row_proj, msa_ok))
    m = add_residual(m, jnp.dot(row_gated, w_row_out, preferred_element_type=jnp.float32))

    col_proj = jnp.swapaxes(project(layer_norm(m), w_col_in), 0, 1)

    def col_step(step_in):
        return gated_rows(step_in[0], None, step_in[1], HEADS_M, HEAD_M)

    col_gated = jnp.swapaxes(lax.map(col_step, (col_proj, msa_ok.T)), 0, 1)
    m = add_residual(m, jnp.dot(col_gated, w_col_out, preferred_element_type=jnp.float32))

    outer_proj = project(layer_norm(m), w_opm_in)
    mask_w = msa_mask.astype(jnp.bfloat16)
    left = outer_proj[:, :, :OPM] * mask_w[:, :, None]
    right = (outer_proj[:, :, OPM:] * mask_w[:, :, None]).astype(jnp.float32)
    pair_norm = jnp.dot(mask_w.T, mask_w, preferred_element_type=jnp.float32)

    def outer_step(step_in):
        outer = jnp.einsum('sa,sjc->jac', step_in[0].astype(jnp.float32), right).astype(jnp.bfloat16)
        mapped = jnp.dot(outer.reshape(NUM_RES, OPM * OPM), w_opm_out, preferred_element_type=jnp.float32)
        return mapped / (1e-3 + step_in[1][:, None])

    z = add_residual(z, lax.map(outer_step, (jnp.swapaxes(left, 0, 1), pair_norm)))

    start_norm = layer_norm(z)
    start_proj = project(start_norm, w_start_in)
    start_bias = jnp.transpose(project(start_norm, w_start_bias), (2, 0, 1))

    def start_step(row_in):
        return gated_rows(row_in, start_bias, res_ok, HEADS_T, HEAD_T)

    start_gated = lax.map(start_step, start_proj)
    z = add_residual(z, jnp.dot(start_gated, w_start_out, preferred_element_type=jnp.float32))

    end_norm = layer_norm(z)
    end_proj = jnp.swapaxes(project(end_norm, w_end_in), 0, 1)
    end_bias = jnp.transpose(project(end_norm, w_end_bias), (2, 1, 0))

    def end_step(col_in):
        return gated_rows(col_in, end_bias, res_ok, HEADS_T, HEAD_T)

    end_gated = jnp.swapaxes(lax.map(end_step, end_proj), 0, 1)
    z = add_residual(z, jnp.dot(end_gated, w_end_out, preferred_element_type=jnp.float32))
    return m, z
```

```python
import functools

import jax
import jax.numpy as jnp
from jax import lax
from jax.experimental import pallas as pl
from jax.experimental.pallas import tpu as pltpu
from jax.sharding import PartitionSpec as P

BF16 = jnp.bfloat16
F32 = jnp.float32
MESH = pl.DeviceIdType.MESH
NDEV = 8
SEQ, RES, CM, CZ = 256, 96, 256, 128
SLOC, RLOC = SEQ // NDEV, RES // NDEV
HM, HT, HD, OPM = 8, 4, 32, 32
LANES = 128
MASKED = -1e9
PADDED = -3e38
SCALE = HD ** -0.5

ROWB, MF0, MF1, MB, CG, STB, ZF, ENB, ZB = range(9)
NSTAGE = 9


def dot(a, b):
    return jnp.dot(a, b, preferred_element_type=F32)


def dot_t(a, b):
    return lax.dot_general(a, b, (((1,), (1,)), ((), ())), preferred_element_type=F32)


def iota(shape, dim):
    return lax.broadcasted_iota(jnp.int32, shape, dim)


def layer_norm(x):
    values = x.astype(F32)
    centred = values - jnp.mean(values, axis=-1, keepdims=True)
    variance = jnp.mean(centred * centred, axis=-1, keepdims=True)
    return (centred * lax.rsqrt(variance + 1e-5)).astype(BF16)


def add_residual(state, update):
    return (state.astype(F32) + update).astype(BF16)


def head_mask(head, channels):
    lane = iota((16, channels), 1)
    return jnp.where((lane >= head * HD) & (lane < (head + 1) * HD), 1.0, 0.0).astype(BF16)


def masked_head(x, head):
    rows, channels = x.shape
    return (x.reshape(rows // 16, 16, channels) * head_mask(head, channels)[None]).reshape(rows, channels)


def softmax_rows(logits):
    top = jnp.max(logits, axis=-1, keepdims=True)
    weights = jnp.exp(logits - top)
    return (weights * (1.0 / jnp.sum(weights, axis=-1, keepdims=True))).astype(BF16)


def attend_padded(q, k, v, g, bias_ref, keep, heads):
    out = None
    for pair in range(heads // 2):
        h0, h1 = 2 * pair, 2 * pair + 1
        kk = jnp.concatenate([masked_head(k, h0), masked_head(k, h1)], axis=0)
        scores = dot_t(q, kk)
        probs = []
        for u in range(2):
            logits = scores[:, u * LANES:(u + 1) * LANES] * SCALE + bias_ref[2 * pair + u]
            probs.append(softmax_rows(jnp.where(keep, logits, MASKED)))
        vv = jnp.concatenate([masked_head(v, h0), masked_head(v, h1)], axis=0)
        mixed = dot(jnp.concatenate(probs, axis=1), vv)
        out = mixed if out is None else out + mixed
    return (out * jax.nn.sigmoid(g.astype(F32))).astype(BF16)


def attend_column(q, k, v, g, keep):
    out = None
    for pair in range(HM // 2):
        probs, values = [], []
        for h in (2 * pair, 2 * pair + 1):
            logits = dot_t(q, masked_head(k, h)) * SCALE
            probs.append(softmax_rows(jnp.where(keep, logits, MASKED)))
            values.append(masked_head(v, h))
        mixed = dot(jnp.concatenate(probs, axis=1), jnp.concatenate(values, axis=0))
        out = mixed if out is None else out + mixed
    return (out * jax.nn.sigmoid(g.astype(F32))).astype(BF16)


def block_kernel(m_ref, z_ref, mask_ref, res_ref, w_row_in, w_row_bias, w_row_out, w_col_in, w_col_out,
                 w_opm_in, w_opm_out, w_start_in, w_start_bias, w_start_out, w_end_in, w_end_bias, w_end_out,
                 m_out, z_out,
                 perm, comp, hperm, keep_row, mask_t, norm, res_keep, wbt, bcol, bias,
                 rowb_recv, stb_recv, enb_recv, proj, gated, m1, msend, mcols, mback, colproj,
                 left, crecv, cbig, outer, w2, w2t, opm_in_t, ynorm, z1, zs, zr, z2, z3, zs2, zr2,
                 send_sem, recv_sem, local_sem):
    data = lax.axis_index('data')
    me = lax.axis_index('chip') * 4 + lax.axis_index('dap')

    def device(d):
        return (data, d // 4, lax.rem(d, 4))

    def peer(r):
        return lax.rem(me + r, NDEV)

    def source(r):
        return lax.rem(me + NDEV - r, NDEV)

    def start_all(stage, src_of, dst_of):
        for r in range(1, NDEV):
            d = peer(r)
            pltpu.make_async_remote_copy(src_ref=src_of(d), dst_ref=dst_of(me), send_sem=send_sem.at[stage, r],
                                         recv_sem=recv_sem.at[stage, r], device_id=device(d), device_id_type=MESH).start()

    def wait_recv(stage, src_of, dst_of):
        for r in range(1, NDEV):
            pltpu.make_async_remote_copy(src_ref=src_of(me), dst_ref=dst_of(source(r)), send_sem=send_sem.at[stage, r],
                                         recv_sem=recv_sem.at[stage, r], device_id=device(peer(r)),
                                         device_id_type=MESH).wait_recv()

    def wait_send(stage, src_of, dst_of):
        for r in range(1, NDEV):
            pltpu.make_async_remote_copy(src_ref=src_of(peer(r)), dst_ref=dst_of(me), send_sem=send_sem.at[stage, r],
                                         recv_sem=recv_sem.at[stage, r], device_id=device(peer(r)),
                                         device_id_type=MESH).wait_send()

    barrier = pltpu.get_barrier_semaphore()
    for r in range(1, NDEV):
        pl.semaphore_signal(barrier, inc=1, device_id=device(peer(r)), device_id_type=MESH)

    r0, c0 = iota((256, 256), 0), iota((256, 256), 1)
    perm[...] = jnp.where(((r0 >> 4) == (c0 & 15)) & ((r0 & 15) == (c0 >> 4)), 1.0, 0.0).astype(BF16)
    r1, c1 = iota((RES, LANES), 0), iota((RES, LANES), 1)
    comp[...] = jnp.where(((c1 & 15) < RLOC) & (r1 == (c1 >> 4) * RLOC + (c1 & 15)), 1.0, 0.0).astype(BF16)
    r2, c2 = iota((LANES, LANES), 0), iota((LANES, LANES), 1)
    hperm[...] = jnp.where(((r2 >> 4) == (c2 & 7)) & ((r2 & 15) == (c2 >> 3)), 1.0, 0.0).astype(BF16)
    bcol[...] = jnp.zeros_like(bcol)
    wbt[...] = jnp.zeros_like(wbt)
    for n, w in enumerate((w_row_bias, w_start_bias, w_end_bias)):
        wbt[n, 0:w.shape[1], :] = jnp.transpose(w[...].astype(F32))

    def send_bias(recv, which, heads, stage):
        weights = wbt[which].astype(BF16)

        @pl.loop(0, RLOC)
        def _(i):
            bcol[i, :, 0:RES] = dot_t(weights, ynorm[i])

        mine = dot(hperm[0:heads * 16, :], bcol[...].reshape(LANES, LANES).astype(BF16)).astype(BF16)
        rows = pl.ds(pl.multiple_of(me * 16, 16), 16)
        recv[:, rows, :] = mine.reshape(heads, 16, LANES)
        start_all(stage, lambda d: recv.at[:, rows, :], lambda s: recv.at[:, rows, :])

    def take_bias(recv, heads, stage):
        def rows_of(s):
            return recv.at[:, pl.ds(pl.multiple_of(s * 16, 16), 16), :]
        wait_recv(stage, rows_of, rows_of)
        lane = iota((RES, LANES), 1)
        for h in range(heads):
            bias[h] = jnp.where(lane < RES, dot(comp[...], recv[h]), PADDED)

    @pl.loop(0, RLOC)
    def _(i):
        ynorm[i] = layer_norm(z_ref[i])

    pl.semaphore_wait(barrier, NDEV - 1)
    send_bias(rowb_recv, 0, HM, ROWB)

    keep_row[...] = jnp.ones_like(keep_row)
    keep_row[:, 0:RES] = mask_ref[...]
    res_keep[...] = jnp.ones_like(res_keep)
    res_keep[0:1, 0:RES] = res_ref[...]
    eye = jnp.where(r2 == c2, 1.0, 0.0).astype(BF16)
    mask_bf = mask_ref[...].astype(F32).astype(BF16)
    mask_t[...] = jnp.zeros_like(mask_t)
    mask_t[0:RES, :] = dot_t(eye[0:RES, 0:RES], mask_bf)
    mt = mask_t[...].astype(BF16)
    norm[...] = dot_t(mt, mt)
    w_full = w_opm_out[...].reshape(OPM, OPM, CZ)
    for a in range(2):
        for c in range(2):
            blk = w_full[16 * a:16 * a + 16, 16 * c:16 * c + 16, :].reshape(256, CZ)
            w2[16 * c:16 * c + 16, 16 * a:16 * a + 16, :] = dot(perm[...], blk).astype(BF16).reshape(16, 16, CZ)
    w2t[...] = dot_t(eye, w2[...].reshape(OPM * OPM, CZ)).astype(BF16)
    opm_in_t[...] = jnp.transpose(w_opm_in[...].astype(F32)).astype(BF16)
    proj[:, RES:, :] = jnp.zeros((proj.shape[0], LANES - RES, 4 * CM), BF16)
    cbig[:, RES:, :] = jnp.zeros((OPM, LANES - RES, SEQ), BF16)
    z1[RLOC:, :, :] = jnp.zeros((16 - RLOC, RES, CZ), BF16)

    take_bias(rowb_recv, HM, ROWB)

    def m_src(half):
        return lambda d: msend.at[pl.ds(d * RLOC, RLOC), 16 * half:16 * half + 16, :]

    def m_dst(half):
        return lambda s: mcols.at[:, pl.ds(pl.multiple_of(s * SLOC + 16 * half, 16), 16), :]

    def local_copy(src, dst, n):
        return pltpu.make_async_copy(src, dst, local_sem.at[n])

    for half in range(2):
        @pl.loop(0, 4)
        def _(blk):
            s0 = half * 16 + blk * 4
            x = m_ref[pl.ds(s0, 4)].reshape(4 * RES, CM)
            proj[:, 0:RES, :] = dot(layer_norm(x), w_row_in[...]).astype(BF16).reshape(4, RES, 4 * CM)
            for u in range(4):
                keep = keep_row[pl.ds(me * SLOC + s0 + u, 1), :] != 0
                gated[u] = attend_padded(proj[u, 0:RES, 0:CM], proj[u, :, CM:2 * CM], proj[u, :, 2 * CM:3 * CM],
                                         proj[u, 0:RES, 3 * CM:4 * CM], bias, keep, HM)
            update = dot(gated[...].reshape(4 * RES, CM), w_row_out[...])
            m1[pl.ds(s0, 4)] = add_residual(x, update).reshape(4, RES, CM)

        for j in range(RES // 16):
            blk = m1[16 * half:16 * half + 16, 16 * j:16 * j + 16, :].reshape(256, CM)
            msend[16 * j:16 * j + 16, 16 * half:16 * half + 16, :] = dot(perm[...], blk).astype(BF16).reshape(16, 16, CM)
        start_all(MF0 + half, m_src(half), m_dst(half))
        local_copy(m_src(half)(me), m_dst(half)(me), half).start()

    for half in range(2):
        local_copy(m_src(half)(me), m_dst(half)(me), half).wait()
        wait_recv(MF0 + half, m_src(half), m_dst(half))

    @pl.loop(0, RLOC)
    def _(j):
        x = mcols[j]
        colproj[...] = dot(layer_norm(x), w_col_in[...]).astype(BF16)
        mask_row = mask_t[pl.ds(me * RLOC + j, 1), :]
        mixed = attend_column(colproj[:, 0:CM], colproj[:, CM:2 * CM], colproj[:, 2 * CM:3 * CM], colproj[:, 3 * CM:],
                              mask_row != 0.0)
        x = add_residual(x, dot(mixed, w_col_out[...]))
        mcols[j] = x
        start_all(MB, lambda d: mcols.at[j, pl.ds(pl.multiple_of(d * SLOC, SLOC), SLOC), :],
                  lambda s: mback.at[s * RLOC + j])
        both = dot_t(opm_in_t[...], layer_norm(x)).astype(BF16).astype(F32) * mask_row
        left[j] = both[0:OPM].astype(BF16)
        crecv[me * RLOC + j] = both[OPM:].astype(BF16)
        start_all(CG, lambda d: crecv.at[me * RLOC + j], lambda s: crecv.at[s * RLOC + j])

    mback[pl.ds(me * RLOC, RLOC)] = mcols[:, pl.ds(pl.multiple_of(me * SLOC, SLOC), SLOC), :]

    def c_rows(s):
        return crecv.at[pl.ds(s * RLOC, RLOC)]
    wait_recv(CG, c_rows, c_rows)
    for c in range(2):
        @pl.loop(0, RES // 16)
        def _(j):
            j0 = pl.multiple_of(j * 16, 16)
            blk = crecv[pl.ds(j0, 16), 16 * c:16 * c + 16, :].reshape(256, SEQ)
            cbig[16 * c:16 * c + 16, pl.ds(j0, 16), :] = dot(perm[...], blk).astype(BF16).reshape(16, 16, SEQ)

    @pl.loop(0, OPM // 2)
    def _(c):
        prod = dot_t(left[...].reshape(RLOC * OPM, SEQ), cbig[pl.ds(2 * c, 2)].reshape(256, SEQ)).astype(BF16)
        for u in range(2):
            outer[:, 2 * c + u] = prod[:, u * LANES:(u + 1) * LANES].reshape(RLOC, OPM, LANES)

    @pl.loop(0, RLOC)
    def _(i):
        update = dot(w2t[...], outer[i].reshape(OPM * OPM, LANES))
        update = update / (1e-3 + norm[pl.ds(me * RLOC + i, 1), :])
        z1[i] = add_residual(z_ref[i], jnp.transpose(update)[0:RES])

    def triangle(state, result, w_in, which, w_out, recv, stage):
        @pl.loop(0, RLOC)
        def _(i):
            ynorm[i] = layer_norm(state[i])
        send_bias(recv, which, HT, stage)
        take_bias(recv, HT, stage)
        keep = res_keep[0:1, :] != 0

        @pl.loop(0, RLOC // 4)
        def _(blk):
            i0 = blk * 4
            y = ynorm[pl.ds(i0, 4)].reshape(4 * RES, CZ)
            proj[:, 0:RES, 0:4 * CZ] = dot(y, w_in[...]).astype(BF16).reshape(4, RES, 4 * CZ)
            for u in range(4):
                gated[u, :, 0:CZ] = attend_padded(proj[u, 0:RES, 0:CZ], proj[u, :, CZ:2 * CZ], proj[u, :, 2 * CZ:3 * CZ],
                                                  proj[u, 0:RES, 3 * CZ:4 * CZ], bias, keep, HT)
            update = dot(gated[:, :, 0:CZ].reshape(4 * RES, CZ), w_out[...])
            x = state[pl.ds(i0, 4)].reshape(4 * RES, CZ)
            result[pl.ds(i0, 4)] = add_residual(x, update).reshape(4, RES, CZ)

    def z_src(buf):
        return lambda d: buf.at[pl.ds(d * RLOC, RLOC)]

    def z_dst(buf):
        return lambda s: buf.at[:, pl.ds(pl.multiple_of(s * 16, 16), 16), :]

    def exchange(state, send, recv, result, stage, n):
        for j in range(RES // 16):
            blk = state[:, 16 * j:16 * j + 16, :].reshape(256, CZ)
            send[16 * j:16 * j + 16] = dot(perm[...], blk).astype(BF16).reshape(16, 16, CZ)
        start_all(stage, z_src(send), z_dst(recv))
        own = local_copy(z_src(send)(me), z_dst(recv)(me), n)
        own.start()
        own.wait()
        wait_recv(stage, z_src(send), z_dst(recv))

        @pl.loop(0, RLOC)
        def _(i):
            result[i] = dot(comp[...], recv[i]).astype(BF16)

    triangle(z1, z1, w_start_in, 1, w_start_out, stb_recv, STB)
    exchange(z1, zs, zr, z2, ZF, 2)
    z3[RLOC:, :, :] = jnp.zeros((16 - RLOC, RES, CZ), BF16)
    triangle(z2, z3, w_end_in, 2, w_end_out, enb_recv, ENB)
    exchange(z3, zs2, zr2, z_out, ZB, 3)

    def mb_src(d):
        return mcols.at[:, pl.ds(pl.multiple_of(d * SLOC, SLOC), SLOC), :]

    def mb_dst(s):
        return mback.at[pl.ds(s * RLOC, RLOC)]
    wait_recv(MB, mb_src, mb_dst)
    for half in range(2):
        @pl.loop(0, RES // 16)
        def _(j):
            j0 = pl.multiple_of(j * 16, 16)
            blk = mback[pl.ds(j0, 16), 16 * half:16 * half + 16, :].reshape(256, CM)
            m_out[16 * half:16 * half + 16, pl.ds(j0, 16), :] = dot(perm[...], blk).astype(BF16).reshape(16, 16, CM)

    def b_rows(buf):
        return lambda s: buf.at[:, pl.ds(pl.multiple_of(me * 16, 16), 16), :]
    wait_send(ROWB, b_rows(rowb_recv), b_rows(rowb_recv))
    for half in range(2):
        wait_send(MF0 + half, m_src(half), m_dst(half))
    wait_send(MB, mb_src, mb_dst)
    wait_send(CG, lambda d: c_rows(me), c_rows)
    wait_send(STB, b_rows(stb_recv), b_rows(stb_recv))
    wait_send(ZF, z_src(zs), z_dst(zr))
    wait_send(ENB, b_rows(enb_recv), b_rows(enb_recv))
    wait_send(ZB, z_src(zs2), z_dst(zr2))


def solution(mesh):
    rows = P(('data', 'chip', 'dap'))
    in_specs = (rows, rows, P('data'), P('data')) + (P(),) * 13
    vmem = pl.BlockSpec(memory_space=pltpu.VMEM)

    def per_device(m_blk, z_blk, msa_mask, res_mask, *weights):
        scratch = [
            pltpu.VMEM((256, 256), BF16),
            pltpu.VMEM((RES, LANES), BF16),
            pltpu.VMEM((LANES, LANES), BF16),
            pltpu.VMEM((SEQ, LANES), jnp.int32),
            pltpu.VMEM((LANES, SEQ), F32),
            pltpu.VMEM((LANES, LANES), F32),
            pltpu.VMEM((8, LANES), jnp.int32),
            pltpu.VMEM((3, 8, CZ), F32),
            pltpu.VMEM((16, 8, LANES), F32),
            pltpu.VMEM((HM, RES, LANES), F32),
            pltpu.VMEM((HM, LANES, LANES), BF16),
            pltpu.VMEM((HT, LANES, LANES), BF16),
            pltpu.VMEM((HT, LANES, LANES), BF16),
            pltpu.VMEM((4, LANES, 4 * CM), BF16),
            pltpu.VMEM((4, RES, CM), BF16),
            pltpu.VMEM((SLOC, RES, CM), BF16),
            pltpu.VMEM((RES, SLOC, CM), BF16),
            pltpu.VMEM((RLOC, SEQ, CM), BF16),
            pltpu.VMEM((RES, SLOC, CM), BF16),
            pltpu.VMEM((SEQ, 4 * CM), BF16),
            pltpu.VMEM((RLOC, OPM, SEQ), BF16),
            pltpu.VMEM((RES, OPM, SEQ), BF16),
            pltpu.VMEM((OPM, LANES, SEQ), BF16),
            pltpu.VMEM((RLOC, OPM, OPM, LANES), BF16),
            pltpu.VMEM((OPM, OPM, CZ), BF16),
            pltpu.VMEM((CZ, OPM * OPM), BF16),
            pltpu.VMEM((2 * OPM, CM), BF16),
            pltpu.VMEM((RLOC, RES, CZ), BF16),
            pltpu.VMEM((16, RES, CZ), BF16),
            pltpu.VMEM((RES, 16, CZ), BF16),
            pltpu.VMEM((RLOC, LANES, CZ), BF16),
            pltpu.VMEM((RLOC, RES, CZ), BF16),
            pltpu.VMEM((16, RES, CZ), BF16),
            pltpu.VMEM((RES, 16, CZ), BF16),
            pltpu.VMEM((RLOC, LANES, CZ), BF16),
            pltpu.SemaphoreType.DMA((NSTAGE, NDEV)),
            pltpu.SemaphoreType.DMA((NSTAGE, NDEV)),
            pltpu.SemaphoreType.DMA((4,)),
        ]
        return pl.pallas_call(
            block_kernel,
            name='evoformer_block',
            out_shape=(jax.ShapeDtypeStruct(m_blk.shape, BF16), jax.ShapeDtypeStruct(z_blk.shape, BF16)),
            in_specs=[vmem] * 17,
            out_specs=(vmem, vmem),
            scratch_shapes=scratch,
            compiler_params=pltpu.CompilerParams(collective_id=0, has_side_effects=True,
                                                 vmem_limit_bytes=56 * 1024 * 1024),
        )(m_blk, z_blk, msa_mask, res_mask.reshape(1, RES), *weights)

    return jax.shard_map(per_device, mesh=mesh, in_specs=in_specs, out_specs=(rows, rows), check_vma=False)
```

```python
import functools

import jax
import jax.numpy as jnp
from jax import lax
from jax.experimental import pallas as pl
from jax.experimental.pallas import tpu as pltpu
from jax.sharding import PartitionSpec as P

BF16 = jnp.bfloat16
F32 = jnp.float32
MESH = pl.DeviceIdType.MESH
NDEV = 8
SEQ, RES, CM, CZ = 256, 96, 256, 128
SLOC, RLOC = SEQ // NDEV, RES // NDEV
HM, HT, HD, OPM = 8, 4, 32, 32
LANES = 128
MASKED = -1e9
PADDED = -3e38
SCALE = HD ** -0.5

ROWB, MF, MB, STB, ZF, ENB, ZB = 0, 1, 5, 6, 7, 8, 9
NSTAGE = 10
CHUNK = 8
NCHUNK = SLOC // CHUNK
CROWS = NDEV * CHUNK
LAG = 2
MB_EARLY = 6


def dot(a, b):
    return jnp.dot(a, b, preferred_element_type=F32)


def dot_t(a, b):
    return lax.dot_general(a, b, (((1,), (1,)), ((), ())), preferred_element_type=F32)


def iota(shape, dim):
    return lax.broadcasted_iota(jnp.int32, shape, dim)


def layer_norm(x):
    values = x.astype(F32)
    centred = values - jnp.mean(values, axis=-1, keepdims=True)
    variance = jnp.mean(centred * centred, axis=-1, keepdims=True)
    return (centred * lax.rsqrt(variance + 1e-5)).astype(BF16)


def add_residual(state, update):
    return (state.astype(F32) + update).astype(BF16)


def head_masks():
    lane = iota((16, LANES), 1)
    return [jnp.where((lane >= h * HD) & (lane < (h + 1) * HD), 1.0, 0.0).astype(BF16) for h in range(LANES // HD)]


def only_head(x, mask):
    return (x.reshape(x.shape[0] // 16, 16, LANES) * mask[None]).reshape(x.shape)


def softmax_rows(logits):
    top = jnp.max(logits, axis=-1, keepdims=True)
    weights = jnp.exp(logits - top)
    return (weights * (1.0 / jnp.sum(weights, axis=-1, keepdims=True))).astype(BF16)


def gate(tiles, g):
    mixed = tiles[0] if len(tiles) == 1 else jnp.concatenate(tiles, axis=1)
    return (mixed * jax.nn.sigmoid(g.astype(F32))).astype(BF16)


def attend_padded(q, k, v, g, bias_ref, keep, heads):
    masks = head_masks()
    tiles = []
    for t in range(heads // 4):
        lanes = slice(t * LANES, (t + 1) * LANES)
        probs = []
        for pair in range(2):
            kk = jnp.concatenate([only_head(k[:, lanes], masks[2 * pair + u]) for u in range(2)], axis=0)
            scores = dot_t(q[:, lanes], kk)
            for u in range(2):
                logits = scores[:, u * LANES:(u + 1) * LANES] * SCALE + bias_ref[4 * t + 2 * pair + u]
                probs.append(softmax_rows(jnp.where(keep, logits, MASKED)))
        vv = jnp.concatenate([only_head(v[:, lanes], mask) for mask in masks], axis=0)
        tiles.append(dot(jnp.concatenate(probs, axis=1), vv))
    return gate(tiles, g)


def attend_column(q, k, v, g, keep):
    masks = head_masks()
    tiles = []
    for t in range(HM // 4):
        lanes = slice(t * LANES, (t + 1) * LANES)
        probs = []
        for mask in masks:
            logits = dot_t(q[:, lanes], only_head(k[:, lanes], mask)) * SCALE
            probs.append(softmax_rows(jnp.where(keep, logits, MASKED)))
        vv = jnp.concatenate([only_head(v[:, lanes], mask) for mask in masks], axis=0)
        tiles.append(dot(jnp.concatenate(probs, axis=1), vv))
    return gate(tiles, g)


def block_kernel(m_ref, z_ref, mask_ref, res_ref, w_row_in, w_row_bias, w_row_out, w_col_in, w_col_out,
                 w_opm_in, w_opm_out, w_start_in, w_start_bias, w_start_out, w_end_in, w_end_bias, w_end_out,
                 m_out, z_out,
                 perm, perm_out, perm_in, comp, hperm, keep_row, mask_t, norm, res_keep, wbt, bcol, bias,
                 rowb_recv, stb_recv, enb_recv, proj, gated, projt, m1, msend, mcols, mback, colproj,
                 left, crecv, cbig, outer, w2, w2t, ynorm, z1, zs, zr, z2, z3, zs2, zr2,
                 send_sem, recv_sem, local_sem, c_send, c_recv, c_pair):
    data = lax.axis_index('data')
    me = lax.axis_index('chip') * 4 + lax.axis_index('dap')
    core, chip_x, chip_y = lax.rem(me, 2), lax.rem(me // 2, 2), me // 4
    partner = me + 1 - 2 * core
    to_x, to_y = 2 - 4 * chip_x, 4 - 8 * chip_y
    twins = (me + to_x + to_y, me + to_x, me + to_y)

    def device(d):
        return (data, d // 4, lax.rem(d, 4))

    def peer(r):
        return lax.rem(me + r, NDEV)

    def source(r):
        return lax.rem(me + NDEV - r, NDEV)

    def remote(src, dst, send, recv, d):
        return pltpu.make_async_remote_copy(src_ref=src, dst_ref=dst, send_sem=send, recv_sem=recv,
                                            device_id=device(d), device_id_type=MESH)

    def start_all(stage, src_of, dst_of):
        for r in range(1, NDEV):
            d = peer(r)
            remote(src_of(d), dst_of(me), send_sem.at[stage, r], recv_sem.at[stage, r], d).start()

    def wait_recv(stage, dst_of):
        for r in range(1, NDEV):
            dst = dst_of(source(r))
            remote(dst, dst, send_sem.at[stage, r], recv_sem.at[stage, r], peer(r)).wait_recv()

    def wait_send(stage, src_of):
        for r in range(1, NDEV):
            src = src_of(peer(r))
            remote(src, src, send_sem.at[stage, r], recv_sem.at[stage, r], peer(r)).wait_send()

    barrier = pltpu.get_barrier_semaphore()
    for r in range(1, NDEV):
        pl.semaphore_signal(barrier, inc=1, device_id=device(peer(r)), device_id_type=MESH)

    r0, c0 = iota((256, 256), 0), iota((256, 256), 1)
    perm[...] = jnp.where(((r0 >> 4) == (c0 & 15)) & ((r0 & 15) == (c0 >> 4)), 1.0, 0.0).astype(BF16)
    perm_out[...] = jnp.where(((r0 >> 3) == (c0 & 31)) & ((r0 & 7) == (c0 >> 5)), 1.0, 0.0).astype(BF16)
    perm_in[...] = jnp.where(((r0 >> 5) == (c0 & 7)) & ((r0 & 31) == (c0 >> 3)), 1.0, 0.0).astype(BF16)
    r1, c1 = iota((RES, LANES), 0), iota((RES, LANES), 1)
    comp[...] = jnp.where(((c1 & 15) < RLOC) & (r1 == (c1 >> 4) * RLOC + (c1 & 15)), 1.0, 0.0).astype(BF16)
    r2, c2 = iota((LANES, LANES), 0), iota((LANES, LANES), 1)
    hperm[...] = jnp.where(((r2 >> 4) == (c2 & 7)) & ((r2 & 15) == (c2 >> 3)), 1.0, 0.0).astype(BF16)
    bcol[...] = jnp.zeros_like(bcol)
    wbt[...] = jnp.zeros_like(wbt)
    for n, w in enumerate((w_row_bias, w_start_bias, w_end_bias)):
        wbt[n, 0:w.shape[0], :] = w[...].astype(F32)

    def send_bias(recv, which, heads, stage):
        weights = wbt[which].astype(BF16)

        @pl.loop(0, RLOC)
        def _(i):
            bcol[i, :, 0:RES] = dot_t(weights, ynorm[i])

        mine = dot(hperm[0:heads * 16, :], bcol[...].reshape(LANES, LANES).astype(BF16)).astype(BF16)
        rows = pl.ds(pl.multiple_of(me * 16, 16), 16)
        recv[:, rows, :] = mine.reshape(heads, 16, LANES)
        start_all(stage, lambda d: recv.at[:, rows, :], lambda s: recv.at[:, rows, :])

    def bias_rows(recv):
        return lambda s: recv.at[:, pl.ds(pl.multiple_of(s * 16, 16), 16), :]

    def take_bias(recv, heads, stage):
        wait_recv(stage, bias_rows(recv))
        lane = iota((RES, LANES), 1)
        for h in range(heads):
            bias[h] = jnp.where(lane < RES, dot(comp[...], recv[h]), PADDED)

    @pl.loop(0, RLOC)
    def _(i):
        ynorm[i] = layer_norm(z_ref[i])

    pl.semaphore_wait(barrier, NDEV - 1)
    send_bias(rowb_recv, 0, HM, ROWB)

    res_keep[...] = jnp.ones_like(res_keep)
    res_keep[0:1, 0:RES] = res_ref[...]
    eye = jnp.where(r2 == c2, 1.0, 0.0).astype(BF16)
    eye256 = jnp.where(r0 == c0, 1.0, 0.0).astype(BF16)
    seq_order = jnp.where(r0 == ((c0 >> 3) & 7) * SLOC + (c0 >> 6) * CHUNK + (c0 & 7), 1.0, 0.0).astype(BF16)
    mt = mask_ref[...].astype(F32).astype(BF16)
    keep_row[...] = jnp.ones_like(keep_row)
    keep_row[:, 0:RES] = dot_t(eye256, mt)
    mask_t[...] = dot(mt, seq_order)
    norm[...] = jnp.zeros_like(norm)
    norm[0:RES, 0:RES] = dot_t(mt, mt)
    w_full = w_opm_out[...].reshape(OPM, OPM, CZ)
    for a in range(2):
        for c in range(2):
            blk = w_full[16 * a:16 * a + 16, 16 * c:16 * c + 16, :].reshape(256, CZ)
            w2[16 * c:16 * c + 16, 16 * a:16 * a + 16, :] = dot(perm[...], blk).astype(BF16).reshape(16, 16, CZ)
    w2t[...] = dot_t(eye, w2[...].reshape(OPM * OPM, CZ)).astype(BF16)
    proj[:, RES:, :] = jnp.zeros((proj.shape[0], LANES - RES, 4 * CM), BF16)
    projt[:, RES:, :] = jnp.zeros((RLOC, LANES - RES, 4 * CZ), BF16)
    cbig[:, RES:, :] = jnp.zeros((OPM, LANES - RES, SEQ), BF16)
    z1[RLOC:, :, :] = jnp.zeros((16 - RLOC, RES, CZ), BF16)
    z3[RLOC:, :, :] = jnp.zeros((16 - RLOC, RES, CZ), BF16)

    take_bias(rowb_recv, HM, ROWB)

    def m_src(q):
        return lambda d: msend.at[q, pl.ds(d * RLOC, RLOC)]

    def m_dst(q):
        return lambda s: mcols.at[q, :, pl.ds(pl.multiple_of(s * CHUNK, CHUNK), CHUNK), :]

    def local_copy(src, dst, n):
        return pltpu.make_async_copy(src, dst, local_sem.at[n])

    def row_chunk(q):
        @pl.loop(0, CHUNK // 4)
        def _(blk):
            s0 = q * CHUNK + blk * 4
            x = m_ref[pl.ds(s0, 4)].reshape(4 * RES, CM)
            proj[:, 0:RES, :] = dot(layer_norm(x), w_row_in[...]).astype(BF16).reshape(4, RES, 4 * CM)
            for u in range(4):
                keep = keep_row[pl.ds(me * SLOC + s0 + u, 1), :] != 0.0
                gated[u] = attend_padded(proj[u, 0:RES, 0:CM], proj[u, :, CM:2 * CM], proj[u, :, 2 * CM:3 * CM],
                                         proj[u, 0:RES, 3 * CM:4 * CM], bias, keep, HM)
            update = dot(gated[...].reshape(4 * RES, CM), w_row_out[...])
            m1[pl.ds(s0, 4)] = add_residual(x, update).reshape(4, RES, CM)

        for j in range(RES // 32):
            blk = m1[CHUNK * q:CHUNK * q + CHUNK, 32 * j:32 * j + 32, :].reshape(256, CM)
            msend[q, 32 * j:32 * j + 32] = dot(perm_out[...], blk).reshape(32, CHUNK, CM).astype(BF16)
        start_all(MF + q, m_src(q), m_dst(q))
        local_copy(m_src(q)(me), m_dst(q)(me), q).start()

    def column_projection(q):
        local_copy(m_src(q)(me), m_dst(q)(me), q).wait()
        wait_recv(MF + q, m_dst(q))

        @pl.loop(0, RLOC // 4)
        def _(blk):
            x = mcols[q, pl.ds(blk * 4, 4)].reshape(4 * CROWS, CM)
            y = dot(layer_norm(x), w_col_in[...]).astype(BF16).reshape(4, CROWS, 4 * CM)
            colproj[pl.ds(blk * 4, 4), CROWS * q:CROWS * q + CROWS, :] = y

    row_chunk(0)
    row_chunk(1)
    row_chunk(2)
    column_projection(0)
    row_chunk(3)
    column_projection(1)
    column_projection(2)
    column_projection(3)

    def mb_start(j):
        start_all(MB, lambda d: mcols.at[:, j, pl.ds(pl.multiple_of(d * CHUNK, CHUNK), CHUNK), :],
                  lambda s: mback.at[:, pl.ds(pl.multiple_of((s * RLOC + j) * CHUNK, CHUNK), CHUNK), :])

    def relay(j):
        for t, twin in enumerate(twins):
            row = crecv.at[twin * RLOC + j]
            remote(row, row, c_send.at[t], c_recv.at[t, j], twin).wait_recv()
            remote(row, row, c_send.at[3 + t], c_pair.at[t], partner).start()

    @pl.loop(0, RLOC)
    def _(j):
        x = mcols[:, j].reshape(SEQ, CM)
        mask_row = mask_t[pl.ds(me * RLOC + j, 1), :]
        mixed = attend_column(colproj[j, :, 0:CM], colproj[j, :, CM:2 * CM], colproj[j, :, 2 * CM:3 * CM],
                              colproj[j, :, 3 * CM:], mask_row != 0.0)
        x = add_residual(x, dot(mixed, w_col_out[...]))
        both = dot_t(w_opm_in[...], layer_norm(x)).astype(BF16).astype(F32) * mask_row
        left[j] = both[0:OPM].astype(BF16)
        crecv[me * RLOC + j] = both[OPM:].astype(BF16)
        row = crecv.at[me * RLOC + j]
        for t, twin in enumerate(twins):
            remote(row, row, c_send.at[t], c_recv.at[t, j], twin).start()
        remote(row, row, c_send.at[6], c_pair.at[3], partner).start()
        mcols[:, j] = x.reshape(NCHUNK, CROWS, CM)

        @pl.when(j >= LAG)
        def _():
            relay(j - LAG)

        @pl.when(j < MB_EARLY)
        def _():
            mb_start(j)

    for j in range(RLOC - LAG, RLOC):
        relay(j)
    for q in range(NCHUNK):
        mine = mcols[q, :, pl.ds(pl.multiple_of(me * CHUNK, CHUNK), CHUNK), :]
        mback[q, pl.ds(pl.multiple_of(me * (RLOC * CHUNK), 32), RLOC * CHUNK), :] = mine.reshape(RLOC * CHUNK, CM)

    def c_rows(s):
        return crecv.at[pl.ds(s * RLOC, RLOC)]

    for t, first in enumerate(twins + (me,)):
        rows = c_rows(first + 1 - 2 * core)
        remote(rows, rows, c_send.at[3 + t], c_pair.at[t], partner).wait_recv()
    for j in range(MB_EARLY, MB_EARLY + 3):
        mb_start(j)
    for c in range(2):
        @pl.loop(0, RES // 16)
        def _(j):
            j0 = pl.multiple_of(j * 16, 16)
            blk = crecv[pl.ds(j0, 16), 16 * c:16 * c + 16, :].reshape(256, SEQ)
            cbig[16 * c:16 * c + 16, pl.ds(j0, 16), :] = dot(perm[...], blk).astype(BF16).reshape(16, 16, SEQ)

    @pl.loop(0, OPM // 2)
    def _(c):
        prod = dot_t(left[...].reshape(RLOC * OPM, SEQ), cbig[pl.ds(2 * c, 2)].reshape(256, SEQ)).astype(BF16)
        for u in range(2):
            outer[:, 2 * c + u] = prod[:, u * LANES:(u + 1) * LANES].reshape(RLOC, OPM, LANES)

    @pl.loop(0, RLOC)
    def _(i):
        update = dot(w2t[...], outer[i].reshape(OPM * OPM, LANES))
        update = update / (1e-3 + norm[pl.ds(me * RLOC + i, 1), :])
        z1[i] = add_residual(z_ref[i], jnp.transpose(update)[0:RES])

    def triangle(state, result, w_in, which, w_out, recv, stage, late):
        @pl.loop(0, RLOC)
        def _(i):
            ynorm[i] = layer_norm(state[i])
        send_bias(recv, which, HT, stage)

        @pl.loop(0, RLOC // 4)
        def _(blk):
            y = ynorm[pl.ds(blk * 4, 4)].reshape(4 * RES, CZ)
            projt[pl.ds(blk * 4, 4), 0:RES, :] = dot(y, w_in[...]).astype(BF16).reshape(4, RES, 4 * CZ)
        take_bias(recv, HT, stage)
        for j in late:
            mb_start(j)
        keep = res_keep[0:1, :] != 0

        @pl.loop(0, RLOC // 4)
        def _(blk):
            i0 = blk * 4
            for u in range(4):
                i = i0 + u
                gated[u, :, 0:CZ] = attend_padded(projt[i, 0:RES, 0:CZ], projt[i, :, CZ:2 * CZ],
                                                  projt[i, :, 2 * CZ:3 * CZ], projt[i, 0:RES, 3 * CZ:4 * CZ],
                                                  bias, keep, HT)
            update = dot(gated[:, :, 0:CZ].reshape(4 * RES, CZ), w_out[...])
            x = state[pl.ds(i0, 4)].reshape(4 * RES, CZ)
            result[pl.ds(i0, 4)] = add_residual(x, update).reshape(4, RES, CZ)

    def z_src(buf):
        return lambda d: buf.at[pl.ds(d * RLOC, RLOC)]

    def z_dst(buf):
        return lambda s: buf.at[:, pl.ds(pl.multiple_of(s * 16, 16), 16), :]

    def exchange(state, send, recv, result, stage, n):
        for j in range(RES // 16):
            blk = state[:, 16 * j:16 * j + 16, :].reshape(256, CZ)
            send[16 * j:16 * j + 16] = dot(perm[...], blk).astype(BF16).reshape(16, 16, CZ)
        start_all(stage, z_src(send), z_dst(recv))
        own = local_copy(z_src(send)(me), z_dst(recv)(me), n)
        own.start()
        own.wait()
        wait_recv(stage, z_dst(recv))

        @pl.loop(0, RLOC)
        def _(i):
            result[i] = dot(comp[...], recv[i]).astype(BF16)

    triangle(z1, z1, w_start_in, 1, w_start_out, stb_recv, STB, (MB_EARLY + 3, MB_EARLY + 4))
    exchange(z1, zs, zr, z2, ZF, NCHUNK)
    triangle(z2, z3, w_end_in, 2, w_end_out, enb_recv, ENB, (MB_EARLY + 5,))
    exchange(z3, zs2, zr2, z_out, ZB, NCHUNK + 1)

    def mb_dst(s):
        return mback.at[:, pl.ds(pl.multiple_of(s * (RLOC * CHUNK), 32), RLOC * CHUNK), :]
    wait_recv(MB, mb_dst)
    for q in range(NCHUNK):
        @pl.loop(0, RES // 32)
        def _(j):
            blk = mback[q, pl.ds(pl.multiple_of(j * 256, 256), 256), :]
            rows = dot(perm_in[...], blk).astype(BF16).reshape(CHUNK, 32, CM)
            m_out[CHUNK * q:CHUNK * q + CHUNK, pl.ds(pl.multiple_of(j * 32, 32), 32), :] = rows

    wait_send(ROWB, lambda d: bias_rows(rowb_recv)(me))
    for q in range(NCHUNK):
        wait_send(MF + q, m_src(q))
    wait_send(MB, lambda d: mcols.at[:, :, pl.ds(pl.multiple_of(d * CHUNK, CHUNK), CHUNK), :])
    for t in range(7):
        rows = c_rows(me if t in (0, 1, 2, 6) else twins[t - 3])
        remote(rows, rows, c_send.at[t], c_pair.at[0], partner).wait_send()
    wait_send(STB, lambda d: bias_rows(stb_recv)(me))
    wait_send(ZF, z_src(zs))
    wait_send(ENB, lambda d: bias_rows(enb_recv)(me))
    wait_send(ZB, z_src(zs2))


def solution(mesh):
    rows = P(('data', 'chip', 'dap'))
    in_specs = (rows, rows, P('data'), P('data')) + (P(),) * 13
    vmem = pl.BlockSpec(memory_space=pltpu.VMEM)

    def per_device(m_blk, z_blk, msa_mask, res_mask, w_row_in, w_row_bias, w_row_out, w_col_in, w_col_out,
                   w_opm_in, w_opm_out, w_start_in, w_start_bias, w_start_out, w_end_in, w_end_bias, w_end_out):
        scratch = [
            pltpu.VMEM((256, 256), BF16),
            pltpu.VMEM((256, 256), BF16),
            pltpu.VMEM((256, 256), BF16),
            pltpu.VMEM((RES, LANES), BF16),
            pltpu.VMEM((LANES, LANES), BF16),
            pltpu.VMEM((SEQ, LANES), F32),
            pltpu.VMEM((RES, SEQ), F32),
            pltpu.VMEM((LANES, LANES), F32),
            pltpu.VMEM((8, LANES), jnp.int32),
            pltpu.VMEM((3, 8, CZ), F32),
            pltpu.VMEM((16, 8, LANES), F32),
            pltpu.VMEM((HM, RES, LANES), F32),
            pltpu.VMEM((HM, LANES, LANES), BF16),
            pltpu.VMEM((HT, LANES, LANES), BF16),
            pltpu.VMEM((HT, LANES, LANES), BF16),
            pltpu.VMEM((4, LANES, 4 * CM), BF16),
            pltpu.VMEM((4, RES, CM), BF16),
            pltpu.VMEM((RLOC, LANES, 4 * CZ), BF16),
            pltpu.VMEM((SLOC, RES, CM), BF16),
            pltpu.VMEM((NCHUNK, RES, CHUNK, CM), BF16),
            pltpu.VMEM((NCHUNK, RLOC, CROWS, CM), BF16),
            pltpu.VMEM((NCHUNK, RES * CHUNK, CM), BF16),
            pltpu.VMEM((RLOC, SEQ, 4 * CM), BF16),
            pltpu.VMEM((RLOC, OPM, SEQ), BF16),
            pltpu.VMEM((RES, OPM, SEQ), BF16),
            pltpu.VMEM((OPM, LANES, SEQ), BF16),
            pltpu.VMEM((RLOC, OPM, OPM, LANES), BF16),
            pltpu.VMEM((OPM, OPM, CZ), BF16),
            pltpu.VMEM((CZ, OPM * OPM), BF16),
            pltpu.VMEM((RLOC, RES, CZ), BF16),
            pltpu.VMEM((16, RES, CZ), BF16),
            pltpu.VMEM((RES, 16, CZ), BF16),
            pltpu.VMEM((RLOC, LANES, CZ), BF16),
            pltpu.VMEM((RLOC, RES, CZ), BF16),
            pltpu.VMEM((16, RES, CZ), BF16),
            pltpu.VMEM((RES, 16, CZ), BF16),
            pltpu.VMEM((RLOC, LANES, CZ), BF16),
            pltpu.SemaphoreType.DMA((NSTAGE, NDEV)),
            pltpu.SemaphoreType.DMA((NSTAGE, NDEV)),
            pltpu.SemaphoreType.DMA((NCHUNK + 2,)),
            pltpu.SemaphoreType.DMA((7,)),
            pltpu.SemaphoreType.DMA((3, RLOC)),
            pltpu.SemaphoreType.DMA((4,)),
        ]
        return pl.pallas_call(
            block_kernel,
            name='evoformer_block',
            out_shape=(jax.ShapeDtypeStruct(m_blk.shape, BF16), jax.ShapeDtypeStruct(z_blk.shape, BF16)),
            in_specs=[vmem] * 17,
            out_specs=(vmem, vmem),
            scratch_shapes=scratch,
            compiler_params=pltpu.CompilerParams(collective_id=0, has_side_effects=True,
                                                 vmem_limit_bytes=56 * 1024 * 1024),
        )(m_blk, z_blk, msa_mask.T, res_mask.reshape(1, RES), w_row_in, w_row_bias.T, w_row_out, w_col_in, w_col_out,
          w_opm_in.T, w_opm_out, w_start_in, w_start_bias.T, w_start_out, w_end_in, w_end_bias.T, w_end_out)

    return jax.shard_map(per_device, mesh=mesh, in_specs=in_specs, out_specs=(rows, rows), check_vma=False)
```

```python
import functools

import jax
import jax.numpy as jnp
from jax import lax
from jax.experimental import pallas as pl
from jax.experimental.pallas import tpu as pltpu
from jax.sharding import PartitionSpec as P

BF16 = jnp.bfloat16
F32 = jnp.float32
MESH = pl.DeviceIdType.MESH
NDEV = 8
SEQ, RES, CM, CZ = 256, 96, 256, 128
SLOC, RLOC = SEQ // NDEV, RES // NDEV
HM, HT, HD, OPM = 8, 4, 32, 32
LANES = 128
MASKED = -1e9
SCALE = HD ** -0.5

ROWB, MF, MB, STB, ZF, ENB, ZB = 0, 1, 5, 6, 7, 8, 9
NSTAGE = 10
CHUNK = 8
NCHUNK = SLOC // CHUNK
CROWS = NDEV * CHUNK
LAG = 2
MB_EARLY = 6


def dot(a, b):
    return jnp.dot(a, b, preferred_element_type=F32)


def dot_t(a, b):
    return lax.dot_general(a, b, (((1,), (1,)), ((), ())), preferred_element_type=F32)


def iota(shape, dim):
    return lax.broadcasted_iota(jnp.int32, shape, dim)


def layer_norm(x):
    values = x.astype(F32)
    centred = values - jnp.mean(values, axis=-1, keepdims=True)
    variance = jnp.mean(centred * centred, axis=-1, keepdims=True)
    return (centred * lax.rsqrt(variance + 1e-5)).astype(BF16)


def add_residual(state, update):
    return (state.astype(F32) + update).astype(BF16)


def head_masks():
    lane = iota((16, LANES), 1)
    return [jnp.where((lane >= h * HD) & (lane < (h + 1) * HD), 1.0, 0.0).astype(BF16) for h in range(LANES // HD)]


def only_head(x, mask):
    return (x.reshape(x.shape[0] // 16, 16, LANES) * mask[None]).reshape(x.shape)


def dot_tl(a, b):
    return lax.dot_general(a, b, (((0,), (0,)), ((), ())), preferred_element_type=F32)


def softmax_keys(logits):
    weights = jnp.exp(logits - jnp.max(logits, axis=0, keepdims=True))
    return (weights * (1.0 / jnp.sum(weights, axis=0, keepdims=True))).astype(BF16)


def pipeline(items, first, middle, last, finish):
    opened, ready = {0: first(items[0])}, {}
    for n in range(len(items) + 2):
        if n + 1 < len(items):
            opened[n + 1] = first(items[n + 1])
        if n < len(items):
            ready[n] = middle(items[n], opened.pop(n))
        if 1 <= n <= len(items):
            last(items[n - 1], ready.pop(n - 1))
        if n >= 2:
            finish(items[n - 2])


def attend_biased(rows, tiles, q_of, k_of, vg_of, bias_ref, keep_of, w_out, store):
    masks = head_masks()
    each = len(masks)
    offsets = {u: (keep_of(u) - 1.0) * -MASKED for u in rows}
    vgs = {}
    mixed = {u: [] for u in rows}

    def first(item):
        u, t = item
        if t == 0:
            vgs[u] = vg_of(u)
        k = k_of(u, t)
        return dot_t(jnp.concatenate([only_head(k, mask) for mask in masks], axis=0), q_of(u, t))

    def middle(item, scores):
        u, t = item
        return [softmax_keys((scores[n * RES:(n + 1) * RES] * SCALE + bias_ref[each * t + n]) * keep_of(u) + offsets[u])
                for n in range(each)]

    def last(item, probs):
        u, t = item
        for n in range(each):
            h = each * t + n
            mixed[u].append(dot(vgs[u][h * HD:(h + 1) * HD], probs[n]))

    def finish(item):
        u, t = item
        if t == tiles - 1:
            gates = jax.nn.sigmoid(vgs[u][tiles * LANES:].astype(F32))
            store(u, dot_tl((jnp.concatenate(mixed[u], axis=0) * gates).astype(BF16), w_out))

    pipeline([(u, t) for u in rows for t in range(tiles)], first, middle, last, finish)


def attend_column(residues, q_of, k_of, vg_of, keep_of, w_out, store):
    masks = head_masks()
    each = len(masks)
    keeps, vgs = {}, {}
    mixed = {u: [] for u in residues}

    def first(item):
        u, h = item
        if h == 0:
            keeps[u] = keep_of(u)
            vgs[u] = vg_of(u)
        return dot_t(only_head(k_of(u, h // each), masks[h % each]), q_of(u, h // each))

    def middle(item, scores):
        return softmax_keys(scores * (keeps[item[0]] * SCALE) + (keeps[item[0]] - 1.0) * -MASKED)

    def last(item, probs):
        u, h = item
        mixed[u].append(dot(vgs[u][h * HD:(h + 1) * HD], probs))

    def finish(item):
        u, h = item
        if h == HM - 1:
            gates = jax.nn.sigmoid(vgs[u][CM:].astype(F32))
            store(u, dot_tl((jnp.concatenate(mixed[u], axis=0) * gates).astype(BF16), w_out))

    pipeline([(u, h) for u in residues for h in range(HM)], first, middle, last, finish)


def block_kernel(m_ref, z_ref, mask_ref, res_ref, w_row_in, w_row_bias, w_row_out, w_col_in, w_col_out,
                 w_opm_in, w_opm_out, w_start_in, w_start_bias, w_start_out, w_end_in, w_end_bias, w_end_out,
                 m_out, z_out,
                 perm, perm_out, perm_in, comp, hperm, keep_row, mask_t, mask_s, norm, res_keep, wbt, bcol, bias,
                 rowb_recv, stb_recv, enb_recv, row_vg, col_vg, tri_vg, yrow, rowqk, triqk, m1, msend, mcols, mback,
                 ycol, colqk,
                 left, crecv, cbig, outer, w2, w2t, ynorm, z1, zs, zr, z2, z3, zs2, zr2,
                 send_sem, recv_sem, local_sem, c_send, c_recv, c_pair):
    data = lax.axis_index('data')
    me = lax.axis_index('chip') * 4 + lax.axis_index('dap')
    core, chip_x, chip_y = lax.rem(me, 2), lax.rem(me // 2, 2), me // 4
    partner = me + 1 - 2 * core
    to_x, to_y = 2 - 4 * chip_x, 4 - 8 * chip_y
    twins = (me + to_x + to_y, me + to_x, me + to_y)

    def device(d):
        return (data, d // 4, lax.rem(d, 4))

    def peer(r):
        return lax.rem(me + r, NDEV)

    def source(r):
        return lax.rem(me + NDEV - r, NDEV)

    def remote(src, dst, send, recv, d):
        return pltpu.make_async_remote_copy(src_ref=src, dst_ref=dst, send_sem=send, recv_sem=recv,
                                            device_id=device(d), device_id_type=MESH)

    def start_all(stage, src_of, dst_of):
        for r in range(1, NDEV):
            d = peer(r)
            remote(src_of(d), dst_of(me), send_sem.at[stage, r], recv_sem.at[stage, r], d).start()

    def wait_recv(stage, dst_of):
        for r in range(1, NDEV):
            dst = dst_of(source(r))
            remote(dst, dst, send_sem.at[stage, r], recv_sem.at[stage, r], peer(r)).wait_recv()

    def wait_send(stage, src_of):
        for r in range(1, NDEV):
            src = src_of(peer(r))
            remote(src, src, send_sem.at[stage, r], recv_sem.at[stage, r], peer(r)).wait_send()

    barrier = pltpu.get_barrier_semaphore()
    for r in range(1, NDEV):
        pl.semaphore_signal(barrier, inc=1, device_id=device(peer(r)), device_id_type=MESH)

    r0, c0 = iota((256, 256), 0), iota((256, 256), 1)
    perm[...] = jnp.where(((r0 >> 4) == (c0 & 15)) & ((r0 & 15) == (c0 >> 4)), 1.0, 0.0).astype(BF16)
    perm_out[...] = jnp.where(((r0 >> 3) == (c0 & 31)) & ((r0 & 7) == (c0 >> 5)), 1.0, 0.0).astype(BF16)
    perm_in[...] = jnp.where(((r0 >> 5) == (c0 & 7)) & ((r0 & 31) == (c0 >> 3)), 1.0, 0.0).astype(BF16)
    r1, c1 = iota((RES, LANES), 0), iota((RES, LANES), 1)
    comp[...] = jnp.where(((c1 & 15) < RLOC) & (r1 == (c1 >> 4) * RLOC + (c1 & 15)), 1.0, 0.0).astype(BF16)
    r2, c2 = iota((LANES, LANES), 0), iota((LANES, LANES), 1)
    hperm[...] = jnp.where(((r2 >> 4) == (c2 & 7)) & ((r2 & 15) == (c2 >> 3)), 1.0, 0.0).astype(BF16)
    eye = jnp.where(r2 == c2, 1.0, 0.0).astype(BF16)
    bcol[...] = jnp.zeros_like(bcol)
    wbt[...] = jnp.zeros_like(wbt)
    for n, w in enumerate((w_row_bias, w_start_bias, w_end_bias)):
        wbt[n, 0:w.shape[0], :] = w[...].astype(F32)

    def send_bias(recv, which, heads, stage):
        weights = wbt[which].astype(BF16)

        @pl.loop(0, RLOC)
        def _(i):
            bcol[i, :, 0:RES] = dot_t(weights, ynorm[i])

        mine = dot(hperm[0:heads * 16, :], bcol[...].reshape(LANES, LANES).astype(BF16)).astype(BF16)
        rows = pl.ds(pl.multiple_of(me * 16, 16), 16)
        recv[:, rows, :] = mine.reshape(heads, 16, LANES)
        start_all(stage, lambda d: recv.at[:, rows, :], lambda s: recv.at[:, rows, :])

    def bias_rows(recv):
        return lambda s: recv.at[:, pl.ds(pl.multiple_of(s * 16, 16), 16), :]

    def take_bias(recv, heads, stage):
        wait_recv(stage, bias_rows(recv))
        for h in range(heads):
            bias[h] = dot_t(eye, dot(comp[...], recv[h]).astype(BF16))[0:RES]

    @pl.loop(0, RLOC)
    def _(i):
        ynorm[i] = layer_norm(z_ref[i])

    pl.semaphore_wait(barrier, NDEV - 1)
    send_bias(rowb_recv, 0, HM, ROWB)

    res_keep[...] = dot((eye[0:RES, 0:RES].astype(F32) * res_ref[...].astype(F32)).astype(BF16),
                        jnp.ones((RES, LANES), BF16))
    seq_order = jnp.where(r0 == ((c0 >> 3) & 7) * SLOC + (c0 >> 6) * CHUNK + (c0 & 7), 1.0, 0.0).astype(BF16)
    seq_rows = jnp.where(c0 == ((r0 >> 3) & 7) * SLOC + (r0 >> 6) * CHUNK + (r0 & 7), 1.0, 0.0).astype(BF16)
    mt = mask_ref[...].astype(F32).astype(BF16)
    mask_t[...] = dot(mt, seq_order)
    mask_s[...] = dot_t(seq_rows, mt).astype(BF16)

    @pl.loop(0, SLOC)
    def _(i):
        pick = jnp.where(iota((SEQ, LANES), 0) == me * SLOC + i, 1.0, 0.0).astype(BF16)
        keep_row[i] = dot(mask_ref[...].astype(F32).astype(BF16), pick)

    row_vg[...] = jnp.transpose(w_row_in[:, 2 * CM:].astype(F32)).astype(BF16)
    col_vg[...] = jnp.transpose(w_col_in[:, 2 * CM:].astype(F32)).astype(BF16)
    tri_vg[0] = jnp.transpose(w_start_in[:, 2 * CZ:].astype(F32)).astype(BF16)
    tri_vg[1] = jnp.transpose(w_end_in[:, 2 * CZ:].astype(F32)).astype(BF16)
    norm[...] = jnp.zeros_like(norm)
    norm[0:RES, 0:RES] = dot_t(mt, mt)
    w_full = w_opm_out[...].reshape(OPM, OPM, CZ)
    for a in range(2):
        for c in range(2):
            blk = w_full[16 * a:16 * a + 16, 16 * c:16 * c + 16, :].reshape(256, CZ)
            w2[16 * c:16 * c + 16, 16 * a:16 * a + 16, :] = dot(perm[...], blk).astype(BF16).reshape(16, 16, CZ)
    w2t[...] = dot_t(eye, w2[...].reshape(OPM * OPM, CZ)).astype(BF16)
    cbig[:, RES:, :] = jnp.zeros((OPM, LANES - RES, SEQ), BF16)
    z1[RLOC:, :, :] = jnp.zeros((16 - RLOC, RES, CZ), BF16)
    z3[RLOC:, :, :] = jnp.zeros((16 - RLOC, RES, CZ), BF16)

    take_bias(rowb_recv, HM, ROWB)

    def m_src(q):
        return lambda d: msend.at[q, pl.ds(d * RLOC, RLOC)]

    def m_dst(q):
        return lambda s: mcols.at[q, :, pl.ds(pl.multiple_of(s * CHUNK, CHUNK), CHUNK), :]

    def local_copy(src, dst, n):
        return pltpu.make_async_copy(src, dst, local_sem.at[n])

    def row_chunk(q):
        @pl.loop(0, CHUNK // 4)
        def _(blk):
            s0 = q * CHUNK + blk * 4
            x = m_ref[pl.ds(s0, 4)].reshape(4 * RES, CM)
            y = layer_norm(x)
            yrow[...] = y.reshape(4, RES, CM)
            qk = dot(y, w_row_in[:, 0:2 * CM]).astype(BF16)
            for t in range(4):
                rowqk[t] = qk[:, t * LANES:(t + 1) * LANES].reshape(4, RES, LANES)

            def store(u, update):
                m1[s0 + u] = add_residual(m_ref[s0 + u], update)
            attend_biased(range(4), 2, lambda u, t: rowqk[t, u], lambda u, t: rowqk[2 + t, u],
                          lambda u: dot_t(row_vg[...], yrow[u]).astype(BF16), bias,
                          lambda u: keep_row[s0 + u, :, 0:RES], w_row_out[...], store)

        for j in range(RES // 32):
            blk = m1[CHUNK * q:CHUNK * q + CHUNK, 32 * j:32 * j + 32, :].reshape(256, CM)
            msend[q, 32 * j:32 * j + 32] = dot(perm_out[...], blk).reshape(32, CHUNK, CM).astype(BF16)
        start_all(MF + q, m_src(q), m_dst(q))
        local_copy(m_src(q)(me), m_dst(q)(me), q).start()

    def column_projection(q):
        local_copy(m_src(q)(me), m_dst(q)(me), q).wait()
        wait_recv(MF + q, m_dst(q))

        @pl.loop(0, RLOC // 4)
        def _(blk):
            x = mcols[q, pl.ds(blk * 4, 4)].reshape(4 * CROWS, CM)
            y = layer_norm(x)
            ycol[pl.ds(blk * 4, 4), CROWS * q:CROWS * q + CROWS, :] = y.reshape(4, CROWS, CM)
            qk = dot(y, w_col_in[:, 0:2 * CM]).astype(BF16)
            for t in range(4):
                colqk[t, pl.ds(blk * 4, 4), CROWS * q:CROWS * q + CROWS, :] = (
                    qk[:, t * LANES:(t + 1) * LANES].reshape(4, CROWS, LANES))

    row_chunk(0)
    row_chunk(1)
    row_chunk(2)
    column_projection(0)
    row_chunk(3)
    column_projection(1)
    column_projection(2)
    column_projection(3)

    def mb_start(j):
        start_all(MB, lambda d: mcols.at[:, j, pl.ds(pl.multiple_of(d * CHUNK, CHUNK), CHUNK), :],
                  lambda s: mback.at[:, pl.ds(pl.multiple_of((s * RLOC + j) * CHUNK, CHUNK), CHUNK), :])

    def relay(j):
        for t, twin in enumerate(twins):
            row = crecv.at[twin * RLOC + j]
            remote(row, row, c_send.at[t], c_recv.at[t, j], twin).wait_recv()
            remote(row, row, c_send.at[3 + t], c_pair.at[t], partner).start()

    @pl.loop(0, RLOC // 2)
    def _(pair):
        def keep_of(u):
            pick = jnp.where(iota((RES, LANES), 0) == me * RLOC + pair * 2 + u, 1.0, 0.0).astype(BF16)
            keep = dot(mask_s[...], pick)
            return jnp.concatenate([keep, keep], axis=1)

        def store(u, update):
            j = pair * 2 + u
            mask_row = mask_t[pl.ds(me * RLOC + j, 1), :]
            x = add_residual(mcols[:, j].reshape(SEQ, CM), update)
            both = dot_t(w_opm_in[...], layer_norm(x)).astype(BF16).astype(F32) * mask_row
            left[j] = both[0:OPM].astype(BF16)
            crecv[me * RLOC + j] = both[OPM:].astype(BF16)
            mcols[:, j] = x.reshape(NCHUNK, CROWS, CM)

        attend_column(range(2), lambda u, t: colqk[t, pair * 2 + u], lambda u, t: colqk[2 + t, pair * 2 + u],
                      lambda u: dot_t(col_vg[...], ycol[pair * 2 + u]).astype(BF16), keep_of, w_col_out[...], store)
        for u in range(2):
            j = pair * 2 + u
            row = crecv.at[me * RLOC + j]
            for t, twin in enumerate(twins):
                remote(row, row, c_send.at[t], c_recv.at[t, j], twin).start()
            remote(row, row, c_send.at[6], c_pair.at[3], partner).start()

        @pl.when(pair >= 1)
        def _():
            for u in range(2):
                relay(pair * 2 - 2 + u)

        @pl.when(pair < MB_EARLY // 2)
        def _():
            for u in range(2):
                mb_start(pair * 2 + u)

    for j in range(RLOC - LAG, RLOC):
        relay(j)
    for q in range(NCHUNK):
        mine = mcols[q, :, pl.ds(pl.multiple_of(me * CHUNK, CHUNK), CHUNK), :]
        mback[q, pl.ds(pl.multiple_of(me * (RLOC * CHUNK), 32), RLOC * CHUNK), :] = mine.reshape(RLOC * CHUNK, CM)

    def c_rows(s):
        return crecv.at[pl.ds(s * RLOC, RLOC)]

    for t, first in enumerate(twins + (me,)):
        rows = c_rows(first + 1 - 2 * core)
        remote(rows, rows, c_send.at[3 + t], c_pair.at[t], partner).wait_recv()
    for j in range(MB_EARLY, MB_EARLY + 3):
        mb_start(j)
    for c in range(2):
        @pl.loop(0, RES // 16)
        def _(j):
            j0 = pl.multiple_of(j * 16, 16)
            blk = crecv[pl.ds(j0, 16), 16 * c:16 * c + 16, :].reshape(256, SEQ)
            cbig[16 * c:16 * c + 16, pl.ds(j0, 16), :] = dot(perm[...], blk).astype(BF16).reshape(16, 16, SEQ)

    @pl.loop(0, OPM // 2)
    def _(c):
        prod = dot_t(left[...].reshape(RLOC * OPM, SEQ), cbig[pl.ds(2 * c, 2)].reshape(256, SEQ)).astype(BF16)
        for u in range(2):
            outer[:, 2 * c + u] = prod[:, u * LANES:(u + 1) * LANES].reshape(RLOC, OPM, LANES)

    @pl.loop(0, RLOC)
    def _(i):
        update = dot(w2t[...], outer[i].reshape(OPM * OPM, LANES))
        update = update / (1e-3 + norm[pl.ds(me * RLOC + i, 1), :])
        z1[i] = add_residual(z_ref[i], jnp.transpose(update)[0:RES])

    def triangle(state, result, w_in, which, w_out, recv, stage, late):
        @pl.loop(0, RLOC)
        def _(i):
            ynorm[i] = layer_norm(state[i])
        send_bias(recv, which, HT, stage)

        @pl.loop(0, RLOC // 4)
        def _(blk):
            y = ynorm[pl.ds(blk * 4, 4)].reshape(4 * RES, CZ)
            qk = dot(y, w_in[:, 0:2 * CZ]).astype(BF16)
            for t in range(2):
                triqk[t, pl.ds(blk * 4, 4)] = qk[:, t * LANES:(t + 1) * LANES].reshape(4, RES, LANES)
        take_bias(recv, HT, stage)
        for j in late:
            mb_start(j)

        @pl.loop(0, RLOC // 4)
        def _(blk):
            def store(u, update):
                result[blk * 4 + u] = add_residual(state[blk * 4 + u], update)
            attend_biased(range(4), 1, lambda u, t: triqk[0, blk * 4 + u], lambda u, t: triqk[1, blk * 4 + u],
                          lambda u: dot_t(tri_vg[which - 1], ynorm[blk * 4 + u]).astype(BF16), bias,
                          lambda u: res_keep[:, 0:RES], w_out[...], store)

    def z_src(buf):
        return lambda d: buf.at[pl.ds(d * RLOC, RLOC)]

    def z_dst(buf):
        return lambda s: buf.at[:, pl.ds(pl.multiple_of(s * 16, 16), 16), :]

    def exchange(state, send, recv, result, stage, n):
        for j in range(RES // 16):
            blk = state[:, 16 * j:16 * j + 16, :].reshape(256, CZ)
            send[16 * j:16 * j + 16] = dot(perm[...], blk).astype(BF16).reshape(16, 16, CZ)
        start_all(stage, z_src(send), z_dst(recv))
        own = local_copy(z_src(send)(me), z_dst(recv)(me), n)
        own.start()
        own.wait()
        wait_recv(stage, z_dst(recv))

        @pl.loop(0, RLOC)
        def _(i):
            result[i] = dot(comp[...], recv[i]).astype(BF16)

    triangle(z1, z1, w_start_in, 1, w_start_out, stb_recv, STB, (MB_EARLY + 3, MB_EARLY + 4))
    exchange(z1, zs, zr, z2, ZF, NCHUNK)
    triangle(z2, z3, w_end_in, 2, w_end_out, enb_recv, ENB, (MB_EARLY + 5,))
    exchange(z3, zs2, zr2, z_out, ZB, NCHUNK + 1)

    def mb_dst(s):
        return mback.at[:, pl.ds(pl.multiple_of(s * (RLOC * CHUNK), 32), RLOC * CHUNK), :]
    wait_recv(MB, mb_dst)
    for q in range(NCHUNK):
        @pl.loop(0, RES // 32)
        def _(j):
            blk = mback[q, pl.ds(pl.multiple_of(j * 256, 256), 256), :]
            rows = dot(perm_in[...], blk).astype(BF16).reshape(CHUNK, 32, CM)
            m_out[CHUNK * q:CHUNK * q + CHUNK, pl.ds(pl.multiple_of(j * 32, 32), 32), :] = rows

    wait_send(ROWB, lambda d: bias_rows(rowb_recv)(me))
    for q in range(NCHUNK):
        wait_send(MF + q, m_src(q))
    wait_send(MB, lambda d: mcols.at[:, :, pl.ds(pl.multiple_of(d * CHUNK, CHUNK), CHUNK), :])
    for t in range(7):
        rows = c_rows(me if t in (0, 1, 2, 6) else twins[t - 3])
        remote(rows, rows, c_send.at[t], c_pair.at[0], partner).wait_send()
    wait_send(STB, lambda d: bias_rows(stb_recv)(me))
    wait_send(ZF, z_src(zs))
    wait_send(ENB, lambda d: bias_rows(enb_recv)(me))
    wait_send(ZB, z_src(zs2))


def solution(mesh):
    rows = P(('data', 'chip', 'dap'))
    in_specs = (rows, rows, P('data'), P('data')) + (P(),) * 13
    vmem = pl.BlockSpec(memory_space=pltpu.VMEM)

    def per_device(m_blk, z_blk, msa_mask, res_mask, w_row_in, w_row_bias, w_row_out, w_col_in, w_col_out,
                   w_opm_in, w_opm_out, w_start_in, w_start_bias, w_start_out, w_end_in, w_end_bias, w_end_out):
        scratch = [
            pltpu.VMEM((256, 256), BF16),
            pltpu.VMEM((256, 256), BF16),
            pltpu.VMEM((256, 256), BF16),
            pltpu.VMEM((RES, LANES), BF16),
            pltpu.VMEM((LANES, LANES), BF16),
            pltpu.VMEM((SLOC, RES, LANES), F32),
            pltpu.VMEM((RES, SEQ), F32),
            pltpu.VMEM((SEQ, RES), BF16),
            pltpu.VMEM((LANES, LANES), F32),
            pltpu.VMEM((RES, LANES), F32),
            pltpu.VMEM((3, 8, CZ), F32),
            pltpu.VMEM((16, 8, LANES), F32),
            pltpu.VMEM((HM, RES, RES), F32),
            pltpu.VMEM((HM, LANES, LANES), BF16),
            pltpu.VMEM((HT, LANES, LANES), BF16),
            pltpu.VMEM((HT, LANES, LANES), BF16),
            pltpu.VMEM((2 * CM, CM), BF16),
            pltpu.VMEM((2 * CM, CM), BF16),
            pltpu.VMEM((2, 2 * CZ, CZ), BF16),
            pltpu.VMEM((4, RES, CM), BF16),
            pltpu.VMEM((4, 4, RES, LANES), BF16),
            pltpu.VMEM((2, RLOC, RES, LANES), BF16),
            pltpu.VMEM((SLOC, RES, CM), BF16),
            pltpu.VMEM((NCHUNK, RES, CHUNK, CM), BF16),
            pltpu.VMEM((NCHUNK, RLOC, CROWS, CM), BF16),
            pltpu.VMEM((NCHUNK, RES * CHUNK, CM), BF16),
            pltpu.VMEM((RLOC, SEQ, CM), BF16),
            pltpu.VMEM((4, RLOC, SEQ, LANES), BF16),
            pltpu.VMEM((RLOC, OPM, SEQ), BF16),
            pltpu.VMEM((RES, OPM, SEQ), BF16),
            pltpu.VMEM((OPM, LANES, SEQ), BF16),
            pltpu.VMEM((RLOC, OPM, OPM, LANES), BF16),
            pltpu.VMEM((OPM, OPM, CZ), BF16),
            pltpu.VMEM((CZ, OPM * OPM), BF16),
            pltpu.VMEM((RLOC, RES, CZ), BF16),
            pltpu.VMEM((16, RES, CZ), BF16),
            pltpu.VMEM((RES, 16, CZ), BF16),
            pltpu.VMEM((RLOC, LANES, CZ), BF16),
            pltpu.VMEM((RLOC, RES, CZ), BF16),
            pltpu.VMEM((16, RES, CZ), BF16),
            pltpu.VMEM((RES, 16, CZ), BF16),
            pltpu.VMEM((RLOC, LANES, CZ), BF16),
            pltpu.SemaphoreType.DMA((NSTAGE, NDEV)),
            pltpu.SemaphoreType.DMA((NSTAGE, NDEV)),
            pltpu.SemaphoreType.DMA((NCHUNK + 2,)),
            pltpu.SemaphoreType.DMA((7,)),
            pltpu.SemaphoreType.DMA((3, RLOC)),
            pltpu.SemaphoreType.DMA((4,)),
        ]
        return pl.pallas_call(
            block_kernel,
            name='evoformer_block',
            out_shape=(jax.ShapeDtypeStruct(m_blk.shape, BF16), jax.ShapeDtypeStruct(z_blk.shape, BF16)),
            in_specs=[vmem] * 17,
            out_specs=(vmem, vmem),
            scratch_shapes=scratch,
            compiler_params=pltpu.CompilerParams(collective_id=0, has_side_effects=True,
                                                 vmem_limit_bytes=56 * 1024 * 1024),
        )(m_blk, z_blk, msa_mask.T, res_mask.reshape(1, RES), w_row_in, w_row_bias.T, w_row_out, w_col_in, w_col_out,
          w_opm_in.T, w_opm_out, w_start_in, w_start_bias.T, w_start_out, w_end_in, w_end_bias.T, w_end_out)

    return jax.shard_map(per_device, mesh=mesh, in_specs=in_specs, out_specs=(rows, rows), check_vma=False)
```

```python
import functools

import jax
import jax.numpy as jnp
from jax import lax
from jax.experimental import pallas as pl
from jax.experimental.pallas import tpu as pltpu
from jax.sharding import PartitionSpec as P

BF16 = jnp.bfloat16
F32 = jnp.float32
MESH = pl.DeviceIdType.MESH
NDEV = 8
SEQ, RES, CM, CZ = 256, 96, 256, 128
SLOC, RLOC = SEQ // NDEV, RES // NDEV
HM, HT, HD, OPM = 8, 4, 32, 32
LANES = 128
MASKED = -1e9
SCALE = HD ** -0.5
LOG2E = 1.4426950408889634

ROWB, MF, MB, STB, ZF, ENB, ZB = 0, 1, 5, 6, 7, 8, 9
NSTAGE = 10
CHUNK = 8
NCHUNK = SLOC // CHUNK
CROWS = NDEV * CHUNK
LAG = 2
MB_EARLY = 6


def dot(a, b):
    return jnp.dot(a, b, preferred_element_type=F32)


def dot_t(a, b):
    return lax.dot_general(a, b, (((1,), (1,)), ((), ())), preferred_element_type=F32)


def iota(shape, dim):
    return lax.broadcasted_iota(jnp.int32, shape, dim)


def layer_norm(x):
    values = x.astype(F32)
    centred = values - jnp.mean(values, axis=-1, keepdims=True)
    variance = jnp.mean(centred * centred, axis=-1, keepdims=True)
    return (centred * lax.rsqrt(variance + 1e-5)).astype(BF16)


def add_residual(state, update):
    return (state.astype(F32) + update).astype(BF16)


def head_masks():
    lane = iota((16, LANES), 1)
    return [jnp.where((lane >= h * HD) & (lane < (h + 1) * HD), 1.0, 0.0).astype(BF16) for h in range(LANES // HD)]


def only_head(x, mask):
    return x * jnp.concatenate([mask] * (x.shape[0] // 16), axis=0)


def dot_tl(a, b):
    return lax.dot_general(a, b, (((0,), (0,)), ((), ())), preferred_element_type=F32)


def softmax_keys(logits, exponential=jnp.exp):
    weights = exponential(logits - jnp.max(logits, axis=0, keepdims=True))
    return (weights * (1.0 / jnp.sum(weights, axis=0, keepdims=True))).astype(BF16)


def pipeline(items, first, middle, last, finish):
    opened, ready = {0: first(items[0])}, {}
    for n in range(len(items) + 2):
        if n + 1 < len(items):
            opened[n + 1] = first(items[n + 1])
        if n < len(items):
            ready[n] = middle(items[n], opened.pop(n))
        if 1 <= n <= len(items):
            last(items[n - 1], ready.pop(n - 1))
        if n >= 2:
            finish(items[n - 2])


def attend_biased(rows, tiles, q_of, k_of, vg_of, bias_ref, keep_of, w_out, store):
    masks = head_masks()
    each = len(masks)
    offsets = {u: (keep_of(u) - 1.0) * -MASKED for u in rows}
    vgs = {}
    mixed = {u: [] for u in rows}

    def first(item):
        u, t = item
        if t == 0:
            vgs[u] = vg_of(u)
        k = k_of(u, t)
        return dot_t(jnp.concatenate([only_head(k, mask) for mask in masks], axis=0), q_of(u, t))

    def middle(item, scores):
        u, t = item
        return [softmax_keys((scores[n * RES:(n + 1) * RES] * SCALE + bias_ref[each * t + n]) * keep_of(u) + offsets[u])
                for n in range(each)]

    def last(item, probs):
        u, t = item
        for n in range(each):
            h = each * t + n
            padded = jnp.concatenate([probs[n], jnp.zeros((LANES - RES, LANES), BF16)], axis=0)
            mixed[u].append(dot(vgs[u][h * HD:(h + 1) * HD], padded))

    def finish(item):
        u, t = item
        if t == tiles - 1:
            gates = jax.nn.sigmoid(vgs[u][tiles * LANES:].astype(F32))
            store(u, dot_tl((jnp.concatenate(mixed[u], axis=0) * gates).astype(BF16), w_out))

    pipeline([(u, t) for u in rows for t in range(tiles)], first, middle, last, finish)


def attend_column(residues, q_of, k_of, vg_of, keep_of, w_out, store):
    masks = head_masks()
    each = len(masks)
    keeps, vgs = {}, {}
    mixed = {u: [] for u in residues}

    def first(item):
        u, h = item
        if h == 0:
            keeps[u] = keep_of(u)
            vgs[u] = vg_of(u)
        return dot_t(only_head(k_of(u, h // each), masks[h % each]), q_of(u, h // each))

    def middle(item, scores):
        keep = keeps[item[0]]
        return softmax_keys(scores * (keep * (SCALE * LOG2E)) + (keep - 1.0) * (-MASKED * LOG2E), jnp.exp2)

    def last(item, probs):
        u, h = item
        mixed[u].append(dot(vgs[u][h * HD:(h + 1) * HD], probs))

    def finish(item):
        u, h = item
        if h == HM - 1:
            gates = jax.nn.sigmoid(vgs[u][CM:].astype(F32))
            store(u, dot_tl((jnp.concatenate(mixed[u], axis=0) * gates).astype(BF16), w_out))

    pipeline([(u, h) for u in residues for h in range(HM)], first, middle, last, finish)


def block_kernel(m_ref, z_ref, mask_ref, res_ref, w_row_in, w_row_bias, w_row_out, w_col_in, w_col_out,
                 w_opm_in, w_opm_out, w_start_in, w_start_bias, w_start_out, w_end_in, w_end_bias, w_end_out,
                 m_out, z_out,
                 perm, perm_out, perm_in, comp, hperm, keep_row, mask_t, mask_s, norm, res_keep, wbt, bcol, bias,
                 rowb_recv, stb_recv, enb_recv, row_vg, col_vg, tri_vg, yrow, rowqk, triqk, m1, msend, mrecv, mcols, mdone, mback,
                 ycol, colqk,
                 left, crecv, cbig, outer, w2, w2t, ynorm, z1, zs, zr, z2, z3, zs2, zr2,
                 send_sem, recv_sem, local_sem, c_send, c_recv, c_pair):
    data = lax.axis_index('data')
    me = lax.axis_index('chip') * 4 + lax.axis_index('dap')
    core, chip_x, chip_y = lax.rem(me, 2), lax.rem(me // 2, 2), me // 4
    partner = me + 1 - 2 * core
    to_x, to_y = 2 - 4 * chip_x, 4 - 8 * chip_y
    twins = (me + to_x + to_y, me + to_x, me + to_y)

    def device(d):
        return (data, d // 4, lax.rem(d, 4))

    def peer(r):
        return lax.rem(me + r, NDEV)

    def source(r):
        return lax.rem(me + NDEV - r, NDEV)

    def remote(src, dst, send, recv, d):
        return pltpu.make_async_remote_copy(src_ref=src, dst_ref=dst, send_sem=send, recv_sem=recv,
                                            device_id=device(d), device_id_type=MESH)

    def start_all(stage, src_of, dst_of):
        for r in range(1, NDEV):
            d = peer(r)
            remote(src_of(d), dst_of(me), send_sem.at[stage, r], recv_sem.at[stage, r], d).start()

    def wait_recv(stage, dst_of):
        for r in range(1, NDEV):
            dst = dst_of(source(r))
            remote(dst, dst, send_sem.at[stage, r], recv_sem.at[stage, r], peer(r)).wait_recv()

    def wait_send(stage, src_of):
        for r in range(1, NDEV):
            src = src_of(peer(r))
            remote(src, src, send_sem.at[stage, r], recv_sem.at[stage, r], peer(r)).wait_send()

    barrier = pltpu.get_barrier_semaphore()
    for r in range(1, NDEV):
        pl.semaphore_signal(barrier, inc=1, device_id=device(peer(r)), device_id_type=MESH)

    r0, c0 = iota((256, 256), 0), iota((256, 256), 1)
    perm[...] = jnp.where(((r0 >> 4) == (c0 & 15)) & ((r0 & 15) == (c0 >> 4)), 1.0, 0.0).astype(BF16)
    perm_out[...] = jnp.where(((r0 >> 3) == (c0 & 31)) & ((r0 & 7) == (c0 >> 5)), 1.0, 0.0).astype(BF16)
    perm_in[...] = jnp.where(((r0 >> 5) == (c0 & 7)) & ((r0 & 31) == (c0 >> 3)), 1.0, 0.0).astype(BF16)
    r1, c1 = iota((RES, LANES), 0), iota((RES, LANES), 1)
    comp[...] = jnp.where(((c1 & 15) < RLOC) & (r1 == (c1 >> 4) * RLOC + (c1 & 15)), 1.0, 0.0).astype(BF16)
    r2, c2 = iota((LANES, LANES), 0), iota((LANES, LANES), 1)
    hperm[...] = jnp.where(((r2 >> 4) == (c2 & 7)) & ((r2 & 15) == (c2 >> 3)), 1.0, 0.0).astype(BF16)
    eye = jnp.where(r2 == c2, 1.0, 0.0).astype(BF16)
    bcol[...] = jnp.zeros_like(bcol)
    wbt[...] = jnp.zeros_like(wbt)
    for n, w in enumerate((w_row_bias, w_start_bias, w_end_bias)):
        wbt[n, 0:w.shape[0], :] = w[...].astype(F32)

    def send_bias(recv, which, heads, stage):
        weights = wbt[which].astype(BF16)

        @pl.loop(0, RLOC)
        def _(i):
            bcol[i] = dot_t(weights, ynorm[i])

        mine = dot(hperm[0:heads * 16, :], bcol[...].reshape(LANES, LANES).astype(BF16)).astype(BF16)
        recv[me] = mine.reshape(heads, 16, LANES)
        start_all(stage, lambda d: recv.at[me], lambda s: recv.at[s])

    def bias_rows(recv):
        return lambda s: recv.at[s]

    def take_bias(recv, heads, stage):
        wait_recv(stage, bias_rows(recv))
        for h in range(heads):
            rows = dot(comp[...], recv[:, h].reshape(LANES, LANES)).astype(BF16)
            bias[h] = dot_t(eye, jnp.concatenate([rows, jnp.zeros((LANES - RES, LANES), BF16)], axis=0))[0:RES]

    ynorm[:, RES:, :] = jnp.zeros((RLOC, LANES - RES, CZ), BF16)

    @pl.loop(0, RLOC)
    def _(i):
        ynorm[i, 0:RES, :] = layer_norm(z_ref[i])

    pl.semaphore_wait(barrier, NDEV - 1)
    send_bias(rowb_recv, 0, HM, ROWB)

    res_keep[...] = dot((eye[0:RES, 0:RES].astype(F32) * res_ref[...].astype(F32)).astype(BF16),
                        jnp.ones((RES, LANES), BF16))
    seq_order = jnp.where(r0 == ((c0 >> 3) & 7) * SLOC + (c0 >> 6) * CHUNK + (c0 & 7), 1.0, 0.0).astype(BF16)
    seq_rows = jnp.where(c0 == ((r0 >> 3) & 7) * SLOC + (r0 >> 6) * CHUNK + (r0 & 7), 1.0, 0.0).astype(BF16)
    mt = mask_ref[...].astype(F32).astype(BF16)
    mask_t[...] = dot(mt, seq_order)
    mask_s[...] = dot_t(seq_rows, mt).astype(BF16)

    @pl.loop(0, SLOC)
    def _(i):
        pick = jnp.where(iota((SEQ, LANES), 0) == me * SLOC + i, 1.0, 0.0).astype(BF16)
        keep_row[i] = dot(mask_ref[...].astype(F32).astype(BF16), pick)

    row_vg[...] = jnp.transpose(w_row_in[:, 2 * CM:])
    col_vg[...] = jnp.transpose(w_col_in[:, 2 * CM:])
    tri_vg[0] = jnp.transpose(w_start_in[:, 2 * CZ:])
    tri_vg[1] = jnp.transpose(w_end_in[:, 2 * CZ:])
    norm[...] = jnp.zeros_like(norm)
    norm[0:RES, 0:RES] = dot_t(mt, mt)
    w_full = w_opm_out[...].reshape(OPM, OPM, CZ)
    for a in range(2):
        for c in range(2):
            blk = w_full[16 * a:16 * a + 16, 16 * c:16 * c + 16, :].reshape(256, CZ)
            w2[16 * c:16 * c + 16, 16 * a:16 * a + 16, :] = dot(perm[...], blk).astype(BF16).reshape(16, 16, CZ)
    w2t[...] = dot_t(eye, w2[...].reshape(OPM * OPM, CZ)).astype(BF16)
    cbig[:, RES:, :] = jnp.zeros((OPM, LANES - RES, SEQ), BF16)
    yrow[:, RES:, :] = jnp.zeros((4, LANES - RES, CM), BF16)
    rowqk[:, :, RES:, :] = jnp.zeros((4, 4, LANES - RES, LANES), BF16)
    triqk[:, :, RES:, :] = jnp.zeros((2, RLOC, LANES - RES, LANES), BF16)
    z1[RLOC:, :, :] = jnp.zeros((16 - RLOC, RES, CZ), BF16)
    z3[RLOC:, :, :] = jnp.zeros((16 - RLOC, RES, CZ), BF16)

    take_bias(rowb_recv, HM, ROWB)

    def m_src(q):
        return lambda d: msend.at[q, pl.ds(d * RLOC, RLOC)]

    def m_dst(q):
        return lambda s: mrecv.at[q, s]

    def local_copy(src, dst, n):
        return pltpu.make_async_copy(src, dst, local_sem.at[n])

    def row_chunk(q):
        @pl.loop(0, CHUNK // 4)
        def _(blk):
            s0 = q * CHUNK + blk * 4
            x = m_ref[pl.ds(s0, 4)].reshape(4 * RES, CM)
            y = layer_norm(x)
            yrow[:, 0:RES, :] = y.reshape(4, RES, CM)
            qk = dot(y, w_row_in[:, 0:2 * CM]).astype(BF16)
            for t in range(4):
                rowqk[t, :, 0:RES, :] = qk[:, t * LANES:(t + 1) * LANES].reshape(4, RES, LANES)

            def store(u, update):
                m1[s0 + u] = add_residual(m_ref[s0 + u], update[0:RES])
            attend_biased(range(4), 2, lambda u, t: rowqk[t, u], lambda u, t: rowqk[2 + t, u, 0:RES],
                          lambda u: dot_t(row_vg[...], yrow[u]).astype(BF16), bias,
                          lambda u: keep_row[s0 + u], w_row_out[...], store)

        for j in range(RES // 32):
            blk = m1[CHUNK * q:CHUNK * q + CHUNK, 32 * j:32 * j + 32, :].reshape(256, CM)
            msend[q, 32 * j:32 * j + 32] = dot(perm_out[...], blk).reshape(32, CHUNK, CM).astype(BF16)
        start_all(MF + q, m_src(q), m_dst(q))
        local_copy(m_src(q)(me), m_dst(q)(me), q).start()

    def column_projection(q):
        local_copy(m_src(q)(me), m_dst(q)(me), q).wait()
        wait_recv(MF + q, m_dst(q))

        @pl.loop(0, RLOC // 4)
        def _(blk):
            x = jnp.concatenate([mrecv[q, :, blk * 4 + u].astype(F32).reshape(CROWS, CM) for u in range(4)], axis=0)
            for u in range(4):
                mcols[q, blk * 4 + u] = x[u * CROWS:(u + 1) * CROWS].astype(BF16)
            y = layer_norm(x)
            ycol[pl.ds(blk * 4, 4), CROWS * q:CROWS * q + CROWS, :] = y.reshape(4, CROWS, CM)
            qk = dot(y, w_col_in[:, 0:2 * CM]).astype(BF16)
            for t in range(4):
                colqk[t, pl.ds(blk * 4, 4), CROWS * q:CROWS * q + CROWS, :] = (
                    qk[:, t * LANES:(t + 1) * LANES].reshape(4, CROWS, LANES))

    row_chunk(0)
    row_chunk(1)
    row_chunk(2)
    column_projection(0)
    row_chunk(3)
    column_projection(1)
    column_projection(2)
    column_projection(3)

    def mb_start(j):
        start_all(MB, lambda d: mdone.at[d, j], lambda s: mback.at[s * RLOC + j])

    def relay(j):
        for t, twin in enumerate(twins):
            row = crecv.at[twin * RLOC + j]
            remote(row, row, c_send.at[t], c_recv.at[t, j], twin).wait_recv()
            remote(row, row, c_send.at[3 + t], c_pair.at[t], partner).start()

    @pl.loop(0, RLOC // 2)
    def _(pair):
        def keep_of(u):
            pick = jnp.where(iota((RES, LANES), 0) == me * RLOC + pair * 2 + u, 1.0, 0.0).astype(BF16)
            keep = dot(mask_s[...], pick)
            return jnp.concatenate([keep, keep], axis=1)

        def store(u, update):
            j = pair * 2 + u
            mask_row = mask_t[pl.ds(me * RLOC + j, 1), :]
            x = add_residual(mcols[:, j].reshape(SEQ, CM), update)
            both = dot_t(w_opm_in[...], layer_norm(x)).astype(BF16).astype(F32) * mask_row
            left[j] = both[0:OPM].astype(BF16)
            crecv[me * RLOC + j] = both[OPM:].astype(BF16)
            done = x.astype(F32).reshape(NCHUNK, NDEV, CHUNK, CM).astype(BF16)
            for d in range(NDEV):
                mdone[d, j] = done[:, d]

        attend_column(range(2), lambda u, t: colqk[t, pair * 2 + u], lambda u, t: colqk[2 + t, pair * 2 + u],
                      lambda u: dot_t(col_vg[...], ycol[pair * 2 + u]).astype(BF16), keep_of, w_col_out[...], store)
        for u in range(2):
            j = pair * 2 + u
            row = crecv.at[me * RLOC + j]
            for t, twin in enumerate(twins):
                remote(row, row, c_send.at[t], c_recv.at[t, j], twin).start()
            remote(row, row, c_send.at[6], c_pair.at[3], partner).start()

        @pl.when(pair >= 1)
        def _():
            for u in range(2):
                relay(pair * 2 - 2 + u)

        @pl.when(pair < MB_EARLY // 2)
        def _():
            for u in range(2):
                mb_start(pair * 2 + u)

    for j in range(RLOC - LAG, RLOC):
        relay(j)
    mback[pl.ds(me * RLOC, RLOC)] = mdone[me]

    def c_rows(s):
        return crecv.at[pl.ds(s * RLOC, RLOC)]

    for t, first in enumerate(twins + (me,)):
        rows = c_rows(first + 1 - 2 * core)
        remote(rows, rows, c_send.at[3 + t], c_pair.at[t], partner).wait_recv()
    for j in range(MB_EARLY, MB_EARLY + 3):
        mb_start(j)
    for c in range(2):
        @pl.loop(0, RES // 16)
        def _(j):
            j0 = pl.multiple_of(j * 16, 16)
            blk = crecv[pl.ds(j0, 16), 16 * c:16 * c + 16, :].reshape(256, SEQ)
            cbig[16 * c:16 * c + 16, pl.ds(j0, 16), :] = dot(perm[...], blk).astype(BF16).reshape(16, 16, SEQ)

    @pl.loop(0, OPM // 2)
    def _(c):
        prod = dot_t(left[...].reshape(RLOC * OPM, SEQ), cbig[pl.ds(2 * c, 2)].reshape(256, SEQ)).astype(BF16)
        for u in range(2):
            outer[:, 2 * c + u] = prod[:, u * LANES:(u + 1) * LANES].reshape(RLOC, OPM, LANES)

    @pl.loop(0, RLOC)
    def _(i):
        update = dot(w2t[...], outer[i].reshape(OPM * OPM, LANES))
        update = update / (1e-3 + norm[pl.ds(me * RLOC + i, 1), :])
        z1[i] = add_residual(z_ref[i], jnp.transpose(update)[0:RES])

    def triangle(state, result, w_in, which, w_out, recv, stage, late):
        @pl.loop(0, RLOC)
        def _(i):
            ynorm[i, 0:RES, :] = layer_norm(state[i])
        send_bias(recv, which, HT, stage)

        @pl.loop(0, RLOC // 4)
        def _(blk):
            y = ynorm[pl.ds(blk * 4, 4), 0:RES, :].reshape(4 * RES, CZ)
            qk = dot(y, w_in[:, 0:2 * CZ]).astype(BF16)
            for t in range(2):
                triqk[t, pl.ds(blk * 4, 4), 0:RES, :] = qk[:, t * LANES:(t + 1) * LANES].reshape(4, RES, LANES)
        take_bias(recv, HT, stage)
        for j in late:
            mb_start(j)

        @pl.loop(0, RLOC // 4)
        def _(blk):
            def store(u, update):
                result[blk * 4 + u] = add_residual(state[blk * 4 + u], update[0:RES])
            attend_biased(range(4), 1, lambda u, t: triqk[0, blk * 4 + u], lambda u, t: triqk[1, blk * 4 + u, 0:RES],
                          lambda u: dot_t(tri_vg[which - 1], ynorm[blk * 4 + u]).astype(BF16), bias,
                          lambda u: res_keep[...], w_out[...], store)

    def z_src(buf):
        return lambda d: buf.at[pl.ds(d * RLOC, RLOC)]

    def z_dst(buf):
        return lambda s: buf.at[s]

    def exchange(state, send, recv, result, stage, n):
        for j in range(RES // 16):
            blk = state[:, 16 * j:16 * j + 16, :].reshape(256, CZ)
            send[16 * j:16 * j + 16] = dot(perm[...], blk).astype(BF16).reshape(16, 16, CZ)
        start_all(stage, z_src(send), z_dst(recv))
        own = local_copy(z_src(send)(me), z_dst(recv)(me), n)
        own.start()
        own.wait()
        wait_recv(stage, z_dst(recv))

        @pl.loop(0, RLOC)
        def _(i):
            result[i] = dot(comp[...], recv[:, i].reshape(LANES, CZ)).astype(BF16)

    triangle(z1, z1, w_start_in, 1, w_start_out, stb_recv, STB, (MB_EARLY + 3, MB_EARLY + 4))
    exchange(z1, zs, zr, z2, ZF, NCHUNK)
    triangle(z2, z3, w_end_in, 2, w_end_out, enb_recv, ENB, (MB_EARLY + 5,))
    exchange(z3, zs2, zr2, z_out, ZB, NCHUNK + 1)

    def mb_dst(s):
        return mback.at[pl.ds(s * RLOC, RLOC)]
    wait_recv(MB, mb_dst)
    for q in range(NCHUNK):
        @pl.loop(0, RES // 32)
        def _(j):
            blk = mback[pl.ds(j * 32, 32), q].astype(F32).reshape(256, CM).astype(BF16)
            rows = dot(perm_in[...], blk).astype(BF16).reshape(CHUNK, 32, CM)
            m_out[CHUNK * q:CHUNK * q + CHUNK, pl.ds(pl.multiple_of(j * 32, 32), 32), :] = rows

    wait_send(ROWB, lambda d: bias_rows(rowb_recv)(me))
    for q in range(NCHUNK):
        wait_send(MF + q, m_src(q))
    wait_send(MB, lambda d: mdone.at[d])
    for t in range(7):
        rows = c_rows(me if t in (0, 1, 2, 6) else twins[t - 3])
        remote(rows, rows, c_send.at[t], c_pair.at[0], partner).wait_send()
    wait_send(STB, lambda d: bias_rows(stb_recv)(me))
    wait_send(ZF, z_src(zs))
    wait_send(ENB, lambda d: bias_rows(enb_recv)(me))
    wait_send(ZB, z_src(zs2))


def solution(mesh):
    rows = P(('data', 'chip', 'dap'))
    in_specs = (rows, rows, P('data'), P('data')) + (P(),) * 13
    vmem = pl.BlockSpec(memory_space=pltpu.VMEM)

    def per_device(m_blk, z_blk, msa_mask, res_mask, w_row_in, w_row_bias, w_row_out, w_col_in, w_col_out,
                   w_opm_in, w_opm_out, w_start_in, w_start_bias, w_start_out, w_end_in, w_end_bias, w_end_out):
        scratch = [
            pltpu.VMEM((256, 256), BF16),
            pltpu.VMEM((256, 256), BF16),
            pltpu.VMEM((256, 256), BF16),
            pltpu.VMEM((RES, LANES), BF16),
            pltpu.VMEM((LANES, LANES), BF16),
            pltpu.VMEM((SLOC, RES, LANES), F32),
            pltpu.VMEM((RES, SEQ), F32),
            pltpu.VMEM((SEQ, RES), BF16),
            pltpu.VMEM((LANES, LANES), F32),
            pltpu.VMEM((RES, LANES), F32),
            pltpu.VMEM((3, 8, CZ), F32),
            pltpu.VMEM((16, 8, LANES), F32),
            pltpu.VMEM((HM, RES, LANES), F32),
            pltpu.VMEM((NDEV, HM, 16, LANES), BF16),
            pltpu.VMEM((NDEV, HT, 16, LANES), BF16),
            pltpu.VMEM((NDEV, HT, 16, LANES), BF16),
            pltpu.VMEM((2 * CM, CM), BF16),
            pltpu.VMEM((2 * CM, CM), BF16),
            pltpu.VMEM((2, 2 * CZ, CZ), BF16),
            pltpu.VMEM((4, LANES, CM), BF16),
            pltpu.VMEM((4, 4, LANES, LANES), BF16),
            pltpu.VMEM((2, RLOC, LANES, LANES), BF16),
            pltpu.VMEM((SLOC, RES, CM), BF16),
            pltpu.VMEM((NCHUNK, RES, CHUNK, CM), BF16),
            pltpu.VMEM((NCHUNK, NDEV, RLOC, CHUNK, CM), BF16),
            pltpu.VMEM((NCHUNK, RLOC, CROWS, CM), BF16),
            pltpu.VMEM((NDEV, RLOC, NCHUNK, CHUNK, CM), BF16),
            pltpu.VMEM((RES, NCHUNK, CHUNK, CM), BF16),
            pltpu.VMEM((RLOC, SEQ, CM), BF16),
            pltpu.VMEM((4, RLOC, SEQ, LANES), BF16),
            pltpu.VMEM((RLOC, OPM, SEQ), BF16),
            pltpu.VMEM((RES, OPM, SEQ), BF16),
            pltpu.VMEM((OPM, LANES, SEQ), BF16),
            pltpu.VMEM((RLOC, OPM, OPM, LANES), BF16),
            pltpu.VMEM((OPM, OPM, CZ), BF16),
            pltpu.VMEM((CZ, OPM * OPM), BF16),
            pltpu.VMEM((RLOC, LANES, CZ), BF16),
            pltpu.VMEM((16, RES, CZ), BF16),
            pltpu.VMEM((RES, 16, CZ), BF16),
            pltpu.VMEM((NDEV, RLOC, 16, CZ), BF16),
            pltpu.VMEM((RLOC, RES, CZ), BF16),
            pltpu.VMEM((16, RES, CZ), BF16),
            pltpu.VMEM((RES, 16, CZ), BF16),
            pltpu.VMEM((NDEV, RLOC, 16, CZ), BF16),
            pltpu.SemaphoreType.DMA((NSTAGE, NDEV)),
            pltpu.SemaphoreType.DMA((NSTAGE, NDEV)),
            pltpu.SemaphoreType.DMA((NCHUNK + 2,)),
            pltpu.SemaphoreType.DMA((7,)),
            pltpu.SemaphoreType.DMA((3, RLOC)),
            pltpu.SemaphoreType.DMA((4,)),
        ]
        return pl.pallas_call(
            block_kernel,
            name='evoformer_block',
            out_shape=(jax.ShapeDtypeStruct(m_blk.shape, BF16), jax.ShapeDtypeStruct(z_blk.shape, BF16)),
            in_specs=[vmem] * 17,
            out_specs=(vmem, vmem),
            scratch_shapes=scratch,
            compiler_params=pltpu.CompilerParams(collective_id=0, has_side_effects=True,
                                                 vmem_limit_bytes=56 * 1024 * 1024),
        )(m_blk, z_blk, msa_mask.T, res_mask.reshape(1, RES), w_row_in, w_row_bias.T, w_row_out, w_col_in, w_col_out,
          w_opm_in.T, w_opm_out, w_start_in, w_start_bias.T, w_start_out, w_end_in, w_end_bias.T, w_end_out)

    return jax.shard_map(per_device, mesh=mesh, in_specs=in_specs, out_specs=(rows, rows), check_vma=False)
```

```python
import functools

import jax
import jax.numpy as jnp
from jax import lax
from jax.experimental import pallas as pl
from jax.experimental.pallas import tpu as pltpu
from jax.sharding import PartitionSpec as P

BF16 = jnp.bfloat16
F32 = jnp.float32
MESH = pl.DeviceIdType.MESH
NDEV = 8
SEQ, RES, CM, CZ = 256, 96, 256, 128
SLOC, RLOC = SEQ // NDEV, RES // NDEV
HM, HT, HD, OPM = 8, 4, 32, 32
LANES = 128
MASKED = -1e9
SCALE = HD ** -0.5
LOG2E = 1.4426950408889634

ROWB, MF, MB, STB, ZF, ENB, ZB = 0, 1, 5, 6, 7, 9, 10
NSTAGE = 12
ZGROUP = RLOC // 2
CHUNK = 8
NCHUNK = SLOC // CHUNK
CROWS = NDEV * CHUNK
LAG = 2
MB_EARLY = 8


def dot(a, b):
    return jnp.dot(a, b, preferred_element_type=F32)


def dot_t(a, b):
    return lax.dot_general(a, b, (((1,), (1,)), ((), ())), preferred_element_type=F32)


def iota(shape, dim):
    return lax.broadcasted_iota(jnp.int32, shape, dim)


def layer_norm(x):
    values = x.astype(F32)
    centred = values - jnp.mean(values, axis=-1, keepdims=True)
    variance = jnp.mean(centred * centred, axis=-1, keepdims=True)
    return (centred * lax.rsqrt(variance + 1e-5)).astype(BF16)


def add_residual(state, update):
    return (state.astype(F32) + update).astype(BF16)


def head_masks():
    lane = iota((16, LANES), 1)
    return [jnp.where((lane >= h * HD) & (lane < (h + 1) * HD), 1.0, 0.0).astype(BF16) for h in range(LANES // HD)]


def only_head(x, mask):
    return x * jnp.concatenate([mask] * (x.shape[0] // 16), axis=0)


def dot_tl(a, b):
    return lax.dot_general(a, b, (((0,), (0,)), ((), ())), preferred_element_type=F32)


def softmax_keys(logits, exponential=jnp.exp):
    weights = exponential(logits - jnp.max(logits, axis=0, keepdims=True))
    return (weights * (1.0 / jnp.sum(weights, axis=0, keepdims=True))).astype(BF16)


def pipeline(items, first, middle, last, finish):
    opened, ready = {0: first(items[0])}, {}
    for n in range(len(items) + 2):
        if n + 1 < len(items):
            opened[n + 1] = first(items[n + 1])
        if n < len(items):
            ready[n] = middle(items[n], opened.pop(n))
        if 1 <= n <= len(items):
            last(items[n - 1], ready.pop(n - 1))
        if n >= 2:
            finish(items[n - 2])


def attend_biased(rows, tiles, q_of, k_of, vg_of, bias_ref, keep_of, w_out, store):
    masks = head_masks()
    each = len(masks)
    offsets = {u: (keep_of(u) - 1.0) * -MASKED for u in rows}
    vgs = {}
    mixed = {u: [] for u in rows}

    def first(item):
        u, t = item
        if t == 0:
            vgs[u] = vg_of(u)
        k = k_of(u, t)
        return dot_t(jnp.concatenate([only_head(k, mask) for mask in masks], axis=0), q_of(u, t))

    def middle(item, scores):
        u, t = item
        return [softmax_keys((scores[n * RES:(n + 1) * RES] * SCALE + bias_ref[each * t + n]) * keep_of(u) + offsets[u])
                for n in range(each)]

    def last(item, probs):
        u, t = item
        for n in range(each):
            h = each * t + n
            padded = jnp.concatenate([probs[n], jnp.zeros((LANES - RES, LANES), BF16)], axis=0)
            mixed[u].append(dot(vgs[u][h * HD:(h + 1) * HD], padded))

    def finish(item):
        u, t = item
        if t == tiles - 1:
            gates = jax.nn.sigmoid(vgs[u][tiles * LANES:].astype(F32))
            store(u, dot_tl((jnp.concatenate(mixed[u], axis=0) * gates).astype(BF16), w_out))

    pipeline([(u, t) for u in rows for t in range(tiles)], first, middle, last, finish)


def attend_column(residues, q_of, k_of, vg_of, keep_of, w_out, store):
    masks = head_masks()
    each = len(masks)
    keeps, vgs = {}, {}
    mixed = {u: [] for u in residues}

    def first(item):
        u, h = item
        if h == 0:
            keeps[u] = keep_of(u)
            vgs[u] = vg_of(u)
        return dot_t(only_head(k_of(u, h // each), masks[h % each]), q_of(u, h // each))

    def middle(item, scores):
        keep = keeps[item[0]]
        return softmax_keys(scores * (keep * (SCALE * LOG2E)) + (keep - 1.0) * (-MASKED * LOG2E), jnp.exp2)

    def last(item, probs):
        u, h = item
        mixed[u].append(dot(vgs[u][h * HD:(h + 1) * HD], probs))

    def finish(item):
        u, h = item
        if h == HM - 1:
            gates = jax.nn.sigmoid(vgs[u][CM:].astype(F32))
            store(u, dot_tl((jnp.concatenate(mixed[u], axis=0) * gates).astype(BF16), w_out))

    pipeline([(u, h) for u in residues for h in range(HM)], first, middle, last, finish)


def block_kernel(m_any, z_ref, mask_ref, res_ref, row_in_any, w_row_bias, row_out_any, col_in_any, col_out_any,
                 w_opm_in, opm_out_any, start_in_any, w_start_bias, start_out_any, end_in_any, w_end_bias, end_out_any,
                 mback, z_out,
                 m_ref, w_row_in, w_row_out, w_col_in, w_col_out, w_opm_out, w_start_in, w_start_out, w_end_in, w_end_out,
                 perm, perm_out, comp, compz, hperm, keep_row, mask_t, mask_s, norm, res_keep, wbt, bcol, bias,
                 rowb_recv, stb_recv, enb_recv, row_vg, col_vg, tri_vg, yrow, rowqk, triqk, m1, msend, mrecv, mcols, mdone,
                 ycol, colqk,
                 left, crecv, cbig, outer, w2, w2t, ynorm, z1, zs, zr, z2, z3, zs2, zr2,
                 send_sem, recv_sem, local_sem, load_sem, c_send, c_recv, c_pair):
    data = lax.axis_index('data')
    me = lax.axis_index('chip') * 4 + lax.axis_index('dap')
    core, chip_x, chip_y = lax.rem(me, 2), lax.rem(me // 2, 2), me // 4
    partner = me + 1 - 2 * core
    to_x, to_y = 2 - 4 * chip_x, 4 - 8 * chip_y
    twins = (me + to_x + to_y, me + to_x, me + to_y)

    def device(d):
        return (data, d // 4, lax.rem(d, 4))

    def peer(r):
        return lax.rem(me + r, NDEV)

    def source(r):
        return lax.rem(me + NDEV - r, NDEV)

    def remote(src, dst, send, recv, d):
        return pltpu.make_async_remote_copy(src_ref=src, dst_ref=dst, send_sem=send, recv_sem=recv,
                                            device_id=device(d), device_id_type=MESH)

    def start_all(stage, src_of, dst_of):
        for r in range(1, NDEV):
            d = peer(r)
            remote(src_of(d), dst_of(me), send_sem.at[stage, r], recv_sem.at[stage, r], d).start()

    def wait_recv(stage, dst_of):
        for r in range(1, NDEV):
            dst = dst_of(source(r))
            remote(dst, dst, send_sem.at[stage, r], recv_sem.at[stage, r], peer(r)).wait_recv()

    def wait_send(stage, src_of):
        for r in range(1, NDEV):
            src = src_of(peer(r))
            remote(src, src, send_sem.at[stage, r], recv_sem.at[stage, r], peer(r)).wait_send()

    barrier = pltpu.get_barrier_semaphore()
    for r in range(1, NDEV):
        pl.semaphore_signal(barrier, inc=1, device_id=device(peer(r)), device_id_type=MESH)

    loads = [pltpu.make_async_copy(src, dst, load_sem.at[n]) for n, (src, dst) in enumerate((
        (row_in_any, w_row_in), (m_any, m_ref), (row_out_any, w_row_out), (col_in_any, w_col_in), (opm_out_any, w_opm_out),
        (start_in_any, w_start_in), (end_in_any, w_end_in), (col_out_any, w_col_out), (start_out_any, w_start_out),
        (end_out_any, w_end_out)))]
    for load in loads:
        load.start()

    r0, c0 = iota((256, 256), 0), iota((256, 256), 1)
    perm[...] = jnp.where(((r0 >> 4) == (c0 & 15)) & ((r0 & 15) == (c0 >> 4)), 1.0, 0.0).astype(BF16)
    perm_out[...] = jnp.where(((r0 >> 3) == (c0 & 31)) & ((r0 & 7) == (c0 >> 5)), 1.0, 0.0).astype(BF16)
    r1, c1 = iota((RES, LANES), 0), iota((RES, LANES), 1)
    comp[...] = jnp.where(((c1 & 15) < RLOC) & (r1 == (c1 >> 4) * RLOC + (c1 & 15)), 1.0, 0.0).astype(BF16)
    compz[...] = jnp.where(((c1 & 7) < ZGROUP) & (r1 == ((c1 >> 3) & 7) * RLOC + (c1 >> 6) * ZGROUP + (c1 & 7)),
                           1.0, 0.0).astype(BF16)
    r2, c2 = iota((LANES, LANES), 0), iota((LANES, LANES), 1)
    hperm[...] = jnp.where(((r2 >> 4) == (c2 & 7)) & ((r2 & 15) == (c2 >> 3)), 1.0, 0.0).astype(BF16)
    eye = jnp.where(r2 == c2, 1.0, 0.0).astype(BF16)
    bcol[...] = jnp.zeros_like(bcol)
    wbt[...] = jnp.zeros_like(wbt)
    for n, w in enumerate((w_row_bias, w_start_bias, w_end_bias)):
        wbt[n, 0:w.shape[0], :] = w[...].astype(F32)

    def send_bias(recv, which, heads, stage):
        weights = wbt[which].astype(BF16)

        @pl.loop(0, RLOC)
        def _(i):
            bcol[i] = dot_t(weights, ynorm[i])

        mine = dot(hperm[0:heads * 16, :], bcol[...].reshape(LANES, LANES).astype(BF16)).astype(BF16)
        recv[me] = mine.reshape(heads, 16, LANES)
        start_all(stage, lambda d: recv.at[me], lambda s: recv.at[s])

    def bias_rows(recv):
        return lambda s: recv.at[s]

    def take_bias(recv, heads, stage):
        wait_recv(stage, bias_rows(recv))
        for h in range(heads):
            rows = dot(comp[...], recv[:, h].reshape(LANES, LANES)).astype(BF16)
            bias[h] = dot_t(eye, jnp.concatenate([rows, jnp.zeros((LANES - RES, LANES), BF16)], axis=0))[0:RES]

    ynorm[:, RES:, :] = jnp.zeros((RLOC, LANES - RES, CZ), BF16)

    @pl.loop(0, RLOC)
    def _(i):
        ynorm[i, 0:RES, :] = layer_norm(z_ref[i])

    pl.semaphore_wait(barrier, NDEV - 1)
    send_bias(rowb_recv, 0, HM, ROWB)

    res_keep[...] = dot((eye[0:RES, 0:RES].astype(F32) * res_ref[...].astype(F32)).astype(BF16),
                        jnp.ones((RES, LANES), BF16))
    seq_order = jnp.where(r0 == ((c0 >> 3) & 7) * SLOC + (c0 >> 6) * CHUNK + (c0 & 7), 1.0, 0.0).astype(BF16)
    seq_rows = jnp.where(c0 == ((r0 >> 3) & 7) * SLOC + (r0 >> 6) * CHUNK + (r0 & 7), 1.0, 0.0).astype(BF16)
    mt = mask_ref[...].astype(F32).astype(BF16)
    mask_t[...] = dot(mt, seq_order)
    mask_s[...] = dot_t(seq_rows, mt).astype(BF16)

    @pl.loop(0, SLOC)
    def _(i):
        pick = jnp.where(iota((SEQ, LANES), 0) == me * SLOC + i, 1.0, 0.0).astype(BF16)
        keep_row[i] = dot(mask_ref[...].astype(F32).astype(BF16), pick)

    for load in loads:
        load.wait()
    row_vg[...] = jnp.transpose(w_row_in[:, 2 * CM:])
    col_vg[...] = jnp.transpose(w_col_in[:, 2 * CM:])
    tri_vg[0] = jnp.transpose(w_start_in[:, 2 * CZ:])
    tri_vg[1] = jnp.transpose(w_end_in[:, 2 * CZ:])
    norm[...] = jnp.zeros_like(norm)
    norm[0:RES, 0:RES] = dot_t(mt, mt)
    w_full = w_opm_out[...].reshape(OPM, OPM, CZ)
    for a in range(2):
        for c in range(2):
            blk = w_full[16 * a:16 * a + 16, 16 * c:16 * c + 16, :].reshape(256, CZ)
            w2[16 * c:16 * c + 16, 16 * a:16 * a + 16, :] = dot(perm[...], blk).astype(BF16).reshape(16, 16, CZ)
    w2t[...] = dot_t(eye, w2[...].reshape(OPM * OPM, CZ)).astype(BF16)
    cbig[:, RES:, :] = jnp.zeros((OPM, LANES - RES, SEQ), BF16)
    yrow[:, RES:, :] = jnp.zeros((4, LANES - RES, CM), BF16)
    rowqk[:, :, RES:, :] = jnp.zeros((4, 4, LANES - RES, LANES), BF16)
    triqk[:, :, RES:, :] = jnp.zeros((2, RLOC, LANES - RES, LANES), BF16)
    z1[RLOC:, :, :] = jnp.zeros((16 - RLOC, RES, CZ), BF16)
    z3[...] = jnp.zeros_like(z3)

    take_bias(rowb_recv, HM, ROWB)

    def m_src(q):
        return lambda d: msend.at[q, pl.ds(d * RLOC, RLOC)]

    def m_dst(q):
        return lambda s: mrecv.at[q, s]

    def local_copy(src, dst, n):
        return pltpu.make_async_copy(src, dst, local_sem.at[n])

    def row_chunk(q):
        @pl.loop(0, CHUNK // 4)
        def _(blk):
            s0 = q * CHUNK + blk * 4
            x = m_ref[pl.ds(s0, 4)].reshape(4 * RES, CM)
            y = layer_norm(x)
            yrow[:, 0:RES, :] = y.reshape(4, RES, CM)
            qk = dot(y, w_row_in[:, 0:2 * CM]).astype(BF16)
            for t in range(4):
                rowqk[t, :, 0:RES, :] = qk[:, t * LANES:(t + 1) * LANES].reshape(4, RES, LANES)

            def store(u, update):
                m1[s0 + u] = add_residual(m_ref[s0 + u], update[0:RES])
            attend_biased(range(4), 2, lambda u, t: rowqk[t, u], lambda u, t: rowqk[2 + t, u, 0:RES],
                          lambda u: dot_t(row_vg[...], yrow[u]).astype(BF16), bias,
                          lambda u: keep_row[s0 + u], w_row_out[...], store)

        for j in range(RES // 32):
            blk = m1[CHUNK * q:CHUNK * q + CHUNK, 32 * j:32 * j + 32, :].reshape(256, CM)
            msend[q, 32 * j:32 * j + 32] = dot(perm_out[...], blk).reshape(32, CHUNK, CM).astype(BF16)
        start_all(MF + q, m_src(q), m_dst(q))
        local_copy(m_src(q)(me), m_dst(q)(me), q).start()

    def column_projection(q):
        local_copy(m_src(q)(me), m_dst(q)(me), q).wait()
        wait_recv(MF + q, m_dst(q))

        @pl.loop(0, RLOC // 4)
        def _(blk):
            x = jnp.concatenate([mrecv[q, :, blk * 4 + u].astype(F32).reshape(CROWS, CM) for u in range(4)], axis=0)
            for u in range(4):
                mcols[q, blk * 4 + u] = x[u * CROWS:(u + 1) * CROWS].astype(BF16)
            y = layer_norm(x)
            ycol[pl.ds(blk * 4, 4), CROWS * q:CROWS * q + CROWS, :] = y.reshape(4, CROWS, CM)
            qk = dot(y, w_col_in[:, 0:2 * CM]).astype(BF16)
            for t in range(4):
                colqk[t, pl.ds(blk * 4, 4), CROWS * q:CROWS * q + CROWS, :] = (
                    qk[:, t * LANES:(t + 1) * LANES].reshape(4, CROWS, LANES))

    row_chunk(0)
    row_chunk(1)
    row_chunk(2)
    column_projection(0)
    row_chunk(3)
    column_projection(1)
    column_projection(2)
    column_projection(3)

    def mb_start(j):
        start_all(MB, lambda d: mdone.at[d, j], lambda s: mback.at[s * RLOC + j])

    def relay(j):
        for t, twin in enumerate(twins):
            row = crecv.at[twin * RLOC + j]
            remote(row, row, c_send.at[t], c_recv.at[t, j], twin).wait_recv()
            remote(row, row, c_send.at[3 + t], c_pair.at[t], partner).start()

    @pl.loop(0, RLOC // 2)
    def _(pair):
        def keep_of(u):
            pick = jnp.where(iota((RES, LANES), 0) == me * RLOC + pair * 2 + u, 1.0, 0.0).astype(BF16)
            keep = dot(mask_s[...], pick)
            return jnp.concatenate([keep, keep], axis=1)

        def store(u, update):
            j = pair * 2 + u
            mask_row = mask_t[pl.ds(me * RLOC + j, 1), :]
            x = add_residual(mcols[:, j].reshape(SEQ, CM), update)
            both = dot_t(w_opm_in[...], layer_norm(x)).astype(BF16).astype(F32) * mask_row
            left[j] = both[0:OPM].astype(BF16)
            crecv[me * RLOC + j] = both[OPM:].astype(BF16)
            done = x.astype(F32).reshape(NCHUNK, NDEV, CHUNK, CM).astype(BF16)
            for d in range(NDEV):
                mdone[d, j] = done[:, d]

        attend_column(range(2), lambda u, t: colqk[t, pair * 2 + u], lambda u, t: colqk[2 + t, pair * 2 + u],
                      lambda u: dot_t(col_vg[...], ycol[pair * 2 + u]).astype(BF16), keep_of, w_col_out[...], store)
        for u in range(2):
            j = pair * 2 + u
            row = crecv.at[me * RLOC + j]
            for t, twin in enumerate(twins):
                remote(row, row, c_send.at[t], c_recv.at[t, j], twin).start()
            remote(row, row, c_send.at[6], c_pair.at[3], partner).start()

        @pl.when(pair >= 1)
        def _():
            for u in range(2):
                relay(pair * 2 - 2 + u)

        @pl.when(pair < MB_EARLY // 2)
        def _():
            for u in range(2):
                mb_start(pair * 2 + u)

    for j in range(RLOC - LAG, RLOC):
        relay(j)
    keep_mine = local_copy(mdone.at[me], mback.at[pl.ds(me * RLOC, RLOC)], NCHUNK + 4)
    keep_mine.start()

    def c_rows(s):
        return crecv.at[pl.ds(s * RLOC, RLOC)]

    for t, first in enumerate(twins + (me,)):
        rows = c_rows(first + 1 - 2 * core)
        remote(rows, rows, c_send.at[3 + t], c_pair.at[t], partner).wait_recv()
    for j in range(MB_EARLY, MB_EARLY + 3):
        mb_start(j)
    for c in range(2):
        @pl.loop(0, RES // 16)
        def _(j):
            j0 = pl.multiple_of(j * 16, 16)
            blk = crecv[pl.ds(j0, 16), 16 * c:16 * c + 16, :].reshape(256, SEQ)
            cbig[16 * c:16 * c + 16, pl.ds(j0, 16), :] = dot(perm[...], blk).astype(BF16).reshape(16, 16, SEQ)

    @pl.loop(0, OPM // 2)
    def _(c):
        prod = dot_t(left[...].reshape(RLOC * OPM, SEQ), cbig[pl.ds(2 * c, 2)].reshape(256, SEQ)).astype(BF16)
        for u in range(2):
            outer[:, 2 * c + u] = prod[:, u * LANES:(u + 1) * LANES].reshape(RLOC, OPM, LANES)

    @pl.loop(0, RLOC)
    def _(i):
        update = dot(w2t[...], outer[i].reshape(OPM * OPM, LANES))
        update = update / (1e-3 + norm[pl.ds(me * RLOC + i, 1), :])
        z1[i] = add_residual(z_ref[i], jnp.transpose(update)[0:RES])

    def z_src(buf, group):
        return lambda d: buf.at[group, pl.ds(d * RLOC, RLOC)]

    def z_dst(buf, group):
        return lambda s: buf.at[group, s]

    def triangle(state, result, w_in, which, w_out, recv, stage, late, send, zrecv, moved, zstage, slot):
        @pl.loop(0, RLOC)
        def _(i):
            ynorm[i, 0:RES, :] = layer_norm(state[i])
        send_bias(recv, which, HT, stage)

        @pl.loop(0, RLOC // 4)
        def _(blk):
            y = ynorm[pl.ds(blk * 4, 4), 0:RES, :].reshape(4 * RES, CZ)
            qk = dot(y, w_in[:, 0:2 * CZ]).astype(BF16)
            for t in range(2):
                triqk[t, pl.ds(blk * 4, 4), 0:RES, :] = qk[:, t * LANES:(t + 1) * LANES].reshape(4, RES, LANES)
        take_bias(recv, HT, stage)
        for j in late:
            mb_start(j)

        for group in range(2):
            first = group * ZGROUP

            def store(u, update):
                result[u] = add_residual(state[u], update[0:RES])
            attend_biased(range(first, first + ZGROUP), 1, lambda u, t: triqk[0, u], lambda u, t: triqk[1, u, 0:RES],
                          lambda u: dot_t(tri_vg[which - 1], ynorm[u]).astype(BF16), bias,
                          lambda u: res_keep[...], w_out[...], store)
            for j in range(RES // 32):
                blk = result[first:first + 8, 32 * j:32 * j + 32, :].reshape(256, CZ)
                send[group, 32 * j:32 * j + 32] = dot(perm_out[...], blk).reshape(32, 8, CZ).astype(BF16)
            start_all(zstage + group, z_src(send, group), z_dst(zrecv, group))
            local_copy(z_src(send, group)(me), z_dst(zrecv, group)(me), slot + group).start()

        for group in range(2):
            local_copy(z_src(send, group)(me), z_dst(zrecv, group)(me), slot + group).wait()
            wait_recv(zstage + group, z_dst(zrecv, group))

        @pl.loop(0, RLOC)
        def _(i):
            rows = zrecv[:, :, i].astype(F32).reshape(LANES, CZ).astype(BF16)
            moved[i] = dot(compz[...], rows).astype(BF16)

    triangle(z1, z1, w_start_in, 1, w_start_out, stb_recv, STB, (MB_EARLY + 3,), zs, zr, z2, ZF, NCHUNK)
    triangle(z2, z3, w_end_in, 2, w_end_out, enb_recv, ENB, (), zs2, zr2, z_out, ZB, NCHUNK + 2)

    wait_recv(MB, lambda s: mback.at[pl.ds(s * RLOC, RLOC)])
    keep_mine.wait()

    wait_send(ROWB, lambda d: bias_rows(rowb_recv)(me))
    for q in range(NCHUNK):
        wait_send(MF + q, m_src(q))
    wait_send(MB, lambda d: mdone.at[d])
    for t in range(7):
        rows = c_rows(me if t in (0, 1, 2, 6) else twins[t - 3])
        remote(rows, rows, c_send.at[t], c_pair.at[0], partner).wait_send()
    wait_send(STB, lambda d: bias_rows(stb_recv)(me))
    for group in range(2):
        wait_send(ZF + group, z_src(zs, group))
    wait_send(ENB, lambda d: bias_rows(enb_recv)(me))
    for group in range(2):
        wait_send(ZB + group, z_src(zs2, group))


def solution(mesh):
    rows = P(('data', 'chip', 'dap'))
    in_specs = (rows, rows, P('data'), P('data')) + (P(),) * 13
    vmem = pl.BlockSpec(memory_space=pltpu.VMEM)
    hbm = pl.BlockSpec(memory_space=pl.ANY)

    def per_device(m_blk, z_blk, msa_mask, res_mask, w_row_in, w_row_bias, w_row_out, w_col_in, w_col_out,
                   w_opm_in, w_opm_out, w_start_in, w_start_bias, w_start_out, w_end_in, w_end_bias, w_end_out):
        loaded = [m_blk, w_row_in, w_row_out, w_col_in, w_col_out, w_opm_out, w_start_in, w_start_out, w_end_in, w_end_out]
        scratch = [pltpu.VMEM(x.shape, x.dtype) for x in loaded] + [
            pltpu.VMEM((256, 256), BF16),
            pltpu.VMEM((256, 256), BF16),
            pltpu.VMEM((RES, LANES), BF16),
            pltpu.VMEM((RES, LANES), BF16),
            pltpu.VMEM((LANES, LANES), BF16),
            pltpu.VMEM((SLOC, RES, LANES), F32),
            pltpu.VMEM((RES, SEQ), F32),
            pltpu.VMEM((SEQ, RES), BF16),
            pltpu.VMEM((LANES, LANES), F32),
            pltpu.VMEM((RES, LANES), F32),
            pltpu.VMEM((3, 8, CZ), F32),
            pltpu.VMEM((16, 8, LANES), F32),
            pltpu.VMEM((HM, RES, LANES), F32),
            pltpu.VMEM((NDEV, HM, 16, LANES), BF16),
            pltpu.VMEM((NDEV, HT, 16, LANES), BF16),
            pltpu.VMEM((NDEV, HT, 16, LANES), BF16),
            pltpu.VMEM((2 * CM, CM), BF16),
            pltpu.VMEM((2 * CM, CM), BF16),
            pltpu.VMEM((2, 2 * CZ, CZ), BF16),
            pltpu.VMEM((4, LANES, CM), BF16),
            pltpu.VMEM((4, 4, LANES, LANES), BF16),
            pltpu.VMEM((2, RLOC, LANES, LANES), BF16),
            pltpu.VMEM((SLOC, RES, CM), BF16),
            pltpu.VMEM((NCHUNK, RES, CHUNK, CM), BF16),
            pltpu.VMEM((NCHUNK, NDEV, RLOC, CHUNK, CM), BF16),
            pltpu.VMEM((NCHUNK, RLOC, CROWS, CM), BF16),
            pltpu.VMEM((NDEV, RLOC, NCHUNK, CHUNK, CM), BF16),
            pltpu.VMEM((RLOC, SEQ, CM), BF16),
            pltpu.VMEM((4, RLOC, SEQ, LANES), BF16),
            pltpu.VMEM((RLOC, OPM, SEQ), BF16),
            pltpu.VMEM((RES, OPM, SEQ), BF16),
            pltpu.VMEM((OPM, LANES, SEQ), BF16),
            pltpu.VMEM((RLOC, OPM, OPM, LANES), BF16),
            pltpu.VMEM((OPM, OPM, CZ), BF16),
            pltpu.VMEM((CZ, OPM * OPM), BF16),
            pltpu.VMEM((RLOC, LANES, CZ), BF16),
            pltpu.VMEM((16, RES, CZ), BF16),
            pltpu.VMEM((2, RES, 8, CZ), BF16),
            pltpu.VMEM((2, NDEV, RLOC, 8, CZ), BF16),
            pltpu.VMEM((RLOC, RES, CZ), BF16),
            pltpu.VMEM((16, RES, CZ), BF16),
            pltpu.VMEM((2, RES, 8, CZ), BF16),
            pltpu.VMEM((2, NDEV, RLOC, 8, CZ), BF16),
            pltpu.SemaphoreType.DMA((NSTAGE, NDEV)),
            pltpu.SemaphoreType.DMA((NSTAGE, NDEV)),
            pltpu.SemaphoreType.DMA((NCHUNK + 5,)),
            pltpu.SemaphoreType.DMA((10,)),
            pltpu.SemaphoreType.DMA((7,)),
            pltpu.SemaphoreType.DMA((3, RLOC)),
            pltpu.SemaphoreType.DMA((4,)),
        ]
        m_home, z_new = pl.pallas_call(
            block_kernel,
            name='evoformer_block',
            out_shape=(jax.ShapeDtypeStruct((RES, NCHUNK, CHUNK, CM), BF16), jax.ShapeDtypeStruct(z_blk.shape, BF16)),
            in_specs=[hbm, vmem, vmem, vmem, hbm, vmem, hbm, hbm, hbm, vmem, hbm, hbm, vmem, hbm, hbm, vmem, hbm],
            out_specs=(hbm, vmem),
            scratch_shapes=scratch,
            compiler_params=pltpu.CompilerParams(collective_id=0, has_side_effects=True,
                                                 vmem_limit_bytes=56 * 1024 * 1024),
        )(m_blk, z_blk, msa_mask.T, res_mask.reshape(1, RES), w_row_in, w_row_bias.T, w_row_out, w_col_in, w_col_out,
          w_opm_in.T, w_opm_out, w_start_in, w_start_bias.T, w_start_out, w_end_in, w_end_bias.T, w_end_out)
        return jnp.swapaxes(m_home.reshape(RES, SLOC, CM), 0, 1), z_new

    return jax.shard_map(per_device, mesh=mesh, in_specs=in_specs, out_specs=(rows, rows), check_vma=False)
```

```python
import functools

import jax
import jax.numpy as jnp
import numpy as np
from jax import lax
from jax.experimental import pallas as pl
from jax.experimental.pallas import tpu as pltpu
from jax.sharding import PartitionSpec as P

BF16 = jnp.bfloat16
F32 = jnp.float32
MESH = pl.DeviceIdType.MESH
NDEV = 8
SEQ, RES, CM, CZ = 256, 96, 256, 128
SLOC, RLOC = SEQ // NDEV, RES // NDEV
HM, HT, HD, OPM = 8, 4, 32, 32
LANES = 128
MASKED = -1e9
SCALE = HD ** -0.5


def bf16_parts(value, n):
    parts = []
    for _ in range(n):
        parts.append(float(np.asarray(value - sum(parts), np.float32).astype(BF16)))
    return parts


MASKED_SCORE = bf16_parts(MASKED / SCALE, 3)

ROWB, MF, MB, STB, ZF, ENB, ZB = 0, 1, 5, 6, 7, 9, 10
NSTAGE = 12
ZGROUP = RLOC // 2
CHUNK = 8
NCHUNK = SLOC // CHUNK
CROWS = NDEV * CHUNK
LAG = 4
MB_EARLY = 8


def dot(a, b):
    return jnp.dot(a, b, preferred_element_type=F32)


def dot_t(a, b):
    return lax.dot_general(a, b, (((1,), (1,)), ((), ())), preferred_element_type=F32)


def iota(shape, dim):
    return lax.broadcasted_iota(jnp.int32, shape, dim)


def layer_norm(x):
    values = x.astype(F32)
    centred = values - jnp.mean(values, axis=-1, keepdims=True)
    variance = jnp.mean(centred * centred, axis=-1, keepdims=True)
    return (centred * lax.rsqrt(variance + 1e-5)).astype(BF16)


def add_residual(state, update):
    return (state.astype(F32) + update).astype(BF16)


def head_masks():
    lane = iota((16, LANES), 1)
    return [jnp.where((lane >= h * HD) & (lane < (h + 1) * HD), 1.0, 0.0).astype(BF16) for h in range(LANES // HD)]


def only_head(x, mask):
    return x * jnp.concatenate([mask] * (x.shape[0] // 16), axis=0)


def dot_tl(a, b):
    return lax.dot_general(a, b, (((0,), (0,)), ((), ())), preferred_element_type=F32)


def softmax_keys(logits):
    weights = jnp.exp(logits - jnp.max(logits, axis=0, keepdims=True))
    return (weights * (1.0 / jnp.sum(weights, axis=0, keepdims=True))).astype(BF16)


def pipeline(items, first, middle, last, finish, ahead=1, behind=1):
    count = len(items)
    opened, ready = {}, {}
    for n in range(-ahead, count + behind + 1):
        if n + ahead < count:
            opened[n + ahead] = first(items[n + ahead])
        if 0 <= n < count:
            ready[n] = middle(items[n], opened.pop(n))
        if 0 <= n - behind < count:
            last(items[n - behind], ready.pop(n - behind))
        if 0 <= n - behind - 1 < count:
            finish(items[n - behind - 1])


def attend_biased(rows, tiles, q_of, k_of, vg_of, bias_ref, keep_of, w_out, store):
    masks = head_masks()
    each = len(masks)
    vgs = {}
    mixed = {u: [] for u in rows}

    def first(item):
        u, t = item
        if t == 0:
            vgs[u] = vg_of(u)
        k = k_of(u, t)
        return dot_t(jnp.concatenate([only_head(k, mask) for mask in masks], axis=0), q_of(u, t))

    def middle(item, scores):
        u, t = item
        keep = keep_of(u) != 0.0
        return [softmax_keys(jnp.where(keep, scores[n * RES:(n + 1) * RES] * SCALE + bias_ref[each * t + n], MASKED))
                for n in range(each)]

    def last(item, probs):
        u, t = item
        for n in range(each):
            h = each * t + n
            padded = jnp.concatenate([probs[n], jnp.zeros((LANES - RES, LANES), BF16)], axis=0)
            mixed[u].append(dot(vgs[u][h * HD:(h + 1) * HD], padded))

    def finish(item):
        u, t = item
        if t == tiles - 1:
            gates = jax.nn.sigmoid(vgs[u][tiles * LANES:].astype(F32))
            store(u, dot_tl((jnp.concatenate(mixed[u], axis=0) * gates).astype(BF16), w_out))

    pipeline([(u, t) for u in rows for t in range(tiles)], first, middle, last, finish)


def attend_column(residues, q_of, k_of, aug_of, ones, vg_of, w_out, store):
    masks = head_masks()
    each = len(masks)
    halves = SEQ // LANES
    vgs, keys = {}, {}
    mixed = {(u, half): [] for u in residues for half in range(halves)}

    def first(item):
        u, h, half = item
        if (h, half) == (0, 0):
            vgs[u] = vg_of(u)
        if half == 0:
            keys[u, h] = jnp.concatenate([only_head(k_of(u, h // each), masks[h % each]), aug_of(u)], axis=1)
        q = q_of(u, h // each)[half * LANES:(half + 1) * LANES]
        return dot_t(keys[u, h], jnp.concatenate([q, ones], axis=1))

    def middle(item, scores):
        return softmax_keys(scores * SCALE)

    def last(item, probs):
        u, h, half = item
        mixed[u, half].append(dot(vgs[u][h * HD:(h + 1) * HD], probs))

    def finish(item):
        u, h, half = item
        if (h, half) == (HM - 1, halves - 1):
            gates = jax.nn.sigmoid(vgs[u][CM:].astype(F32))
            out = jnp.concatenate([jnp.concatenate(mixed[u, n], axis=0) for n in range(halves)], axis=1)
            store(u, dot_tl((out * gates).astype(BF16), w_out))

    pipeline([(u, h, half) for u in residues for h in range(HM) for half in range(halves)], first, middle, last, finish, 4, 2)


def block_kernel(m_any, z_ref, mask_ref, res_ref, row_in_any, w_row_bias, row_out_any, col_in_any, col_out_any,
                 w_opm_in, opm_out_any, start_in_any, w_start_bias, start_out_any, end_in_any, w_end_bias, end_out_any,
                 mback, z_out,
                 m_ref, w_row_in, w_row_out, w_col_in, w_col_out, w_opm_out, w_start_in, w_start_out, w_end_in, w_end_out,
                 perm, perm_out, comp, compz, hperm, keep_row, mask_t, mask_s, norm, res_keep, wbt, bcol, bias,
                 rowb_recv, stb_recv, enb_recv, row_vg, col_vg, tri_vg, yrow, rowqk, triqk, m1, msend, mrecv, mcols, mdone,
                 ycol, colqk, caug, ckeep, ones,
                 left, crecv, cbig, outer, w2, w2t, ynorm, z1, zs, zr, z2, z3, zs2, zr2,
                 send_sem, recv_sem, local_sem, load_sem, c_send, c_recv, c_pair):
    data = lax.axis_index('data')
    me = lax.axis_index('chip') * 4 + lax.axis_index('dap')
    core, chip_x, chip_y = lax.rem(me, 2), lax.rem(me // 2, 2), me // 4
    partner = me + 1 - 2 * core
    to_x, to_y = 2 - 4 * chip_x, 4 - 8 * chip_y
    twins = (me + to_x + to_y, me + to_x, me + to_y)

    def device(d):
        return (data, d // 4, lax.rem(d, 4))

    def peer(r):
        return lax.rem(me + r, NDEV)

    def source(r):
        return lax.rem(me + NDEV - r, NDEV)

    def remote(src, dst, send, recv, d):
        return pltpu.make_async_remote_copy(src_ref=src, dst_ref=dst, send_sem=send, recv_sem=recv,
                                            device_id=device(d), device_id_type=MESH)

    def start_all(stage, src_of, dst_of):
        for r in range(1, NDEV):
            d = peer(r)
            remote(src_of(d), dst_of(me), send_sem.at[stage, r], recv_sem.at[stage, r], d).start()

    def wait_recv(stage, dst_of):
        for r in range(1, NDEV):
            dst = dst_of(source(r))
            remote(dst, dst, send_sem.at[stage, r], recv_sem.at[stage, r], peer(r)).wait_recv()

    def wait_send(stage, src_of):
        for r in range(1, NDEV):
            src = src_of(peer(r))
            remote(src, src, send_sem.at[stage, r], recv_sem.at[stage, r], peer(r)).wait_send()

    barrier = pltpu.get_barrier_semaphore()
    for r in range(1, NDEV):
        pl.semaphore_signal(barrier, inc=1, device_id=device(peer(r)), device_id_type=MESH)

    loads = [pltpu.make_async_copy(src, dst, load_sem.at[n]) for n, (src, dst) in enumerate((
        (row_in_any, w_row_in), (m_any, m_ref), (row_out_any, w_row_out), (col_in_any, w_col_in), (opm_out_any, w_opm_out),
        (start_in_any, w_start_in), (end_in_any, w_end_in), (col_out_any, w_col_out), (start_out_any, w_start_out),
        (end_out_any, w_end_out)))]
    for load in loads:
        load.start()

    r0, c0 = iota((256, 256), 0), iota((256, 256), 1)
    perm[...] = jnp.where(((r0 >> 4) == (c0 & 15)) & ((r0 & 15) == (c0 >> 4)), 1.0, 0.0).astype(BF16)
    perm_out[...] = jnp.where(((r0 >> 3) == (c0 & 31)) & ((r0 & 7) == (c0 >> 5)), 1.0, 0.0).astype(BF16)
    r1, c1 = iota((RES, LANES), 0), iota((RES, LANES), 1)
    comp[...] = jnp.where(((c1 & 15) < RLOC) & (r1 == (c1 >> 4) * RLOC + (c1 & 15)), 1.0, 0.0).astype(BF16)
    compz[...] = jnp.where(((c1 & 7) < ZGROUP) & (r1 == ((c1 >> 3) & 7) * RLOC + (c1 >> 6) * ZGROUP + (c1 & 7)),
                           1.0, 0.0).astype(BF16)
    r2, c2 = iota((LANES, LANES), 0), iota((LANES, LANES), 1)
    hperm[...] = jnp.where(((r2 >> 4) == (c2 & 7)) & ((r2 & 15) == (c2 >> 3)), 1.0, 0.0).astype(BF16)
    eye = jnp.where(r2 == c2, 1.0, 0.0).astype(BF16)
    ones[...] = jnp.where(iota((SEQ, LANES), 1) < len(MASKED_SCORE), 1.0, 0.0).astype(BF16)
    bcol[...] = jnp.zeros_like(bcol)
    wbt[...] = jnp.zeros_like(wbt)
    for n, w in enumerate((w_row_bias, w_start_bias, w_end_bias)):
        wbt[n, 0:w.shape[0], :] = w[...].astype(F32)

    def send_bias(recv, which, heads, stage):
        weights = wbt[which].astype(BF16)

        @pl.loop(0, RLOC)
        def _(i):
            bcol[i] = dot_t(weights, ynorm[i])

        mine = dot(hperm[0:heads * 16, :], bcol[...].reshape(LANES, LANES).astype(BF16)).astype(BF16)
        recv[me] = mine.reshape(heads, 16, LANES)
        start_all(stage, lambda d: recv.at[me], lambda s: recv.at[s])

    def bias_rows(recv):
        return lambda s: recv.at[s]

    def take_bias(recv, heads, stage):
        wait_recv(stage, bias_rows(recv))
        for h in range(heads):
            rows = dot(comp[...], recv[:, h].reshape(LANES, LANES)).astype(BF16)
            bias[h] = dot_t(eye, jnp.concatenate([rows, jnp.zeros((LANES - RES, LANES), BF16)], axis=0))[0:RES]

    ynorm[:, RES:, :] = jnp.zeros((RLOC, LANES - RES, CZ), BF16)

    @pl.loop(0, RLOC)
    def _(i):
        ynorm[i, 0:RES, :] = layer_norm(z_ref[i])

    pl.semaphore_wait(barrier, NDEV - 1)
    send_bias(rowb_recv, 0, HM, ROWB)

    res_keep[...] = dot((eye[0:RES, 0:RES].astype(F32) * res_ref[...].astype(F32)).astype(BF16),
                        jnp.ones((RES, LANES), BF16))
    seq_order = jnp.where(r0 == ((c0 >> 3) & 7) * SLOC + (c0 >> 6) * CHUNK + (c0 & 7), 1.0, 0.0).astype(BF16)
    seq_rows = jnp.where(c0 == ((r0 >> 3) & 7) * SLOC + (r0 >> 6) * CHUNK + (r0 & 7), 1.0, 0.0).astype(BF16)
    mt = mask_ref[...].astype(F32).astype(BF16)
    mask_t[...] = dot(mt, seq_order)
    mask_s[...] = dot_t(seq_rows, mt).astype(BF16)

    @pl.loop(0, SLOC)
    def _(i):
        pick = jnp.where(iota((SEQ, LANES), 0) == me * SLOC + i, 1.0, 0.0).astype(BF16)
        keep_row[i] = dot(mask_ref[...].astype(F32).astype(BF16), pick)

    for load in loads:
        load.wait()
    row_vg[...] = jnp.transpose(w_row_in[:, 2 * CM:])
    col_vg[...] = jnp.transpose(w_col_in[:, 2 * CM:])
    tri_vg[0] = jnp.transpose(w_start_in[:, 2 * CZ:])
    tri_vg[1] = jnp.transpose(w_end_in[:, 2 * CZ:])
    norm[...] = jnp.zeros_like(norm)
    norm[0:RES, 0:RES] = dot_t(mt, mt)
    w_full = w_opm_out[...].reshape(OPM, OPM, CZ)
    for a in range(2):
        for c in range(2):
            blk = w_full[16 * a:16 * a + 16, 16 * c:16 * c + 16, :].reshape(256, CZ)
            w2[16 * c:16 * c + 16, 16 * a:16 * a + 16, :] = dot(perm[...], blk).astype(BF16).reshape(16, 16, CZ)
    w2t[...] = dot_t(eye, w2[...].reshape(OPM * OPM, CZ)).astype(BF16)
    cbig[:, RES:, :] = jnp.zeros((OPM, LANES - RES, SEQ), BF16)
    yrow[:, RES:, :] = jnp.zeros((4, LANES - RES, CM), BF16)
    rowqk[:, :, RES:, :] = jnp.zeros((4, 4, LANES - RES, LANES), BF16)
    triqk[:, :, RES:, :] = jnp.zeros((2, RLOC, LANES - RES, LANES), BF16)
    z1[RLOC:, :, :] = jnp.zeros((16 - RLOC, RES, CZ), BF16)
    z3[...] = jnp.zeros_like(z3)

    take_bias(rowb_recv, HM, ROWB)

    def m_src(q):
        return lambda d: msend.at[q, pl.ds(d * RLOC, RLOC)]

    def m_dst(q):
        return lambda s: mrecv.at[q, s]

    def local_copy(src, dst, n):
        return pltpu.make_async_copy(src, dst, local_sem.at[n])

    def row_chunk(q):
        @pl.loop(0, CHUNK // 4)
        def _(blk):
            s0 = q * CHUNK + blk * 4
            x = m_ref[pl.ds(s0, 4)].reshape(4 * RES, CM)
            y = layer_norm(x)
            yrow[:, 0:RES, :] = y.reshape(4, RES, CM)
            qk = dot(y, w_row_in[:, 0:2 * CM]).astype(BF16)
            for t in range(4):
                rowqk[t, :, 0:RES, :] = qk[:, t * LANES:(t + 1) * LANES].reshape(4, RES, LANES)

            def store(u, update):
                m1[s0 + u] = add_residual(m_ref[s0 + u], update[0:RES])
            attend_biased(range(4), 2, lambda u, t: rowqk[t, u], lambda u, t: rowqk[2 + t, u, 0:RES],
                          lambda u: dot_t(row_vg[...], yrow[u]).astype(BF16), bias,
                          lambda u: keep_row[s0 + u], w_row_out[...], store)

        for j in range(RES // 32):
            blk = m1[CHUNK * q:CHUNK * q + CHUNK, 32 * j:32 * j + 32, :].reshape(256, CM)
            msend[q, 32 * j:32 * j + 32] = dot(perm_out[...], blk).reshape(32, CHUNK, CM).astype(BF16)
        start_all(MF + q, m_src(q), m_dst(q))
        local_copy(m_src(q)(me), m_dst(q)(me), q).start()

    def column_projection(q):
        local_copy(m_src(q)(me), m_dst(q)(me), q).wait()
        wait_recv(MF + q, m_dst(q))

        @pl.loop(0, RLOC // 4)
        def _(blk):
            x = jnp.concatenate([mrecv[q, :, blk * 4 + u].astype(F32).reshape(CROWS, CM) for u in range(4)], axis=0)
            for u in range(4):
                mcols[q, blk * 4 + u] = x[u * CROWS:(u + 1) * CROWS].astype(BF16)
            y = layer_norm(x)
            ycol[pl.ds(blk * 4, 4), CROWS * q:CROWS * q + CROWS, :] = y.reshape(4, CROWS, CM)
            qk = dot(y, w_col_in[:, 0:2 * CM]).astype(BF16)
            for t in range(4):
                colqk[t, pl.ds(blk * 4, 4), CROWS * q:CROWS * q + CROWS, :] = (
                    qk[:, t * LANES:(t + 1) * LANES].reshape(4, CROWS, LANES))

    row_chunk(0)
    row_chunk(1)
    row_chunk(2)
    column_projection(0)
    row_chunk(3)
    column_projection(1)
    column_projection(2)
    column_projection(3)

    def mb_start(j):
        start_all(MB, lambda d: mdone.at[d, j], lambda s: mback.at[s * RLOC + j])

    def relay(j):
        for t, twin in enumerate(twins):
            row = crecv.at[twin * RLOC + j]
            remote(row, row, c_send.at[t], c_recv.at[t, j], twin).wait_recv()
            remote(row, row, c_send.at[3 + t], c_pair.at[t], partner).start()

    @pl.loop(0, RLOC // 2)
    def _(pair):
        lane = iota((SEQ, LANES), 1)
        offset = jnp.zeros((SEQ, LANES), F32)
        for n, part in enumerate(MASKED_SCORE):
            offset = jnp.where(lane == n, part, offset)
        for u in range(2):
            pick = jnp.where(iota((RES, LANES), 0) == me * RLOC + pair * 2 + u, 1.0, 0.0).astype(BF16)
            keep = dot(mask_s[...], pick)
            caug[u] = ((1.0 - keep) * offset).astype(BF16)
            keep = keep.astype(BF16)
            for t in range(2):
                ckeep[u, t] = colqk[2 + t, pair * 2 + u] * keep

        def store(u, update):
            j = pair * 2 + u
            mask_row = mask_t[pl.ds(me * RLOC + j, 1), :]
            x = add_residual(mcols[:, j].reshape(SEQ, CM), update)
            both = dot_t(w_opm_in[...], layer_norm(x)).astype(BF16).astype(F32) * mask_row
            left[j] = both[0:OPM].astype(BF16)
            crecv[me * RLOC + j] = both[OPM:].astype(BF16)
            done = x.astype(F32).reshape(NCHUNK, NDEV, CHUNK, CM).astype(BF16)
            for d in range(NDEV):
                mdone[d, j] = done[:, d]

        attend_column(range(2), lambda u, t: colqk[t, pair * 2 + u], lambda u, t: ckeep[u, t], lambda u: caug[u],
                      ones[0:LANES], lambda u: dot_t(col_vg[...], ycol[pair * 2 + u]).astype(BF16), w_col_out[...], store)
        for u in range(2):
            j = pair * 2 + u
            row = crecv.at[me * RLOC + j]
            for t, twin in enumerate(twins):
                remote(row, row, c_send.at[t], c_recv.at[t, j], twin).start()
            remote(row, row, c_send.at[6], c_pair.at[3], partner).start()

        @pl.when(pair >= LAG // 2)
        def _():
            for u in range(2):
                relay(pair * 2 - LAG + u)

        @pl.when(pair < MB_EARLY // 2)
        def _():
            for u in range(2):
                mb_start(pair * 2 + u)

    for j in range(RLOC - LAG, RLOC):
        relay(j)
    keep_mine = local_copy(mdone.at[me], mback.at[pl.ds(me * RLOC, RLOC)], NCHUNK + 4)
    keep_mine.start()

    def c_rows(s):
        return crecv.at[pl.ds(s * RLOC, RLOC)]

    for t, first in enumerate(twins + (me,)):
        rows = c_rows(first + 1 - 2 * core)
        remote(rows, rows, c_send.at[3 + t], c_pair.at[t], partner).wait_recv()
    for j in range(MB_EARLY, MB_EARLY + 3):
        mb_start(j)
    for c in range(2):
        @pl.loop(0, RES // 16)
        def _(j):
            j0 = pl.multiple_of(j * 16, 16)
            blk = crecv[pl.ds(j0, 16), 16 * c:16 * c + 16, :].reshape(256, SEQ)
            cbig[16 * c:16 * c + 16, pl.ds(j0, 16), :] = dot(perm[...], blk).astype(BF16).reshape(16, 16, SEQ)

    @pl.loop(0, OPM // 2)
    def _(c):
        prod = dot_t(left[...].reshape(RLOC * OPM, SEQ), cbig[pl.ds(2 * c, 2)].reshape(256, SEQ)).astype(BF16)
        for u in range(2):
            outer[:, 2 * c + u] = prod[:, u * LANES:(u + 1) * LANES].reshape(RLOC, OPM, LANES)

    @pl.loop(0, RLOC)
    def _(i):
        update = dot(w2t[...], outer[i].reshape(OPM * OPM, LANES))
        update = update / (1e-3 + norm[pl.ds(me * RLOC + i, 1), :])
        z1[i] = add_residual(z_ref[i], jnp.transpose(update)[0:RES])

    def z_src(buf, group):
        return lambda d: buf.at[group, pl.ds(d * RLOC, RLOC)]

    def z_dst(buf, group):
        return lambda s: buf.at[group, s]

    def triangle(state, result, w_in, which, w_out, recv, stage, late, send, zrecv, moved, zstage, slot):
        @pl.loop(0, RLOC)
        def _(i):
            ynorm[i, 0:RES, :] = layer_norm(state[i])
        send_bias(recv, which, HT, stage)

        @pl.loop(0, RLOC // 4)
        def _(blk):
            y = ynorm[pl.ds(blk * 4, 4), 0:RES, :].reshape(4 * RES, CZ)
            qk = dot(y, w_in[:, 0:2 * CZ]).astype(BF16)
            for t in range(2):
                triqk[t, pl.ds(blk * 4, 4), 0:RES, :] = qk[:, t * LANES:(t + 1) * LANES].reshape(4, RES, LANES)
        take_bias(recv, HT, stage)
        for j in late:
            mb_start(j)

        for group in range(2):
            first = group * ZGROUP

            def store(u, update):
                result[u] = add_residual(state[u], update[0:RES])
            attend_biased(range(first, first + ZGROUP), 1, lambda u, t: triqk[0, u], lambda u, t: triqk[1, u, 0:RES],
                          lambda u: dot_t(tri_vg[which - 1], ynorm[u]).astype(BF16), bias,
                          lambda u: res_keep[...], w_out[...], store)
            for j in range(RES // 32):
                blk = result[first:first + 8, 32 * j:32 * j + 32, :].reshape(256, CZ)
                send[group, 32 * j:32 * j + 32] = dot(perm_out[...], blk).reshape(32, 8, CZ).astype(BF16)
            start_all(zstage + group, z_src(send, group), z_dst(zrecv, group))
            local_copy(z_src(send, group)(me), z_dst(zrecv, group)(me), slot + group).start()

        for group in range(2):
            local_copy(z_src(send, group)(me), z_dst(zrecv, group)(me), slot + group).wait()
            wait_recv(zstage + group, z_dst(zrecv, group))

        @pl.loop(0, RLOC)
        def _(i):
            rows = zrecv[:, :, i].astype(F32).reshape(LANES, CZ).astype(BF16)
            moved[i] = dot(compz[...], rows).astype(BF16)

    triangle(z1, z1, w_start_in, 1, w_start_out, stb_recv, STB, (MB_EARLY + 3,), zs, zr, z2, ZF, NCHUNK)
    triangle(z2, z3, w_end_in, 2, w_end_out, enb_recv, ENB, (), zs2, zr2, z_out, ZB, NCHUNK + 2)

    wait_recv(MB, lambda s: mback.at[pl.ds(s * RLOC, RLOC)])
    keep_mine.wait()

    wait_send(ROWB, lambda d: bias_rows(rowb_recv)(me))
    for q in range(NCHUNK):
        wait_send(MF + q, m_src(q))
    wait_send(MB, lambda d: mdone.at[d])
    for t in range(7):
        rows = c_rows(me if t in (0, 1, 2, 6) else twins[t - 3])
        remote(rows, rows, c_send.at[t], c_pair.at[0], partner).wait_send()
    wait_send(STB, lambda d: bias_rows(stb_recv)(me))
    for group in range(2):
        wait_send(ZF + group, z_src(zs, group))
    wait_send(ENB, lambda d: bias_rows(enb_recv)(me))
    for group in range(2):
        wait_send(ZB + group, z_src(zs2, group))


def solution(mesh):
    rows = P(('data', 'chip', 'dap'))
    in_specs = (rows, rows, P('data'), P('data')) + (P(),) * 13
    vmem = pl.BlockSpec(memory_space=pltpu.VMEM)
    hbm = pl.BlockSpec(memory_space=pl.ANY)

    def per_device(m_blk, z_blk, msa_mask, res_mask, w_row_in, w_row_bias, w_row_out, w_col_in, w_col_out,
                   w_opm_in, w_opm_out, w_start_in, w_start_bias, w_start_out, w_end_in, w_end_bias, w_end_out):
        loaded = [m_blk, w_row_in, w_row_out, w_col_in, w_col_out, w_opm_out, w_start_in, w_start_out, w_end_in, w_end_out]
        scratch = [pltpu.VMEM(x.shape, x.dtype) for x in loaded] + [
            pltpu.VMEM((256, 256), BF16),
            pltpu.VMEM((256, 256), BF16),
            pltpu.VMEM((RES, LANES), BF16),
            pltpu.VMEM((RES, LANES), BF16),
            pltpu.VMEM((LANES, LANES), BF16),
            pltpu.VMEM((SLOC, RES, LANES), F32),
            pltpu.VMEM((RES, SEQ), F32),
            pltpu.VMEM((SEQ, RES), BF16),
            pltpu.VMEM((LANES, LANES), F32),
            pltpu.VMEM((RES, LANES), F32),
            pltpu.VMEM((3, 8, CZ), F32),
            pltpu.VMEM((16, 8, LANES), F32),
            pltpu.VMEM((HM, RES, LANES), F32),
            pltpu.VMEM((NDEV, HM, 16, LANES), BF16),
            pltpu.VMEM((NDEV, HT, 16, LANES), BF16),
            pltpu.VMEM((NDEV, HT, 16, LANES), BF16),
            pltpu.VMEM((2 * CM, CM), BF16),
            pltpu.VMEM((2 * CM, CM), BF16),
            pltpu.VMEM((2, 2 * CZ, CZ), BF16),
            pltpu.VMEM((4, LANES, CM), BF16),
            pltpu.VMEM((4, 4, LANES, LANES), BF16),
            pltpu.VMEM((2, RLOC, LANES, LANES), BF16),
            pltpu.VMEM((SLOC, RES, CM), BF16),
            pltpu.VMEM((NCHUNK, RES, CHUNK, CM), BF16),
            pltpu.VMEM((NCHUNK, NDEV, RLOC, CHUNK, CM), BF16),
            pltpu.VMEM((NCHUNK, RLOC, CROWS, CM), BF16),
            pltpu.VMEM((NDEV, RLOC, NCHUNK, CHUNK, CM), BF16),
            pltpu.VMEM((RLOC, SEQ, CM), BF16),
            pltpu.VMEM((4, RLOC, SEQ, LANES), BF16),
            pltpu.VMEM((2, SEQ, LANES), BF16),
            pltpu.VMEM((2, 2, SEQ, LANES), BF16),
            pltpu.VMEM((SEQ, LANES), BF16),
            pltpu.VMEM((RLOC, OPM, SEQ), BF16),
            pltpu.VMEM((RES, OPM, SEQ), BF16),
            pltpu.VMEM((OPM, LANES, SEQ), BF16),
            pltpu.VMEM((RLOC, OPM, OPM, LANES), BF16),
            pltpu.VMEM((OPM, OPM, CZ), BF16),
            pltpu.VMEM((CZ, OPM * OPM), BF16),
            pltpu.VMEM((RLOC, LANES, CZ), BF16),
            pltpu.VMEM((16, RES, CZ), BF16),
            pltpu.VMEM((2, RES, 8, CZ), BF16),
            pltpu.VMEM((2, NDEV, RLOC, 8, CZ), BF16),
            pltpu.VMEM((RLOC, RES, CZ), BF16),
            pltpu.VMEM((16, RES, CZ), BF16),
            pltpu.VMEM((2, RES, 8, CZ), BF16),
            pltpu.VMEM((2, NDEV, RLOC, 8, CZ), BF16),
            pltpu.SemaphoreType.DMA((NSTAGE, NDEV)),
            pltpu.SemaphoreType.DMA((NSTAGE, NDEV)),
            pltpu.SemaphoreType.DMA((NCHUNK + 5,)),
            pltpu.SemaphoreType.DMA((10,)),
            pltpu.SemaphoreType.DMA((7,)),
            pltpu.SemaphoreType.DMA((3, RLOC)),
            pltpu.SemaphoreType.DMA((4,)),
        ]
        m_home, z_new = pl.pallas_call(
            block_kernel,
            name='evoformer_block',
            out_shape=(jax.ShapeDtypeStruct((RES, NCHUNK, CHUNK, CM), BF16), jax.ShapeDtypeStruct(z_blk.shape, BF16)),
            in_specs=[hbm, vmem, vmem, vmem, hbm, vmem, hbm, hbm, hbm, vmem, hbm, hbm, vmem, hbm, hbm, vmem, hbm],
            out_specs=(hbm, vmem),
            scratch_shapes=scratch,
            compiler_params=pltpu.CompilerParams(collective_id=0, has_side_effects=True,
                                                 vmem_limit_bytes=56 * 1024 * 1024),
        )(m_blk, z_blk, msa_mask.T, res_mask.reshape(1, RES), w_row_in, w_row_bias.T, w_row_out, w_col_in, w_col_out,
          w_opm_in.T, w_opm_out, w_start_in, w_start_bias.T, w_start_out, w_end_in, w_end_bias.T, w_end_out)
        return jnp.swapaxes(m_home.reshape(RES, SLOC, CM), 0, 1), z_new

    return jax.shard_map(per_device, mesh=mesh, in_specs=in_specs, out_specs=(rows, rows), check_vma=False)
```

```python
import functools

import jax
import jax.numpy as jnp
import numpy as np
from jax import lax
from jax.experimental import pallas as pl
from jax.experimental.pallas import tpu as pltpu
from jax.sharding import PartitionSpec as P

BF16 = jnp.bfloat16
F32 = jnp.float32
MESH = pl.DeviceIdType.MESH
NDEV = 8
SEQ, RES, CM, CZ = 256, 96, 256, 128
SLOC, RLOC = SEQ // NDEV, RES // NDEV
HM, HT, HD, OPM = 8, 4, 32, 32
LANES = 128
MASKED = -1e9
SCALE = HD ** -0.5


def bf16_parts(value, n):
    parts = []
    for _ in range(n):
        parts.append(float(np.asarray(value - sum(parts), np.float32).astype(BF16)))
    return parts


MASKED_SCORE = bf16_parts(MASKED / SCALE, 3)

ROWB, MF, MB, STB, ZF, ENB, ZB = 0, 1, 5, 6, 7, 9, 10
NSTAGE = 12
ZGROUP = RLOC // 2
CHUNK = 8
NCHUNK = SLOC // CHUNK
CROWS = NDEV * CHUNK
LAG = 4
MB_EARLY = 8
NRES = 2


def dot(a, b):
    return jnp.dot(a, b, preferred_element_type=F32)


def dot_t(a, b):
    return lax.dot_general(a, b, (((1,), (1,)), ((), ())), preferred_element_type=F32)


def iota(shape, dim):
    return lax.broadcasted_iota(jnp.int32, shape, dim)


def layer_norm(x):
    values = x.astype(F32)
    centred = values - jnp.mean(values, axis=-1, keepdims=True)
    variance = jnp.mean(centred * centred, axis=-1, keepdims=True)
    return (centred * lax.rsqrt(variance + 1e-5)).astype(BF16)


def add_residual(state, update):
    return (state.astype(F32) + update).astype(BF16)


def head_masks():
    lane = iota((16, LANES), 1)
    return [jnp.where((lane >= h * HD) & (lane < (h + 1) * HD), 1.0, 0.0).astype(BF16) for h in range(LANES // HD)]


def only_head(x, mask):
    return x * jnp.concatenate([mask] * (x.shape[0] // 16), axis=0)


def dot_tl(a, b):
    return lax.dot_general(a, b, (((0,), (0,)), ((), ())), preferred_element_type=F32)


def softmax_keys(logits):
    weights = jnp.exp(logits - jnp.max(logits, axis=0, keepdims=True))
    return (weights * (1.0 / jnp.sum(weights, axis=0, keepdims=True))).astype(BF16)


def pipeline(items, first, middle, last, finish, ahead=1, behind=1):
    count = len(items)
    opened, ready = {}, {}
    for n in range(-ahead, count + behind + 1):
        if n + ahead < count:
            opened[n + ahead] = first(items[n + ahead])
        if 0 <= n < count:
            ready[n] = middle(items[n], opened.pop(n))
        if 0 <= n - behind < count:
            last(items[n - behind], ready.pop(n - behind))
        if 0 <= n - behind - 1 < count:
            finish(items[n - behind - 1])


def attend_biased(rows, tiles, q_of, k_of, vg_of, bias_ref, keep_of, w_out, store):
    masks = head_masks()
    each = len(masks)
    vgs = {}
    mixed = {u: [] for u in rows}

    def first(item):
        u, t = item
        if t == 0:
            vgs[u] = vg_of(u)
        k = k_of(u, t)
        return dot_t(jnp.concatenate([only_head(k, mask) for mask in masks], axis=0), q_of(u, t))

    def middle(item, scores):
        u, t = item
        keep = keep_of(u) != 0.0
        return [softmax_keys(jnp.where(keep, scores[n * RES:(n + 1) * RES] * SCALE + bias_ref[each * t + n], MASKED))
                for n in range(each)]

    def last(item, probs):
        u, t = item
        for n in range(each):
            h = each * t + n
            padded = jnp.concatenate([probs[n], jnp.zeros((LANES - RES, LANES), BF16)], axis=0)
            mixed[u].append(dot(vgs[u][h * HD:(h + 1) * HD], padded))

    def finish(item):
        u, t = item
        if t == tiles - 1:
            gates = jax.nn.sigmoid(vgs[u][tiles * LANES:].astype(F32))
            store(u, dot_tl((jnp.concatenate(mixed[u], axis=0) * gates).astype(BF16), w_out))

    pipeline([(u, t) for u in rows for t in range(tiles)], first, middle, last, finish)


def attend_column(residues, q_of, k_of, aug_of, ones, vg_of, w_out, store):
    masks = head_masks()
    each = len(masks)
    halves = SEQ // LANES
    vgs, keys = {}, {}
    mixed = {(u, half): [] for u in residues for half in range(halves)}

    def first(item):
        u, h, half = item
        if (h, half) == (0, 0):
            vgs[u] = vg_of(u)
        if half == 0:
            keys[u, h] = jnp.concatenate([only_head(k_of(u, h // each), masks[h % each]), aug_of(u)], axis=1)
        q = q_of(u, h // each)[half * LANES:(half + 1) * LANES]
        return dot_t(keys[u, h], jnp.concatenate([q, ones], axis=1))

    def middle(item, scores):
        return softmax_keys(scores * SCALE)

    def last(item, probs):
        u, h, half = item
        mixed[u, half].append(dot(vgs[u][h * HD:(h + 1) * HD], probs))

    def finish(item):
        u, h, half = item
        if (h, half) == (HM - 1, halves - 1):
            gates = jax.nn.sigmoid(vgs[u][CM:].astype(F32))
            out = jnp.concatenate([jnp.concatenate(mixed[u, n], axis=0) for n in range(halves)], axis=1)
            store(u, dot_tl((out * gates).astype(BF16), w_out))

    pipeline([(u, h, half) for u in residues for h in range(HM) for half in range(halves)], first, middle, last, finish, 4, 2)


def block_kernel(m_any, z_ref, mask_ref, res_ref, row_in_any, w_row_bias, row_out_any, col_in_any, col_out_any,
                 w_opm_in, opm_out_any, start_in_any, w_start_bias, start_out_any, end_in_any, w_end_bias, end_out_any,
                 mback, z_out,
                 m_ref, w_row_in, w_row_out, w_col_in, w_col_out, w_opm_out, w_start_in, w_start_out, w_end_in, w_end_out,
                 perm, perm_out, comp, compz, hperm, keep_row, mask_t, mask_s, norm, res_keep, wbt, bcol, bias,
                 rowb_recv, stb_recv, enb_recv, row_vg, col_vg, tri_vg, yrow, rowqk, triqk, m1, msend, mrecv, mcols, mdone,
                 ycol, colqk, caug, ckeep, ones,
                 left, crecv, cbig, outer, w2, w2t, ynorm, z1, zs, zr, z2, z3, zs2, zr2,
                 send_sem, recv_sem, local_sem, load_sem, c_send, c_recv, c_pair):
    data = lax.axis_index('data')
    me = lax.axis_index('chip') * 4 + lax.axis_index('dap')
    core, chip_x, chip_y = lax.rem(me, 2), lax.rem(me // 2, 2), me // 4
    partner = me + 1 - 2 * core
    to_x, to_y = 2 - 4 * chip_x, 4 - 8 * chip_y
    twins = (me + to_x + to_y, me + to_x, me + to_y)

    def device(d):
        return (data, d // 4, lax.rem(d, 4))

    def peer(r):
        return lax.rem(me + r, NDEV)

    def source(r):
        return lax.rem(me + NDEV - r, NDEV)

    def remote(src, dst, send, recv, d):
        return pltpu.make_async_remote_copy(src_ref=src, dst_ref=dst, send_sem=send, recv_sem=recv,
                                            device_id=device(d), device_id_type=MESH)

    def start_all(stage, src_of, dst_of):
        for r in range(1, NDEV):
            d = peer(r)
            remote(src_of(d), dst_of(me), send_sem.at[stage, r], recv_sem.at[stage, r], d).start()

    def wait_recv(stage, dst_of):
        for r in range(1, NDEV):
            dst = dst_of(source(r))
            remote(dst, dst, send_sem.at[stage, r], recv_sem.at[stage, r], peer(r)).wait_recv()

    def wait_send(stage, src_of):
        for r in range(1, NDEV):
            src = src_of(peer(r))
            remote(src, src, send_sem.at[stage, r], recv_sem.at[stage, r], peer(r)).wait_send()

    barrier = pltpu.get_barrier_semaphore()
    for r in range(1, NDEV):
        pl.semaphore_signal(barrier, inc=1, device_id=device(peer(r)), device_id_type=MESH)

    loads = [pltpu.make_async_copy(src, dst, load_sem.at[n]) for n, (src, dst) in enumerate((
        (row_in_any, w_row_in), (m_any, m_ref), (row_out_any, w_row_out), (col_in_any, w_col_in), (opm_out_any, w_opm_out),
        (start_in_any, w_start_in), (end_in_any, w_end_in), (col_out_any, w_col_out), (start_out_any, w_start_out),
        (end_out_any, w_end_out)))]
    for load in loads:
        load.start()

    r0, c0 = iota((256, 256), 0), iota((256, 256), 1)
    perm[...] = jnp.where(((r0 >> 4) == (c0 & 15)) & ((r0 & 15) == (c0 >> 4)), 1.0, 0.0).astype(BF16)
    perm_out[...] = jnp.where(((r0 >> 3) == (c0 & 31)) & ((r0 & 7) == (c0 >> 5)), 1.0, 0.0).astype(BF16)
    r1, c1 = iota((RES, LANES), 0), iota((RES, LANES), 1)
    comp[...] = jnp.where(((c1 & 15) < RLOC) & (r1 == (c1 >> 4) * RLOC + (c1 & 15)), 1.0, 0.0).astype(BF16)
    compz[...] = jnp.where(((c1 & 7) < ZGROUP) & (r1 == ((c1 >> 3) & 7) * RLOC + (c1 >> 6) * ZGROUP + (c1 & 7)),
                           1.0, 0.0).astype(BF16)
    r2, c2 = iota((LANES, LANES), 0), iota((LANES, LANES), 1)
    hperm[...] = jnp.where(((r2 >> 4) == (c2 & 7)) & ((r2 & 15) == (c2 >> 3)), 1.0, 0.0).astype(BF16)
    eye = jnp.where(r2 == c2, 1.0, 0.0).astype(BF16)
    ones[...] = jnp.where(iota((SEQ, LANES), 1) < len(MASKED_SCORE), 1.0, 0.0).astype(BF16)
    bcol[...] = jnp.zeros_like(bcol)
    wbt[...] = jnp.zeros_like(wbt)
    for n, w in enumerate((w_row_bias, w_start_bias, w_end_bias)):
        wbt[n, 0:w.shape[0], :] = w[...].astype(F32)

    def send_bias(recv, which, heads, stage):
        weights = wbt[which].astype(BF16)

        @pl.loop(0, RLOC)
        def _(i):
            bcol[i] = dot_t(weights, ynorm[i])

        mine = dot(hperm[0:heads * 16, :], bcol[...].reshape(LANES, LANES).astype(BF16)).astype(BF16)
        recv[me] = mine.reshape(heads, 16, LANES)
        start_all(stage, lambda d: recv.at[me], lambda s: recv.at[s])

    def bias_rows(recv):
        return lambda s: recv.at[s]

    def take_bias(recv, heads, stage):
        wait_recv(stage, bias_rows(recv))
        for h in range(heads):
            rows = dot(comp[...], recv[:, h].reshape(LANES, LANES)).astype(BF16)
            bias[h] = dot_t(eye, jnp.concatenate([rows, jnp.zeros((LANES - RES, LANES), BF16)], axis=0))[0:RES]

    ynorm[:, RES:, :] = jnp.zeros((RLOC, LANES - RES, CZ), BF16)

    @pl.loop(0, RLOC)
    def _(i):
        ynorm[i, 0:RES, :] = layer_norm(z_ref[i])

    pl.semaphore_wait(barrier, NDEV - 1)
    send_bias(rowb_recv, 0, HM, ROWB)

    res_keep[...] = dot((eye[0:RES, 0:RES].astype(F32) * res_ref[...].astype(F32)).astype(BF16),
                        jnp.ones((RES, LANES), BF16))
    seq_order = jnp.where(r0 == ((c0 >> 3) & 7) * SLOC + (c0 >> 6) * CHUNK + (c0 & 7), 1.0, 0.0).astype(BF16)
    seq_rows = jnp.where(c0 == ((r0 >> 3) & 7) * SLOC + (r0 >> 6) * CHUNK + (r0 & 7), 1.0, 0.0).astype(BF16)
    mt = mask_ref[...].astype(F32).astype(BF16)
    mask_t[...] = dot(mt, seq_order)
    mask_s[...] = dot_t(seq_rows, mt).astype(BF16)

    @pl.loop(0, SLOC)
    def _(i):
        pick = jnp.where(iota((SEQ, LANES), 0) == me * SLOC + i, 1.0, 0.0).astype(BF16)
        keep_row[i] = dot(mask_ref[...].astype(F32).astype(BF16), pick)

    for load in loads:
        load.wait()
    row_vg[...] = jnp.transpose(w_row_in[:, 2 * CM:])
    col_vg[...] = jnp.transpose(w_col_in[:, 2 * CM:])
    tri_vg[0] = jnp.transpose(w_start_in[:, 2 * CZ:])
    tri_vg[1] = jnp.transpose(w_end_in[:, 2 * CZ:])
    norm[...] = jnp.zeros_like(norm)
    norm[0:RES, 0:RES] = dot_t(mt, mt)
    w_full = w_opm_out[...].reshape(OPM, OPM, CZ)
    for a in range(2):
        for c in range(2):
            blk = w_full[16 * a:16 * a + 16, 16 * c:16 * c + 16, :].reshape(256, CZ)
            w2[16 * c:16 * c + 16, 16 * a:16 * a + 16, :] = dot(perm[...], blk).astype(BF16).reshape(16, 16, CZ)
    w2t[...] = dot_t(eye, w2[...].reshape(OPM * OPM, CZ)).astype(BF16)
    cbig[:, RES:, :] = jnp.zeros((OPM, LANES - RES, SEQ), BF16)
    yrow[:, RES:, :] = jnp.zeros((4, LANES - RES, CM), BF16)
    rowqk[:, :, RES:, :] = jnp.zeros((4, 4, LANES - RES, LANES), BF16)
    triqk[:, :, RES:, :] = jnp.zeros((2, RLOC, LANES - RES, LANES), BF16)
    z1[RLOC:, :, :] = jnp.zeros((16 - RLOC, RES, CZ), BF16)
    z3[...] = jnp.zeros_like(z3)

    take_bias(rowb_recv, HM, ROWB)

    def m_src(q):
        return lambda d: msend.at[q, pl.ds(d * RLOC, RLOC)]

    def m_dst(q):
        return lambda s: mrecv.at[q, s]

    def local_copy(src, dst, n):
        return pltpu.make_async_copy(src, dst, local_sem.at[n])

    def row_chunk(q):
        @pl.loop(0, CHUNK // 4)
        def _(blk):
            s0 = q * CHUNK + blk * 4
            x = m_ref[pl.ds(s0, 4)].reshape(4 * RES, CM)
            y = layer_norm(x)
            yrow[:, 0:RES, :] = y.reshape(4, RES, CM)
            qk = dot(y, w_row_in[:, 0:2 * CM]).astype(BF16)
            for t in range(4):
                rowqk[t, :, 0:RES, :] = qk[:, t * LANES:(t + 1) * LANES].reshape(4, RES, LANES)

            def store(u, update):
                m1[s0 + u] = add_residual(m_ref[s0 + u], update[0:RES])
            attend_biased(range(4), 2, lambda u, t: rowqk[t, u], lambda u, t: rowqk[2 + t, u, 0:RES],
                          lambda u: dot_t(row_vg[...], yrow[u]).astype(BF16), bias,
                          lambda u: keep_row[s0 + u], w_row_out[...], store)

        for j in range(RES // 32):
            blk = m1[CHUNK * q:CHUNK * q + CHUNK, 32 * j:32 * j + 32, :].reshape(256, CM)
            msend[q, 32 * j:32 * j + 32] = dot(perm_out[...], blk).reshape(32, CHUNK, CM).astype(BF16)
        start_all(MF + q, m_src(q), m_dst(q))
        local_copy(m_src(q)(me), m_dst(q)(me), q).start()

    def column_projection(q):
        local_copy(m_src(q)(me), m_dst(q)(me), q).wait()
        wait_recv(MF + q, m_dst(q))

        @pl.loop(0, RLOC // 4)
        def _(blk):
            x = jnp.concatenate([mrecv[q, :, blk * 4 + u].astype(F32).reshape(CROWS, CM) for u in range(4)], axis=0)
            for u in range(4):
                mcols[q, blk * 4 + u] = x[u * CROWS:(u + 1) * CROWS].astype(BF16)
            y = layer_norm(x)
            ycol[pl.ds(blk * 4, 4), CROWS * q:CROWS * q + CROWS, :] = y.reshape(4, CROWS, CM)
            qk = dot(y, w_col_in[:, 0:2 * CM]).astype(BF16)
            for t in range(4):
                colqk[t, pl.ds(blk * 4, 4), CROWS * q:CROWS * q + CROWS, :] = (
                    qk[:, t * LANES:(t + 1) * LANES].reshape(4, CROWS, LANES))

    row_chunk(0)
    row_chunk(1)
    row_chunk(2)
    column_projection(0)
    row_chunk(3)
    column_projection(1)
    column_projection(2)
    column_projection(3)

    def mb_start(j):
        start_all(MB, lambda d: mdone.at[d, j], lambda s: mback.at[s * RLOC + j])

    def relay(j):
        for t, twin in enumerate(twins):
            row = crecv.at[twin * RLOC + j]
            remote(row, row, c_send.at[t], c_recv.at[t, j], twin).wait_recv()
            remote(row, row, c_send.at[3 + t], c_pair.at[t], partner).start()

    @pl.loop(0, RLOC // NRES)
    def _(pair):
        lane = iota((SEQ, LANES), 1)
        offset = jnp.zeros((SEQ, LANES), F32)
        for n, part in enumerate(MASKED_SCORE):
            offset = jnp.where(lane == n, part, offset)
        for u in range(NRES):
            pick = jnp.where(iota((RES, LANES), 0) == me * RLOC + pair * NRES + u, 1.0, 0.0).astype(BF16)
            keep = dot(mask_s[...], pick)
            caug[u] = ((1.0 - keep) * offset).astype(BF16)
            keep = keep.astype(BF16)
            for t in range(2):
                ckeep[u, t] = colqk[2 + t, pair * NRES + u] * keep

        def store(u, update):
            j = pair * NRES + u
            mask_row = mask_t[pl.ds(me * RLOC + j, 1), :]
            x = add_residual(mcols[:, j].reshape(SEQ, CM), update)
            both = dot_t(w_opm_in[...], layer_norm(x)).astype(BF16).astype(F32) * mask_row
            left[j] = both[0:OPM].astype(BF16)
            crecv[me * RLOC + j] = both[OPM:].astype(BF16)
            done = x.astype(F32).reshape(NCHUNK, NDEV, CHUNK, CM).astype(BF16)
            for d in range(NDEV):
                mdone[d, j] = done[:, d]

        attend_column(range(NRES), lambda u, t: colqk[t, pair * NRES + u], lambda u, t: ckeep[u, t], lambda u: caug[u],
                      ones[0:LANES], lambda u: dot_t(col_vg[...], ycol[pair * NRES + u]).astype(BF16), w_col_out[...], store)
        for u in range(NRES):
            j = pair * NRES + u
            row = crecv.at[me * RLOC + j]
            for t, twin in enumerate(twins):
                remote(row, row, c_send.at[t], c_recv.at[t, j], twin).start()
            remote(row, row, c_send.at[6], c_pair.at[3], partner).start()

        @pl.when(pair >= LAG // NRES)
        def _():
            for u in range(NRES):
                relay(pair * NRES - LAG + u)

        @pl.when(pair < MB_EARLY // NRES)
        def _():
            for u in range(NRES):
                mb_start(pair * NRES + u)

    for j in range(RLOC - LAG, RLOC):
        relay(j)
    keep_mine = local_copy(mdone.at[me], mback.at[pl.ds(me * RLOC, RLOC)], NCHUNK + 4)
    keep_mine.start()

    def c_rows(s):
        return crecv.at[pl.ds(s * RLOC, RLOC)]

    for t, first in enumerate(twins + (me,)):
        rows = c_rows(first + 1 - 2 * core)
        remote(rows, rows, c_send.at[3 + t], c_pair.at[t], partner).wait_recv()
    for j in range(MB_EARLY, MB_EARLY + 3):
        mb_start(j)
    for c in range(2):
        @pl.loop(0, RES // 16)
        def _(j):
            j0 = pl.multiple_of(j * 16, 16)
            blk = crecv[pl.ds(j0, 16), 16 * c:16 * c + 16, :].reshape(256, SEQ)
            cbig[16 * c:16 * c + 16, pl.ds(j0, 16), :] = dot(perm[...], blk).astype(BF16).reshape(16, 16, SEQ)

    @pl.loop(0, OPM // 2)
    def _(c):
        prod = dot_t(left[...].reshape(RLOC * OPM, SEQ), cbig[pl.ds(2 * c, 2)].reshape(256, SEQ)).astype(BF16)
        for u in range(2):
            outer[:, 2 * c + u] = prod[:, u * LANES:(u + 1) * LANES].reshape(RLOC, OPM, LANES)

    @pl.loop(0, RLOC)
    def _(i):
        update = dot(w2t[...], outer[i].reshape(OPM * OPM, LANES))
        update = update / (1e-3 + norm[pl.ds(me * RLOC + i, 1), :])
        z1[i] = add_residual(z_ref[i], jnp.transpose(update)[0:RES])

    def z_src(buf, group):
        return lambda d: buf.at[group, pl.ds(d * RLOC, RLOC)]

    def z_dst(buf, group):
        return lambda s: buf.at[group, s]

    def triangle(state, result, w_in, which, w_out, recv, stage, late, send, zrecv, moved, zstage, slot):
        @pl.loop(0, RLOC)
        def _(i):
            ynorm[i, 0:RES, :] = layer_norm(state[i])
        send_bias(recv, which, HT, stage)

        @pl.loop(0, RLOC // 4)
        def _(blk):
            y = ynorm[pl.ds(blk * 4, 4), 0:RES, :].reshape(4 * RES, CZ)
            qk = dot(y, w_in[:, 0:2 * CZ]).astype(BF16)
            for t in range(2):
                triqk[t, pl.ds(blk * 4, 4), 0:RES, :] = qk[:, t * LANES:(t + 1) * LANES].reshape(4, RES, LANES)
        take_bias(recv, HT, stage)
        for j in late:
            mb_start(j)

        for group in range(2):
            first = group * ZGROUP

            def store(u, update):
                result[u] = add_residual(state[u], update[0:RES])
            attend_biased(range(first, first + ZGROUP), 1, lambda u, t: triqk[0, u], lambda u, t: triqk[1, u, 0:RES],
                          lambda u: dot_t(tri_vg[which - 1], ynorm[u]).astype(BF16), bias,
                          lambda u: res_keep[...], w_out[...], store)
            for j in range(RES // 32):
                blk = result[first:first + 8, 32 * j:32 * j + 32, :].reshape(256, CZ)
                send[group, 32 * j:32 * j + 32] = dot(perm_out[...], blk).reshape(32, 8, CZ).astype(BF16)
            start_all(zstage + group, z_src(send, group), z_dst(zrecv, group))
            local_copy(z_src(send, group)(me), z_dst(zrecv, group)(me), slot + group).start()

        for group in range(2):
            local_copy(z_src(send, group)(me), z_dst(zrecv, group)(me), slot + group).wait()
            wait_recv(zstage + group, z_dst(zrecv, group))

        @pl.loop(0, RLOC)
        def _(i):
            rows = zrecv[:, :, i].astype(F32).reshape(LANES, CZ).astype(BF16)
            moved[i] = dot(compz[...], rows).astype(BF16)

    triangle(z1, z1, w_start_in, 1, w_start_out, stb_recv, STB, (MB_EARLY + 3,), zs, zr, z2, ZF, NCHUNK)
    triangle(z2, z3, w_end_in, 2, w_end_out, enb_recv, ENB, (), zs2, zr2, z_out, ZB, NCHUNK + 2)

    wait_recv(MB, lambda s: mback.at[pl.ds(s * RLOC, RLOC)])
    keep_mine.wait()

    wait_send(ROWB, lambda d: bias_rows(rowb_recv)(me))
    for q in range(NCHUNK):
        wait_send(MF + q, m_src(q))
    wait_send(MB, lambda d: mdone.at[d])
    for t in range(7):
        rows = c_rows(me if t in (0, 1, 2, 6) else twins[t - 3])
        remote(rows, rows, c_send.at[t], c_pair.at[0], partner).wait_send()
    wait_send(STB, lambda d: bias_rows(stb_recv)(me))
    for group in range(2):
        wait_send(ZF + group, z_src(zs, group))
    wait_send(ENB, lambda d: bias_rows(enb_recv)(me))
    for group in range(2):
        wait_send(ZB + group, z_src(zs2, group))


def finish_kernel(m_home, z_new, m_out, z_out, perm_in):
    @pl.when(pl.program_id(0) == 0)
    def _():
        r, c = iota((256, 256), 0), iota((256, 256), 1)
        perm_in[...] = jnp.where(((r >> 5) == (c & 7)) & ((r & 31) == (c >> 3)), 1.0, 0.0).astype(BF16)
        z_out[...] = z_new[...]

    for j in range(RES // 32):
        blk = m_home[32 * j:32 * j + 32, 0].astype(F32).reshape(256, CM).astype(BF16)
        m_out[:, 32 * j:32 * j + 32, :] = dot(perm_in[...], blk).astype(BF16).reshape(CHUNK, 32, CM)


def solution(mesh):
    rows = P(('data', 'chip', 'dap'))
    in_specs = (rows, rows, P('data'), P('data')) + (P(),) * 13
    vmem = pl.BlockSpec(memory_space=pltpu.VMEM)
    hbm = pl.BlockSpec(memory_space=pl.ANY)

    def per_device(m_blk, z_blk, msa_mask, res_mask, w_row_in, w_row_bias, w_row_out, w_col_in, w_col_out,
                   w_opm_in, w_opm_out, w_start_in, w_start_bias, w_start_out, w_end_in, w_end_bias, w_end_out):
        loaded = [m_blk, w_row_in, w_row_out, w_col_in, w_col_out, w_opm_out, w_start_in, w_start_out, w_end_in, w_end_out]
        scratch = [pltpu.VMEM(x.shape, x.dtype) for x in loaded] + [
            pltpu.VMEM((256, 256), BF16),
            pltpu.VMEM((256, 256), BF16),
            pltpu.VMEM((RES, LANES), BF16),
            pltpu.VMEM((RES, LANES), BF16),
            pltpu.VMEM((LANES, LANES), BF16),
            pltpu.VMEM((SLOC, RES, LANES), F32),
            pltpu.VMEM((RES, SEQ), F32),
            pltpu.VMEM((SEQ, RES), BF16),
            pltpu.VMEM((LANES, LANES), F32),
            pltpu.VMEM((RES, LANES), F32),
            pltpu.VMEM((3, 8, CZ), F32),
            pltpu.VMEM((16, 8, LANES), F32),
            pltpu.VMEM((HM, RES, LANES), F32),
            pltpu.VMEM((NDEV, HM, 16, LANES), BF16),
            pltpu.VMEM((NDEV, HT, 16, LANES), BF16),
            pltpu.VMEM((NDEV, HT, 16, LANES), BF16),
            pltpu.VMEM((2 * CM, CM), BF16),
            pltpu.VMEM((2 * CM, CM), BF16),
            pltpu.VMEM((2, 2 * CZ, CZ), BF16),
            pltpu.VMEM((4, LANES, CM), BF16),
            pltpu.VMEM((4, 4, LANES, LANES), BF16),
            pltpu.VMEM((2, RLOC, LANES, LANES), BF16),
            pltpu.VMEM((SLOC, RES, CM), BF16),
            pltpu.VMEM((NCHUNK, RES, CHUNK, CM), BF16),
            pltpu.VMEM((NCHUNK, NDEV, RLOC, CHUNK, CM), BF16),
            pltpu.VMEM((NCHUNK, RLOC, CROWS, CM), BF16),
            pltpu.VMEM((NDEV, RLOC, NCHUNK, CHUNK, CM), BF16),
            pltpu.VMEM((RLOC, SEQ, CM), BF16),
            pltpu.VMEM((4, RLOC, SEQ, LANES), BF16),
            pltpu.VMEM((NRES, SEQ, LANES), BF16),
            pltpu.VMEM((NRES, 2, SEQ, LANES), BF16),
            pltpu.VMEM((SEQ, LANES), BF16),
            pltpu.VMEM((RLOC, OPM, SEQ), BF16),
            pltpu.VMEM((RES, OPM, SEQ), BF16),
            pltpu.VMEM((OPM, LANES, SEQ), BF16),
            pltpu.VMEM((RLOC, OPM, OPM, LANES), BF16),
            pltpu.VMEM((OPM, OPM, CZ), BF16),
            pltpu.VMEM((CZ, OPM * OPM), BF16),
            pltpu.VMEM((RLOC, LANES, CZ), BF16),
            pltpu.VMEM((16, RES, CZ), BF16),
            pltpu.VMEM((2, RES, 8, CZ), BF16),
            pltpu.VMEM((2, NDEV, RLOC, 8, CZ), BF16),
            pltpu.VMEM((RLOC, RES, CZ), BF16),
            pltpu.VMEM((16, RES, CZ), BF16),
            pltpu.VMEM((2, RES, 8, CZ), BF16),
            pltpu.VMEM((2, NDEV, RLOC, 8, CZ), BF16),
            pltpu.SemaphoreType.DMA((NSTAGE, NDEV)),
            pltpu.SemaphoreType.DMA((NSTAGE, NDEV)),
            pltpu.SemaphoreType.DMA((NCHUNK + 5,)),
            pltpu.SemaphoreType.DMA((10,)),
            pltpu.SemaphoreType.DMA((7,)),
            pltpu.SemaphoreType.DMA((3, RLOC)),
            pltpu.SemaphoreType.DMA((4,)),
        ]
        m_home, z_new = pl.pallas_call(
            block_kernel,
            name='evoformer_block',
            out_shape=(jax.ShapeDtypeStruct((RES, NCHUNK, CHUNK, CM), BF16), jax.ShapeDtypeStruct(z_blk.shape, BF16)),
            in_specs=[hbm, vmem, vmem, vmem, hbm, vmem, hbm, hbm, hbm, vmem, hbm, hbm, vmem, hbm, hbm, vmem, hbm],
            out_specs=(hbm, vmem),
            scratch_shapes=scratch,
            compiler_params=pltpu.CompilerParams(collective_id=0, has_side_effects=True,
                                                 vmem_limit_bytes=56 * 1024 * 1024),
        )(m_blk, z_blk, msa_mask.T, res_mask.reshape(1, RES), w_row_in, w_row_bias.T, w_row_out, w_col_in, w_col_out,
          w_opm_in.T, w_opm_out, w_start_in, w_start_bias.T, w_start_out, w_end_in, w_end_bias.T, w_end_out)
        whole = pl.BlockSpec((RLOC, RES, CZ), lambda q: (0, 0, 0))
        return pl.pallas_call(
            finish_kernel,
            name='finish',
            grid=(NCHUNK,),
            out_shape=(jax.ShapeDtypeStruct(m_blk.shape, BF16), jax.ShapeDtypeStruct(z_blk.shape, BF16)),
            in_specs=[pl.BlockSpec((RES, 1, CHUNK, CM), lambda q: (0, q, 0, 0)), whole],
            out_specs=(pl.BlockSpec((CHUNK, RES, CM), lambda q: (q, 0, 0)), whole),
            scratch_shapes=[pltpu.VMEM((256, 256), BF16)],
            compiler_params=pltpu.CompilerParams(dimension_semantics=('arbitrary',)),
        )(m_home, z_new)

    return jax.shard_map(per_device, mesh=mesh, in_specs=in_specs, out_specs=(rows, rows), check_vma=False)
```

```python
import functools

import jax
import jax.numpy as jnp
import numpy as np
from jax import lax
from jax.experimental import pallas as pl
from jax.experimental.pallas import tpu as pltpu
from jax.sharding import PartitionSpec as P

BF16 = jnp.bfloat16
F32 = jnp.float32
MESH = pl.DeviceIdType.MESH
NDEV = 8
SEQ, RES, CM, CZ = 256, 96, 256, 128
SLOC, RLOC = SEQ // NDEV, RES // NDEV
HM, HT, HD, OPM = 8, 4, 32, 32
LANES = 128
MASKED = -1e9
SCALE = HD ** -0.5


def bf16_parts(value, n):
    parts = []
    for _ in range(n):
        parts.append(float(np.asarray(value - sum(parts), np.float32).astype(BF16)))
    return parts


MASKED_SCORE = bf16_parts(MASKED / SCALE, 3)

ROWB, MF, MB, STB, ZF, ENB, ZB = 0, 1, 5, 6, 7, 9, 10
NSTAGE = 12
ZGROUP = RLOC // 2
CHUNK = 8
NCHUNK = SLOC // CHUNK
CROWS = NDEV * CHUNK
LAG = 4
MB_EARLY = 10
NRES = 2


def dot(a, b):
    return jnp.dot(a, b, preferred_element_type=F32)


def dot_t(a, b):
    return lax.dot_general(a, b, (((1,), (1,)), ((), ())), preferred_element_type=F32)


def iota(shape, dim):
    return lax.broadcasted_iota(jnp.int32, shape, dim)


def layer_norm(x):
    values = x.astype(F32)
    centred = values - jnp.mean(values, axis=-1, keepdims=True)
    variance = jnp.mean(centred * centred, axis=-1, keepdims=True)
    return (centred * lax.rsqrt(variance + 1e-5)).astype(BF16)


def add_residual(state, update):
    return (state.astype(F32) + update).astype(BF16)


def head_masks():
    lane = iota((16, LANES), 1)
    return [jnp.where((lane >= h * HD) & (lane < (h + 1) * HD), 1.0, 0.0).astype(BF16) for h in range(LANES // HD)]


def only_head(x, mask):
    return x * jnp.concatenate([mask] * (x.shape[0] // 16), axis=0)


def dot_tl(a, b):
    return lax.dot_general(a, b, (((0,), (0,)), ((), ())), preferred_element_type=F32)


def softmax_keys(logits):
    weights = jnp.exp(logits - jnp.max(logits, axis=0, keepdims=True))
    return (weights * (1.0 / jnp.sum(weights, axis=0, keepdims=True))).astype(BF16)


def pipeline(items, first, middle, last, finish, ahead=1, behind=1):
    count = len(items)
    opened, ready = {}, {}
    for n in range(-ahead, count + behind + 1):
        if n + ahead < count:
            opened[n + ahead] = first(items[n + ahead])
        if 0 <= n < count:
            ready[n] = middle(items[n], opened.pop(n))
        if 0 <= n - behind < count:
            last(items[n - behind], ready.pop(n - behind))
        if 0 <= n - behind - 1 < count:
            finish(items[n - behind - 1])


def attend_biased(rows, tiles, q_of, k_of, vg_of, bias_ref, keep_of, w_out, store):
    masks = head_masks()
    each = len(masks)
    vgs = {}
    mixed = {u: [] for u in rows}

    def first(item):
        u, t = item
        if t == 0:
            vgs[u] = vg_of(u)
        k = k_of(u, t)
        return dot_t(jnp.concatenate([only_head(k, mask) for mask in masks], axis=0), q_of(u, t))

    def middle(item, scores):
        u, t = item
        keep = keep_of(u) != 0.0
        return [softmax_keys(jnp.where(keep, scores[n * RES:(n + 1) * RES] * SCALE + bias_ref[each * t + n], MASKED))
                for n in range(each)]

    def last(item, probs):
        u, t = item
        for n in range(each):
            h = each * t + n
            padded = jnp.concatenate([probs[n], jnp.zeros((LANES - RES, LANES), BF16)], axis=0)
            mixed[u].append(dot(vgs[u][h * HD:(h + 1) * HD], padded))

    def finish(item):
        u, t = item
        if t == tiles - 1:
            gates = jax.nn.sigmoid(vgs[u][tiles * LANES:].astype(F32))
            store(u, dot_tl((jnp.concatenate(mixed[u], axis=0) * gates).astype(BF16), w_out))

    pipeline([(u, t) for u in rows for t in range(tiles)], first, middle, last, finish)


def attend_column(residues, q_of, k_of, aug_of, ones, vg_of, w_out, store):
    masks = head_masks()
    each = len(masks)
    halves = SEQ // LANES
    vgs, keys = {}, {}
    mixed = {(u, half): [] for u in residues for half in range(halves)}

    def first(item):
        u, h, half = item
        if (h, half) == (0, 0):
            vgs[u] = vg_of(u)
        if half == 0:
            keys[u, h] = jnp.concatenate([only_head(k_of(u, h // each), masks[h % each]), aug_of(u)], axis=1)
        q = q_of(u, h // each)[half * LANES:(half + 1) * LANES]
        return dot_t(keys[u, h], jnp.concatenate([q, ones], axis=1))

    def middle(item, scores):
        return softmax_keys(scores * SCALE)

    def last(item, probs):
        u, h, half = item
        mixed[u, half].append(dot(vgs[u][h * HD:(h + 1) * HD], probs))

    def finish(item):
        u, h, half = item
        if (h, half) == (HM - 1, halves - 1):
            gates = jax.nn.sigmoid(vgs[u][CM:].astype(F32))
            out = jnp.concatenate([jnp.concatenate(mixed[u, n], axis=0) for n in range(halves)], axis=1)
            store(u, dot_tl((out * gates).astype(BF16), w_out))

    pipeline([(u, h, half) for u in residues for h in range(HM) for half in range(halves)], first, middle, last, finish, 4, 2)


def block_kernel(m_any, z_ref, mask_ref, res_ref, row_in_any, w_row_bias, row_out_any, col_in_any, col_out_any,
                 w_opm_in, opm_out_any, start_in_any, w_start_bias, start_out_any, end_in_any, w_end_bias, end_out_any,
                 mback, z_out,
                 m_ref, w_row_in, w_row_out, w_col_in, w_col_out, w_opm_out, w_start_in, w_start_out, w_end_in, w_end_out,
                 perm, perm_out, comp, compz, hperm, keep_row, mask_t, mask_s, norm, res_keep, wbt, bcol, bias,
                 rowb_recv, stb_recv, enb_recv, row_vg, col_vg, tri_vg, yrow, rowqk, triqk, m1, msend, mrecv, mcols, mdone,
                 ycol, colqk, caug, ckeep, ones,
                 left, crecv, cbig, outer, w2, w2t, ynorm, z1, zs, zr, z2, z3, zs2, zr2,
                 send_sem, recv_sem, local_sem, load_sem, c_send, c_recv, c_pair):
    data = lax.axis_index('data')
    me = lax.axis_index('chip') * 4 + lax.axis_index('dap')
    core, chip_x, chip_y = lax.rem(me, 2), lax.rem(me // 2, 2), me // 4
    partner = me + 1 - 2 * core
    to_x, to_y = 2 - 4 * chip_x, 4 - 8 * chip_y
    twins = (me + to_x + to_y, me + to_x, me + to_y)

    def device(d):
        return (data, d // 4, lax.rem(d, 4))

    def peer(r):
        return lax.rem(me + r, NDEV)

    def source(r):
        return lax.rem(me + NDEV - r, NDEV)

    def remote(src, dst, send, recv, d):
        return pltpu.make_async_remote_copy(src_ref=src, dst_ref=dst, send_sem=send, recv_sem=recv,
                                            device_id=device(d), device_id_type=MESH)

    def start_all(stage, src_of, dst_of):
        for r in range(1, NDEV):
            d = peer(r)
            remote(src_of(d), dst_of(me), send_sem.at[stage, r], recv_sem.at[stage, r], d).start()

    def wait_recv(stage, dst_of):
        for r in range(1, NDEV):
            dst = dst_of(source(r))
            remote(dst, dst, send_sem.at[stage, r], recv_sem.at[stage, r], peer(r)).wait_recv()

    def wait_send(stage, src_of):
        for r in range(1, NDEV):
            src = src_of(peer(r))
            remote(src, src, send_sem.at[stage, r], recv_sem.at[stage, r], peer(r)).wait_send()

    barrier = pltpu.get_barrier_semaphore()
    for r in range(1, NDEV):
        pl.semaphore_signal(barrier, inc=1, device_id=device(peer(r)), device_id_type=MESH)

    loads = [pltpu.make_async_copy(src, dst, load_sem.at[n]) for n, (src, dst) in enumerate((
        (row_in_any, w_row_in), (m_any, m_ref), (row_out_any, w_row_out), (col_in_any, w_col_in), (opm_out_any, w_opm_out),
        (start_in_any, w_start_in), (end_in_any, w_end_in), (col_out_any, w_col_out), (start_out_any, w_start_out),
        (end_out_any, w_end_out)))]
    for load in loads:
        load.start()

    r0, c0 = iota((256, 256), 0), iota((256, 256), 1)
    perm[...] = jnp.where(((r0 >> 4) == (c0 & 15)) & ((r0 & 15) == (c0 >> 4)), 1.0, 0.0).astype(BF16)
    perm_out[...] = jnp.where(((r0 >> 3) == (c0 & 31)) & ((r0 & 7) == (c0 >> 5)), 1.0, 0.0).astype(BF16)
    r1, c1 = iota((RES, LANES), 0), iota((RES, LANES), 1)
    comp[...] = jnp.where(((c1 & 15) < RLOC) & (r1 == (c1 >> 4) * RLOC + (c1 & 15)), 1.0, 0.0).astype(BF16)
    compz[...] = jnp.where(((c1 & 7) < ZGROUP) & (r1 == ((c1 >> 3) & 7) * RLOC + (c1 >> 6) * ZGROUP + (c1 & 7)),
                           1.0, 0.0).astype(BF16)
    r2, c2 = iota((LANES, LANES), 0), iota((LANES, LANES), 1)
    hperm[...] = jnp.where(((r2 >> 4) == (c2 & 7)) & ((r2 & 15) == (c2 >> 3)), 1.0, 0.0).astype(BF16)
    eye = jnp.where(r2 == c2, 1.0, 0.0).astype(BF16)
    ones[...] = jnp.where(iota((SEQ, LANES), 1) < len(MASKED_SCORE), 1.0, 0.0).astype(BF16)
    bcol[...] = jnp.zeros_like(bcol)
    wbt[...] = jnp.zeros_like(wbt)
    for n, w in enumerate((w_row_bias, w_start_bias, w_end_bias)):
        wbt[n, 0:w.shape[0], :] = w[...].astype(F32)

    def send_bias(recv, which, heads, stage):
        weights = wbt[which].astype(BF16)

        for i in range(RLOC):
            bcol[i] = dot_t(weights, ynorm[i])

        mine = dot(hperm[0:heads * 16, :], bcol[...].reshape(LANES, LANES).astype(BF16)).astype(BF16)
        recv[me] = mine.reshape(heads, 16, LANES)
        start_all(stage, lambda d: recv.at[me], lambda s: recv.at[s])

    def bias_rows(recv):
        return lambda s: recv.at[s]

    def take_bias(recv, heads, stage):
        wait_recv(stage, bias_rows(recv))
        for h in range(heads):
            rows = dot(comp[...], recv[:, h].reshape(LANES, LANES)).astype(BF16)
            bias[h] = dot_t(eye, jnp.concatenate([rows, jnp.zeros((LANES - RES, LANES), BF16)], axis=0))[0:RES]

    ynorm[:, RES:, :] = jnp.zeros((RLOC, LANES - RES, CZ), BF16)

    ynorm[:, 0:RES, :] = layer_norm(z_ref[...].reshape(RLOC * RES, CZ)).reshape(RLOC, RES, CZ)

    pl.semaphore_wait(barrier, NDEV - 1)
    send_bias(rowb_recv, 0, HM, ROWB)

    res_keep[...] = dot((eye[0:RES, 0:RES].astype(F32) * res_ref[...].astype(F32)).astype(BF16),
                        jnp.ones((RES, LANES), BF16))
    seq_order = jnp.where(r0 == ((c0 >> 3) & 7) * SLOC + (c0 >> 6) * CHUNK + (c0 & 7), 1.0, 0.0).astype(BF16)
    seq_rows = jnp.where(c0 == ((r0 >> 3) & 7) * SLOC + (r0 >> 6) * CHUNK + (r0 & 7), 1.0, 0.0).astype(BF16)
    mt = mask_ref[...].astype(F32).astype(BF16)
    mask_t[...] = dot(mt, seq_order)
    mask_s[...] = dot_t(seq_rows, mt).astype(BF16)

    @pl.loop(0, SLOC // 4)
    def _(blk):
        for u in range(4):
            pick = jnp.where(iota((SEQ, LANES), 0) == me * SLOC + blk * 4 + u, 1.0, 0.0).astype(BF16)
            keep_row[blk * 4 + u] = dot(mask_ref[...].astype(F32).astype(BF16), pick)

    for load in loads:
        load.wait()
    row_vg[...] = jnp.transpose(w_row_in[:, 2 * CM:])
    col_vg[...] = jnp.transpose(w_col_in[:, 2 * CM:])
    tri_vg[0] = jnp.transpose(w_start_in[:, 2 * CZ:])
    tri_vg[1] = jnp.transpose(w_end_in[:, 2 * CZ:])
    norm[...] = jnp.zeros_like(norm)
    norm[0:RES, 0:RES] = dot_t(mt, mt)
    w_full = w_opm_out[...].reshape(OPM, OPM, CZ)
    for a in range(2):
        for c in range(2):
            blk = w_full[16 * a:16 * a + 16, 16 * c:16 * c + 16, :].reshape(256, CZ)
            w2[16 * c:16 * c + 16, 16 * a:16 * a + 16, :] = dot(perm[...], blk).astype(BF16).reshape(16, 16, CZ)
    w2t[...] = dot_t(eye, w2[...].reshape(OPM * OPM, CZ)).astype(BF16)
    cbig[:, RES:, :] = jnp.zeros((OPM, LANES - RES, SEQ), BF16)
    yrow[:, RES:, :] = jnp.zeros((4, LANES - RES, CM), BF16)
    rowqk[:, :, RES:, :] = jnp.zeros((4, 4, LANES - RES, LANES), BF16)
    triqk[:, :, RES:, :] = jnp.zeros((2, RLOC, LANES - RES, LANES), BF16)
    z1[RLOC:, :, :] = jnp.zeros((16 - RLOC, RES, CZ), BF16)
    z3[...] = jnp.zeros_like(z3)

    take_bias(rowb_recv, HM, ROWB)

    def m_src(q):
        return lambda d: msend.at[q, pl.ds(d * RLOC, RLOC)]

    def m_dst(q):
        return lambda s: mrecv.at[q, s]

    def local_copy(src, dst, n):
        return pltpu.make_async_copy(src, dst, local_sem.at[n])

    def row_chunk(q):
        @pl.loop(0, CHUNK // 4)
        def _(blk):
            s0 = q * CHUNK + blk * 4
            x = m_ref[pl.ds(s0, 4)].reshape(4 * RES, CM)
            y = layer_norm(x)
            yrow[:, 0:RES, :] = y.reshape(4, RES, CM)
            qk = dot(y, w_row_in[:, 0:2 * CM]).astype(BF16)
            for t in range(4):
                rowqk[t, :, 0:RES, :] = qk[:, t * LANES:(t + 1) * LANES].reshape(4, RES, LANES)

            def store(u, update):
                m1[s0 + u] = add_residual(m_ref[s0 + u], update[0:RES])
            attend_biased(range(4), 2, lambda u, t: rowqk[t, u], lambda u, t: rowqk[2 + t, u, 0:RES],
                          lambda u: dot_t(row_vg[...], yrow[u]).astype(BF16), bias,
                          lambda u: keep_row[s0 + u], w_row_out[...], store)

        for j in range(RES // 32):
            blk = m1[CHUNK * q:CHUNK * q + CHUNK, 32 * j:32 * j + 32, :].reshape(256, CM)
            msend[q, 32 * j:32 * j + 32] = dot(perm_out[...], blk).reshape(32, CHUNK, CM).astype(BF16)
        start_all(MF + q, m_src(q), m_dst(q))
        local_copy(m_src(q)(me), m_dst(q)(me), q).start()

    def column_projection(q):
        local_copy(m_src(q)(me), m_dst(q)(me), q).wait()
        wait_recv(MF + q, m_dst(q))

        for blk in range(RLOC // 4):
            x = jnp.concatenate([mrecv[q, :, blk * 4 + u].astype(F32).reshape(CROWS, CM) for u in range(4)], axis=0)
            for u in range(4):
                mcols[q, blk * 4 + u] = x[u * CROWS:(u + 1) * CROWS].astype(BF16)
            y = layer_norm(x)
            ycol[blk * 4:blk * 4 + 4, CROWS * q:CROWS * q + CROWS, :] = y.reshape(4, CROWS, CM)
            qk = dot(y, w_col_in[:, 0:2 * CM]).astype(BF16)
            for t in range(4):
                colqk[t, blk * 4:blk * 4 + 4, CROWS * q:CROWS * q + CROWS, :] = (
                    qk[:, t * LANES:(t + 1) * LANES].reshape(4, CROWS, LANES))

    row_chunk(0)
    row_chunk(1)
    row_chunk(2)
    column_projection(0)
    row_chunk(3)
    column_projection(1)
    column_projection(2)
    column_projection(3)

    def mb_start(j):
        start_all(MB, lambda d: mdone.at[d, j], lambda s: mback.at[s * RLOC + j])

    def relay(j):
        for t, twin in enumerate(twins):
            row = crecv.at[twin * RLOC + j]
            remote(row, row, c_send.at[t], c_recv.at[t, j], twin).wait_recv()
            remote(row, row, c_send.at[3 + t], c_pair.at[t], partner).start()

    @pl.loop(0, RLOC // NRES)
    def _(pair):
        lane = iota((SEQ, LANES), 1)
        offset = jnp.zeros((SEQ, LANES), F32)
        for n, part in enumerate(MASKED_SCORE):
            offset = jnp.where(lane == n, part, offset)
        for u in range(NRES):
            pick = jnp.where(iota((RES, LANES), 0) == me * RLOC + pair * NRES + u, 1.0, 0.0).astype(BF16)
            keep = dot(mask_s[...], pick)
            caug[u] = ((1.0 - keep) * offset).astype(BF16)
            keep = keep.astype(BF16)
            for t in range(2):
                ckeep[u, t] = colqk[2 + t, pair * NRES + u] * keep

        def store(u, update):
            j = pair * NRES + u
            mask_row = mask_t[pl.ds(me * RLOC + j, 1), :]
            x = add_residual(mcols[:, j].reshape(SEQ, CM), update)
            both = dot_t(w_opm_in[...], layer_norm(x)).astype(BF16).astype(F32) * mask_row
            left[j] = both[0:OPM].astype(BF16)
            crecv[me * RLOC + j] = both[OPM:].astype(BF16)
            done = x.astype(F32).reshape(NCHUNK, NDEV, CHUNK, CM).astype(BF16)
            for d in range(NDEV):
                mdone[d, j] = done[:, d]

        attend_column(range(NRES), lambda u, t: colqk[t, pair * NRES + u], lambda u, t: ckeep[u, t], lambda u: caug[u],
                      ones[0:LANES], lambda u: dot_t(col_vg[...], ycol[pair * NRES + u]).astype(BF16), w_col_out[...], store)
        for u in range(NRES):
            j = pair * NRES + u
            row = crecv.at[me * RLOC + j]
            for t, twin in enumerate(twins):
                remote(row, row, c_send.at[t], c_recv.at[t, j], twin).start()
            remote(row, row, c_send.at[6], c_pair.at[3], partner).start()

        @pl.when(pair >= LAG // NRES)
        def _():
            for u in range(NRES):
                relay(pair * NRES - LAG + u)

        @pl.when(pair < MB_EARLY // NRES)
        def _():
            for u in range(NRES):
                mb_start(pair * NRES + u)

    for j in range(RLOC - LAG, RLOC):
        relay(j)
    keep_mine = local_copy(mdone.at[me], mback.at[pl.ds(me * RLOC, RLOC)], NCHUNK + 4)
    keep_mine.start()

    def c_rows(s):
        return crecv.at[pl.ds(s * RLOC, RLOC)]

    for t, first in enumerate(twins + (me,)):
        rows = c_rows(first + 1 - 2 * core)
        remote(rows, rows, c_send.at[3 + t], c_pair.at[t], partner).wait_recv()
    for j in range(MB_EARLY, RLOC):
        mb_start(j)
    for c in range(2):
        for j0 in range(0, RES, 16):
            blk = crecv[j0:j0 + 16, 16 * c:16 * c + 16, :].reshape(256, SEQ)
            cbig[16 * c:16 * c + 16, j0:j0 + 16, :] = dot(perm[...], blk).astype(BF16).reshape(16, 16, SEQ)

    @pl.loop(0, OPM // 8)
    def _(blk):
        for c2 in range(4):
            c = blk * 4 + c2
            prod = dot_t(left[...].reshape(RLOC * OPM, SEQ), cbig[pl.ds(2 * c, 2)].reshape(256, SEQ)).astype(BF16)
            for u in range(2):
                outer[:, 2 * c + u] = prod[:, u * LANES:(u + 1) * LANES].reshape(RLOC, OPM, LANES)

    @pl.loop(0, 2)
    def _(half):
        for u in range(RLOC // 2):
            i = half * (RLOC // 2) + u
            update = dot(w2t[...], outer[i].reshape(OPM * OPM, LANES))
            update = update / (1e-3 + norm[pl.ds(me * RLOC + i, 1), :])
            z1[i] = add_residual(z_ref[i], jnp.transpose(update)[0:RES])

    def z_src(buf, group):
        return lambda d: buf.at[group, pl.ds(d * RLOC, RLOC)]

    def z_dst(buf, group):
        return lambda s: buf.at[group, s]

    def triangle(state, result, w_in, which, w_out, recv, stage, late, send, zrecv, moved, zstage, slot):
        ynorm[:, 0:RES, :] = layer_norm(state[0:RLOC].reshape(RLOC * RES, CZ)).reshape(RLOC, RES, CZ)
        send_bias(recv, which, HT, stage)

        for blk in range(RLOC // 4):
            y = ynorm[blk * 4:blk * 4 + 4, 0:RES, :].reshape(4 * RES, CZ)
            qk = dot(y, w_in[:, 0:2 * CZ]).astype(BF16)
            for t in range(2):
                triqk[t, blk * 4:blk * 4 + 4, 0:RES, :] = qk[:, t * LANES:(t + 1) * LANES].reshape(4, RES, LANES)
        take_bias(recv, HT, stage)
        for j in late:
            mb_start(j)

        for group in range(2):
            first = group * ZGROUP

            def store(u, update):
                result[u] = add_residual(state[u], update[0:RES])
            attend_biased(range(first, first + ZGROUP), 1, lambda u, t: triqk[0, u], lambda u, t: triqk[1, u, 0:RES],
                          lambda u: dot_t(tri_vg[which - 1], ynorm[u]).astype(BF16), bias,
                          lambda u: res_keep[...], w_out[...], store)
            for j in range(RES // 32):
                blk = result[first:first + 8, 32 * j:32 * j + 32, :].reshape(256, CZ)
                send[group, 32 * j:32 * j + 32] = dot(perm_out[...], blk).reshape(32, 8, CZ).astype(BF16)
            start_all(zstage + group, z_src(send, group), z_dst(zrecv, group))
            local_copy(z_src(send, group)(me), z_dst(zrecv, group)(me), slot + group).start()

        for group in range(2):
            local_copy(z_src(send, group)(me), z_dst(zrecv, group)(me), slot + group).wait()
            wait_recv(zstage + group, z_dst(zrecv, group))

        for i in range(RLOC):
            rows = zrecv[:, :, i].astype(F32).reshape(LANES, CZ).astype(BF16)
            moved[i] = dot(compz[...], rows).astype(BF16)

    triangle(z1, z1, w_start_in, 1, w_start_out, stb_recv, STB, (), zs, zr, z2, ZF, NCHUNK)
    triangle(z2, z3, w_end_in, 2, w_end_out, enb_recv, ENB, (), zs2, zr2, z_out, ZB, NCHUNK + 2)

    wait_recv(MB, lambda s: mback.at[pl.ds(s * RLOC, RLOC)])
    keep_mine.wait()

    wait_send(ROWB, lambda d: bias_rows(rowb_recv)(me))
    for q in range(NCHUNK):
        wait_send(MF + q, m_src(q))
    wait_send(MB, lambda d: mdone.at[d])
    for t in range(7):
        rows = c_rows(me if t in (0, 1, 2, 6) else twins[t - 3])
        remote(rows, rows, c_send.at[t], c_pair.at[0], partner).wait_send()
    wait_send(STB, lambda d: bias_rows(stb_recv)(me))
    for group in range(2):
        wait_send(ZF + group, z_src(zs, group))
    wait_send(ENB, lambda d: bias_rows(enb_recv)(me))
    for group in range(2):
        wait_send(ZB + group, z_src(zs2, group))


def finish_kernel(m_home, z_new, m_out, z_out, perm_in):
    @pl.when(pl.program_id(0) == 0)
    def _():
        r, c = iota((256, 256), 0), iota((256, 256), 1)
        perm_in[...] = jnp.where(((r >> 5) == (c & 7)) & ((r & 31) == (c >> 3)), 1.0, 0.0).astype(BF16)
        z_out[...] = z_new[...]

    for j in range(RES // 32):
        blk = m_home[32 * j:32 * j + 32, 0].astype(F32).reshape(256, CM).astype(BF16)
        m_out[:, 32 * j:32 * j + 32, :] = dot(perm_in[...], blk).astype(BF16).reshape(CHUNK, 32, CM)


def solution(mesh):
    rows = P(('data', 'chip', 'dap'))
    in_specs = (rows, rows, P('data'), P('data')) + (P(),) * 13
    vmem = pl.BlockSpec(memory_space=pltpu.VMEM)
    hbm = pl.BlockSpec(memory_space=pl.ANY)

    def per_device(m_blk, z_blk, msa_mask, res_mask, w_row_in, w_row_bias, w_row_out, w_col_in, w_col_out,
                   w_opm_in, w_opm_out, w_start_in, w_start_bias, w_start_out, w_end_in, w_end_bias, w_end_out):
        loaded = [m_blk, w_row_in, w_row_out, w_col_in, w_col_out, w_opm_out, w_start_in, w_start_out, w_end_in, w_end_out]
        scratch = [pltpu.VMEM(x.shape, x.dtype) for x in loaded] + [
            pltpu.VMEM((256, 256), BF16),
            pltpu.VMEM((256, 256), BF16),
            pltpu.VMEM((RES, LANES), BF16),
            pltpu.VMEM((RES, LANES), BF16),
            pltpu.VMEM((LANES, LANES), BF16),
            pltpu.VMEM((SLOC, RES, LANES), F32),
            pltpu.VMEM((RES, SEQ), F32),
            pltpu.VMEM((SEQ, RES), BF16),
            pltpu.VMEM((LANES, LANES), F32),
            pltpu.VMEM((RES, LANES), F32),
            pltpu.VMEM((3, 8, CZ), F32),
            pltpu.VMEM((16, 8, LANES), F32),
            pltpu.VMEM((HM, RES, LANES), F32),
            pltpu.VMEM((NDEV, HM, 16, LANES), BF16),
            pltpu.VMEM((NDEV, HT, 16, LANES), BF16),
            pltpu.VMEM((NDEV, HT, 16, LANES), BF16),
            pltpu.VMEM((2 * CM, CM), BF16),
            pltpu.VMEM((2 * CM, CM), BF16),
            pltpu.VMEM((2, 2 * CZ, CZ), BF16),
            pltpu.VMEM((4, LANES, CM), BF16),
            pltpu.VMEM((4, 4, LANES, LANES), BF16),
            pltpu.VMEM((2, RLOC, LANES, LANES), BF16),
            pltpu.VMEM((SLOC, RES, CM), BF16),
            pltpu.VMEM((NCHUNK, RES, CHUNK, CM), BF16),
            pltpu.VMEM((NCHUNK, NDEV, RLOC, CHUNK, CM), BF16),
            pltpu.VMEM((NCHUNK, RLOC, CROWS, CM), BF16),
            pltpu.VMEM((NDEV, RLOC, NCHUNK, CHUNK, CM), BF16),
            pltpu.VMEM((RLOC, SEQ, CM), BF16),
            pltpu.VMEM((4, RLOC, SEQ, LANES), BF16),
            pltpu.VMEM((NRES, SEQ, LANES), BF16),
            pltpu.VMEM((NRES, 2, SEQ, LANES), BF16),
            pltpu.VMEM((SEQ, LANES), BF16),
            pltpu.VMEM((RLOC, OPM, SEQ), BF16),
            pltpu.VMEM((RES, OPM, SEQ), BF16),
            pltpu.VMEM((OPM, LANES, SEQ), BF16),
            pltpu.VMEM((RLOC, OPM, OPM, LANES), BF16),
            pltpu.VMEM((OPM, OPM, CZ), BF16),
            pltpu.VMEM((CZ, OPM * OPM), BF16),
            pltpu.VMEM((RLOC, LANES, CZ), BF16),
            pltpu.VMEM((16, RES, CZ), BF16),
            pltpu.VMEM((2, RES, 8, CZ), BF16),
            pltpu.VMEM((2, NDEV, RLOC, 8, CZ), BF16),
            pltpu.VMEM((RLOC, RES, CZ), BF16),
            pltpu.VMEM((16, RES, CZ), BF16),
            pltpu.VMEM((2, RES, 8, CZ), BF16),
            pltpu.VMEM((2, NDEV, RLOC, 8, CZ), BF16),
            pltpu.SemaphoreType.DMA((NSTAGE, NDEV)),
            pltpu.SemaphoreType.DMA((NSTAGE, NDEV)),
            pltpu.SemaphoreType.DMA((NCHUNK + 5,)),
            pltpu.SemaphoreType.DMA((10,)),
            pltpu.SemaphoreType.DMA((7,)),
            pltpu.SemaphoreType.DMA((3, RLOC)),
            pltpu.SemaphoreType.DMA((4,)),
        ]
        m_home, z_new = pl.pallas_call(
            block_kernel,
            name='evoformer_block',
            out_shape=(jax.ShapeDtypeStruct((RES, NCHUNK, CHUNK, CM), BF16), jax.ShapeDtypeStruct(z_blk.shape, BF16)),
            in_specs=[hbm, vmem, vmem, vmem, hbm, vmem, hbm, hbm, hbm, vmem, hbm, hbm, vmem, hbm, hbm, vmem, hbm],
            out_specs=(hbm, vmem),
            scratch_shapes=scratch,
            compiler_params=pltpu.CompilerParams(collective_id=0, has_side_effects=True,
                                                 vmem_limit_bytes=56 * 1024 * 1024),
        )(m_blk, z_blk, msa_mask.T, res_mask.reshape(1, RES), w_row_in, w_row_bias.T, w_row_out, w_col_in, w_col_out,
          w_opm_in.T, w_opm_out, w_start_in, w_start_bias.T, w_start_out, w_end_in, w_end_bias.T, w_end_out)
        whole = pl.BlockSpec((RLOC, RES, CZ), lambda q: (0, 0, 0))
        return pl.pallas_call(
            finish_kernel,
            name='finish',
            grid=(NCHUNK,),
            out_shape=(jax.ShapeDtypeStruct(m_blk.shape, BF16), jax.ShapeDtypeStruct(z_blk.shape, BF16)),
            in_specs=[pl.BlockSpec((RES, 1, CHUNK, CM), lambda q: (0, q, 0, 0)), whole],
            out_specs=(pl.BlockSpec((CHUNK, RES, CM), lambda q: (q, 0, 0)), whole),
            scratch_shapes=[pltpu.VMEM((256, 256), BF16)],
            compiler_params=pltpu.CompilerParams(dimension_semantics=('arbitrary',)),
        )(m_home, z_new)

    return jax.shard_map(per_device, mesh=mesh, in_specs=in_specs, out_specs=(rows, rows), check_vma=False)
```

```python
import functools

import jax
import jax.numpy as jnp
import numpy as np
from jax import lax
from jax.experimental import pallas as pl
from jax.experimental.pallas import tpu as pltpu
from jax.sharding import PartitionSpec as P

BF16 = jnp.bfloat16
F32 = jnp.float32
MESH = pl.DeviceIdType.MESH
NDEV = 8
SEQ, RES, CM, CZ = 256, 96, 256, 128
SLOC, RLOC = SEQ // NDEV, RES // NDEV
HM, HT, HD, OPM = 8, 4, 32, 32
LANES = 128
MASKED = -1e9
SCALE = HD ** -0.5


def bf16_parts(value, n):
    parts = []
    for _ in range(n):
        parts.append(float(np.asarray(value - sum(parts), np.float32).astype(BF16)))
    return parts


MASKED_SCORE = bf16_parts(MASKED / SCALE, 3)

ROWB, MF, MB, STB, ZF, ENB, ZB = 0, 1, 5, 6, 7, 9, 10
NSTAGE = 12
ZGROUP = RLOC // 2
CHUNK = 8
NCHUNK = SLOC // CHUNK
CROWS = NDEV * CHUNK
LAG = 4
MB_EARLY = 8
NRES = 4


def dot(a, b):
    return jnp.dot(a, b, preferred_element_type=F32)


def dot_t(a, b):
    return lax.dot_general(a, b, (((1,), (1,)), ((), ())), preferred_element_type=F32)


def iota(shape, dim):
    return lax.broadcasted_iota(jnp.int32, shape, dim)


def layer_norm(x):
    values = x.astype(F32)
    centred = values - jnp.mean(values, axis=-1, keepdims=True)
    variance = jnp.mean(centred * centred, axis=-1, keepdims=True)
    return (centred * lax.rsqrt(variance + 1e-5)).astype(BF16)


def add_residual(state, update):
    return (state.astype(F32) + update).astype(BF16)


def head_masks():
    lane = iota((16, LANES), 1)
    return [jnp.where((lane >= h * HD) & (lane < (h + 1) * HD), 1.0, 0.0).astype(BF16) for h in range(LANES // HD)]


def only_head(x, mask):
    return x * jnp.concatenate([mask] * (x.shape[0] // 16), axis=0)


def dot_tl(a, b):
    return lax.dot_general(a, b, (((0,), (0,)), ((), ())), preferred_element_type=F32)


def softmax_keys(logits):
    weights = jnp.exp(logits - jnp.max(logits, axis=0, keepdims=True))
    return (weights * (1.0 / jnp.sum(weights, axis=0, keepdims=True))).astype(BF16)


def pipeline(items, first, middle, last, finish, ahead=1, behind=1):
    count = len(items)
    opened, ready = {}, {}
    for n in range(-ahead, count + behind + 1):
        if n + ahead < count:
            opened[n + ahead] = first(items[n + ahead])
        if 0 <= n < count:
            ready[n] = middle(items[n], opened.pop(n))
        if 0 <= n - behind < count:
            last(items[n - behind], ready.pop(n - behind))
        if 0 <= n - behind - 1 < count:
            finish(items[n - behind - 1])


def attend_biased(rows, tiles, q_of, k_of, vg_of, bias_ref, keep_of, w_out, store):
    masks = head_masks()
    each = len(masks)
    vgs = {}
    mixed = {u: [] for u in rows}

    def first(item):
        u, t = item
        if t == 0:
            vgs[u] = vg_of(u)
        k = k_of(u, t)
        return dot_t(jnp.concatenate([only_head(k, mask) for mask in masks], axis=0), q_of(u, t))

    def middle(item, scores):
        u, t = item
        keep = keep_of(u) != 0.0
        return [softmax_keys(jnp.where(keep, scores[n * RES:(n + 1) * RES] * SCALE + bias_ref[each * t + n], MASKED))
                for n in range(each)]

    def last(item, probs):
        u, t = item
        for n in range(each):
            h = each * t + n
            padded = jnp.concatenate([probs[n], jnp.zeros((LANES - RES, LANES), BF16)], axis=0)
            mixed[u].append(dot(vgs[u][h * HD:(h + 1) * HD], padded))

    def finish(item):
        u, t = item
        if t == tiles - 1:
            gates = jax.nn.sigmoid(vgs[u][tiles * LANES:].astype(F32))
            store(u, dot_tl((jnp.concatenate(mixed[u], axis=0) * gates).astype(BF16), w_out))

    pipeline([(u, t) for u in rows for t in range(tiles)], first, middle, last, finish)


def attend_column(residues, q_of, k_of, aug_of, ones, vg_of, w_out, store):
    masks = head_masks()
    each = len(masks)
    halves = SEQ // LANES
    vgs, keys = {}, {}
    mixed = {(u, half): [] for u in residues for half in range(halves)}

    def first(item):
        u, h, half = item
        if (h, half) == (0, 0):
            vgs[u] = vg_of(u)
        if half == 0:
            keys[u, h] = jnp.concatenate([only_head(k_of(u, h // each), masks[h % each]), aug_of(u)], axis=1)
        q = q_of(u, h // each)[half * LANES:(half + 1) * LANES]
        return dot_t(keys[u, h], jnp.concatenate([q, ones], axis=1))

    def middle(item, scores):
        return softmax_keys(scores * SCALE)

    def last(item, probs):
        u, h, half = item
        mixed[u, half].append(dot(vgs[u][h * HD:(h + 1) * HD], probs))

    def finish(item):
        u, h, half = item
        if (h, half) == (HM - 1, halves - 1):
            gates = jax.nn.sigmoid(vgs[u][CM:].astype(F32))
            out = jnp.concatenate([jnp.concatenate(mixed[u, n], axis=0) for n in range(halves)], axis=1)
            store(u, dot_tl((out * gates).astype(BF16), w_out))

    pipeline([(u, h, half) for u in residues for h in range(HM) for half in range(halves)], first, middle, last, finish, 4, 2)


def block_kernel(m_any, z_ref, mask_ref, res_ref, row_in_any, w_row_bias, row_out_any, col_in_any, col_out_any,
                 w_opm_in, opm_out_any, start_in_any, w_start_bias, start_out_any, end_in_any, w_end_bias, end_out_any,
                 mback, z_out,
                 m_ref, w_row_in, w_row_out, w_col_in, w_col_out, w_opm_out, w_start_in, w_start_out, w_end_in, w_end_out,
                 perm, perm_out, comp, compz, hperm, keep_row, mask_t, mask_s, norm, res_keep, wbt, bcol, bias,
                 rowb_recv, stb_recv, enb_recv, row_vg, col_vg, tri_vg, yrow, rowqk, triqk, m1, msend, mrecv, mcols, mdone,
                 ycol, colqk, caug, ckeep, ones,
                 left, crecv, cbig, outer, w2, w2t, ynorm, z1, zs, zr, z2, z3, zs2, zr2,
                 send_sem, recv_sem, local_sem, load_sem, c_send, c_recv, c_pair):
    data = lax.axis_index('data')
    me = lax.axis_index('chip') * 4 + lax.axis_index('dap')
    core, chip_x, chip_y = lax.rem(me, 2), lax.rem(me // 2, 2), me // 4
    partner = me + 1 - 2 * core
    to_x, to_y = 2 - 4 * chip_x, 4 - 8 * chip_y
    twins = (me + to_x + to_y, me + to_x, me + to_y)

    def device(d):
        return (data, d // 4, lax.rem(d, 4))

    def peer(r):
        return lax.rem(me + r, NDEV)

    def source(r):
        return lax.rem(me + NDEV - r, NDEV)

    def remote(src, dst, send, recv, d):
        return pltpu.make_async_remote_copy(src_ref=src, dst_ref=dst, send_sem=send, recv_sem=recv,
                                            device_id=device(d), device_id_type=MESH)

    def start_all(stage, src_of, dst_of):
        for r in range(1, NDEV):
            d = peer(r)
            remote(src_of(d), dst_of(me), send_sem.at[stage, r], recv_sem.at[stage, r], d).start()

    def wait_recv(stage, dst_of):
        for r in range(1, NDEV):
            dst = dst_of(source(r))
            remote(dst, dst, send_sem.at[stage, r], recv_sem.at[stage, r], peer(r)).wait_recv()

    def wait_send(stage, src_of):
        for r in range(1, NDEV):
            src = src_of(peer(r))
            remote(src, src, send_sem.at[stage, r], recv_sem.at[stage, r], peer(r)).wait_send()

    barrier = pltpu.get_barrier_semaphore()
    for r in range(1, NDEV):
        pl.semaphore_signal(barrier, inc=1, device_id=device(peer(r)), device_id_type=MESH)

    loads = [pltpu.make_async_copy(src, dst, load_sem.at[n]) for n, (src, dst) in enumerate((
        (row_in_any, w_row_in), (m_any, m_ref), (row_out_any, w_row_out), (col_in_any, w_col_in), (opm_out_any, w_opm_out),
        (start_in_any, w_start_in), (end_in_any, w_end_in), (col_out_any, w_col_out), (start_out_any, w_start_out),
        (end_out_any, w_end_out)))]
    for load in loads:
        load.start()

    r0, c0 = iota((256, 256), 0), iota((256, 256), 1)
    perm[...] = jnp.where(((r0 >> 4) == (c0 & 15)) & ((r0 & 15) == (c0 >> 4)), 1.0, 0.0).astype(BF16)
    perm_out[...] = jnp.where(((r0 >> 3) == (c0 & 31)) & ((r0 & 7) == (c0 >> 5)), 1.0, 0.0).astype(BF16)
    r1, c1 = iota((RES, LANES), 0), iota((RES, LANES), 1)
    comp[...] = jnp.where(((c1 & 15) < RLOC) & (r1 == (c1 >> 4) * RLOC + (c1 & 15)), 1.0, 0.0).astype(BF16)
    compz[...] = jnp.where(((c1 & 7) < ZGROUP) & (r1 == ((c1 >> 3) & 7) * RLOC + (c1 >> 6) * ZGROUP + (c1 & 7)),
                           1.0, 0.0).astype(BF16)
    r2, c2 = iota((LANES, LANES), 0), iota((LANES, LANES), 1)
    hperm[...] = jnp.where(((r2 >> 4) == (c2 & 7)) & ((r2 & 15) == (c2 >> 3)), 1.0, 0.0).astype(BF16)
    eye = jnp.where(r2 == c2, 1.0, 0.0).astype(BF16)
    ones[...] = jnp.where(iota((SEQ, LANES), 1) < len(MASKED_SCORE), 1.0, 0.0).astype(BF16)
    bcol[...] = jnp.zeros_like(bcol)
    wbt[...] = jnp.zeros_like(wbt)
    for n, w in enumerate((w_row_bias, w_start_bias, w_end_bias)):
        wbt[n, 0:w.shape[0], :] = w[...].astype(F32)

    def send_bias(recv, which, heads, stage):
        weights = wbt[which].astype(BF16)

        for i in range(RLOC):
            bcol[i] = dot_t(weights, ynorm[i])

        mine = dot(hperm[0:heads * 16, :], bcol[...].reshape(LANES, LANES).astype(BF16)).astype(BF16)
        recv[me] = mine.reshape(heads, 16, LANES)
        start_all(stage, lambda d: recv.at[me], lambda s: recv.at[s])

    def bias_rows(recv):
        return lambda s: recv.at[s]

    def take_bias(recv, heads, stage):
        wait_recv(stage, bias_rows(recv))
        for h in range(heads):
            rows = dot(comp[...], recv[:, h].reshape(LANES, LANES)).astype(BF16)
            bias[h] = dot_t(eye, jnp.concatenate([rows, jnp.zeros((LANES - RES, LANES), BF16)], axis=0))[0:RES]

    ynorm[:, RES:, :] = jnp.zeros((RLOC, LANES - RES, CZ), BF16)

    ynorm[:, 0:RES, :] = layer_norm(z_ref[...].reshape(RLOC * RES, CZ)).reshape(RLOC, RES, CZ)

    pl.semaphore_wait(barrier, NDEV - 1)
    send_bias(rowb_recv, 0, HM, ROWB)

    res_keep[...] = dot((eye[0:RES, 0:RES].astype(F32) * res_ref[...].astype(F32)).astype(BF16),
                        jnp.ones((RES, LANES), BF16))
    seq_order = jnp.where(r0 == ((c0 >> 3) & 7) * SLOC + (c0 >> 6) * CHUNK + (c0 & 7), 1.0, 0.0).astype(BF16)
    seq_rows = jnp.where(c0 == ((r0 >> 3) & 7) * SLOC + (r0 >> 6) * CHUNK + (r0 & 7), 1.0, 0.0).astype(BF16)
    mt = mask_ref[...].astype(F32).astype(BF16)
    mask_t[...] = dot(mt, seq_order)
    mask_s[...] = dot_t(seq_rows, mt).astype(BF16)

    @pl.loop(0, SLOC // 4)
    def _(blk):
        for u in range(4):
            pick = jnp.where(iota((SEQ, LANES), 0) == me * SLOC + blk * 4 + u, 1.0, 0.0).astype(BF16)
            keep_row[blk * 4 + u] = dot(mask_ref[...].astype(F32).astype(BF16), pick)

    for load in loads:
        load.wait()
    row_vg[...] = jnp.transpose(w_row_in[:, 2 * CM:])
    col_vg[...] = jnp.transpose(w_col_in[:, 2 * CM:])
    tri_vg[0] = jnp.transpose(w_start_in[:, 2 * CZ:])
    tri_vg[1] = jnp.transpose(w_end_in[:, 2 * CZ:])
    norm[...] = jnp.zeros_like(norm)
    norm[0:RES, 0:RES] = dot_t(mt, mt)
    w_full = w_opm_out[...].reshape(OPM, OPM, CZ)
    for a in range(2):
        for c in range(2):
            blk = w_full[16 * a:16 * a + 16, 16 * c:16 * c + 16, :].reshape(256, CZ)
            w2[16 * c:16 * c + 16, 16 * a:16 * a + 16, :] = dot(perm[...], blk).astype(BF16).reshape(16, 16, CZ)
    w2t[...] = dot_t(eye, w2[...].reshape(OPM * OPM, CZ)).astype(BF16)
    cbig[:, RES:, :] = jnp.zeros((OPM, LANES - RES, SEQ), BF16)
    yrow[:, RES:, :] = jnp.zeros((CHUNK, LANES - RES, CM), BF16)
    rowqk[:, :, RES:, :] = jnp.zeros((4, CHUNK, LANES - RES, LANES), BF16)
    triqk[:, :, RES:, :] = jnp.zeros((2, RLOC, LANES - RES, LANES), BF16)
    z1[RLOC:, :, :] = jnp.zeros((16 - RLOC, RES, CZ), BF16)
    z3[...] = jnp.zeros_like(z3)

    take_bias(rowb_recv, HM, ROWB)

    def m_src(q):
        return lambda d: msend.at[q, pl.ds(d * RLOC, RLOC)]

    def m_dst(q):
        return lambda s: mrecv.at[q, s]

    def local_copy(src, dst, n):
        return pltpu.make_async_copy(src, dst, local_sem.at[n])

    def row_chunk(q):
        s0 = q * CHUNK
        for part in range(CHUNK // 4):
            here = slice(4 * part, 4 * part + 4)
            y = layer_norm(m_ref[s0 + 4 * part:s0 + 4 * part + 4].reshape(4 * RES, CM))
            yrow[here, 0:RES, :] = y.reshape(4, RES, CM)
            qk = dot(y, w_row_in[:, 0:2 * CM]).astype(BF16)
            for t in range(4):
                rowqk[t, here, 0:RES, :] = qk[:, t * LANES:(t + 1) * LANES].reshape(4, RES, LANES)

        def store(u, update):
            m1[s0 + u] = add_residual(m_ref[s0 + u], update[0:RES])
        attend_biased(range(CHUNK), 2, lambda u, t: rowqk[t, u], lambda u, t: rowqk[2 + t, u, 0:RES],
                      lambda u: dot_t(row_vg[...], yrow[u]).astype(BF16), bias,
                      lambda u: keep_row[s0 + u], w_row_out[...], store)

        for j in range(RES // 32):
            blk = m1[CHUNK * q:CHUNK * q + CHUNK, 32 * j:32 * j + 32, :].reshape(256, CM)
            msend[q, 32 * j:32 * j + 32] = dot(perm_out[...], blk).reshape(32, CHUNK, CM).astype(BF16)
        start_all(MF + q, m_src(q), m_dst(q))
        local_copy(m_src(q)(me), m_dst(q)(me), q).start()

    def column_projection(q):
        local_copy(m_src(q)(me), m_dst(q)(me), q).wait()
        wait_recv(MF + q, m_dst(q))

        for blk in range(RLOC // 4):
            x = jnp.concatenate([mrecv[q, :, blk * 4 + u].astype(F32).reshape(CROWS, CM) for u in range(4)], axis=0)
            for u in range(4):
                mcols[q, blk * 4 + u] = x[u * CROWS:(u + 1) * CROWS].astype(BF16)
            y = layer_norm(x)
            ycol[blk * 4:blk * 4 + 4, CROWS * q:CROWS * q + CROWS, :] = y.reshape(4, CROWS, CM)
            qk = dot(y, w_col_in[:, 0:2 * CM]).astype(BF16)
            for t in range(4):
                colqk[t, blk * 4:blk * 4 + 4, CROWS * q:CROWS * q + CROWS, :] = (
                    qk[:, t * LANES:(t + 1) * LANES].reshape(4, CROWS, LANES))

    row_chunk(0)
    row_chunk(1)
    row_chunk(2)
    column_projection(0)
    row_chunk(3)
    column_projection(1)
    column_projection(2)
    column_projection(3)

    def mb_start(j):
        start_all(MB, lambda d: mdone.at[d, j], lambda s: mback.at[s * RLOC + j])

    def relay(j):
        for t, twin in enumerate(twins):
            row = crecv.at[twin * RLOC + j]
            remote(row, row, c_send.at[t], c_recv.at[t, j], twin).wait_recv()
            remote(row, row, c_send.at[3 + t], c_pair.at[t], partner).start()

    @pl.loop(0, RLOC // NRES)
    def _(pair):
        lane = iota((SEQ, LANES), 1)
        offset = jnp.zeros((SEQ, LANES), F32)
        for n, part in enumerate(MASKED_SCORE):
            offset = jnp.where(lane == n, part, offset)
        for u in range(NRES):
            pick = jnp.where(iota((RES, LANES), 0) == me * RLOC + pair * NRES + u, 1.0, 0.0).astype(BF16)
            keep = dot(mask_s[...], pick)
            caug[u] = ((1.0 - keep) * offset).astype(BF16)
            keep = keep.astype(BF16)
            for t in range(2):
                ckeep[u, t] = colqk[2 + t, pair * NRES + u] * keep

        def store(u, update):
            j = pair * NRES + u
            mask_row = mask_t[pl.ds(me * RLOC + j, 1), :]
            x = add_residual(mcols[:, j].reshape(SEQ, CM), update)
            both = dot_t(w_opm_in[...], layer_norm(x)).astype(BF16).astype(F32) * mask_row
            left[j] = both[0:OPM].astype(BF16)
            crecv[me * RLOC + j] = both[OPM:].astype(BF16)
            done = x.astype(F32).reshape(NCHUNK, NDEV, CHUNK, CM).astype(BF16)
            for d in range(NDEV):
                mdone[d, j] = done[:, d]

        attend_column(range(NRES), lambda u, t: colqk[t, pair * NRES + u], lambda u, t: ckeep[u, t], lambda u: caug[u],
                      ones[0:LANES], lambda u: dot_t(col_vg[...], ycol[pair * NRES + u]).astype(BF16), w_col_out[...], store)
        for u in range(NRES):
            j = pair * NRES + u
            row = crecv.at[me * RLOC + j]
            for t, twin in enumerate(twins):
                remote(row, row, c_send.at[t], c_recv.at[t, j], twin).start()
            remote(row, row, c_send.at[6], c_pair.at[3], partner).start()

        @pl.when(pair >= LAG // NRES)
        def _():
            for u in range(NRES):
                relay(pair * NRES - LAG + u)

        @pl.when(pair < MB_EARLY // NRES)
        def _():
            for u in range(NRES):
                mb_start(pair * NRES + u)

    for j in range(RLOC - LAG, RLOC):
        relay(j)
    keep_mine = local_copy(mdone.at[me], mback.at[pl.ds(me * RLOC, RLOC)], NCHUNK + 4)
    keep_mine.start()

    def c_rows(s):
        return crecv.at[pl.ds(s * RLOC, RLOC)]

    for t, first in enumerate(twins + (me,)):
        rows = c_rows(first + 1 - 2 * core)
        remote(rows, rows, c_send.at[3 + t], c_pair.at[t], partner).wait_recv()
    for j in range(MB_EARLY, RLOC):
        mb_start(j)
    for c in range(2):
        for j0 in range(0, RES, 16):
            blk = crecv[j0:j0 + 16, 16 * c:16 * c + 16, :].reshape(256, SEQ)
            cbig[16 * c:16 * c + 16, j0:j0 + 16, :] = dot(perm[...], blk).astype(BF16).reshape(16, 16, SEQ)

    @pl.loop(0, OPM // 8)
    def _(blk):
        for c2 in range(4):
            c = blk * 4 + c2
            prod = dot_t(left[...].reshape(RLOC * OPM, SEQ), cbig[pl.ds(2 * c, 2)].reshape(256, SEQ)).astype(BF16)
            for u in range(2):
                outer[:, 2 * c + u] = prod[:, u * LANES:(u + 1) * LANES].reshape(RLOC, OPM, LANES)

    @pl.loop(0, 2)
    def _(half):
        for u in range(RLOC // 2):
            i = half * (RLOC // 2) + u
            update = dot(w2t[...], outer[i].reshape(OPM * OPM, LANES))
            update = update / (1e-3 + norm[pl.ds(me * RLOC + i, 1), :])
            z1[i] = add_residual(z_ref[i], jnp.transpose(update)[0:RES])

    def z_src(buf, group):
        return lambda d: buf.at[group, pl.ds(d * RLOC, RLOC)]

    def z_dst(buf, group):
        return lambda s: buf.at[group, s]

    def triangle(state, result, w_in, which, w_out, recv, stage, late, send, zrecv, moved, zstage, slot):
        ynorm[:, 0:RES, :] = layer_norm(state[0:RLOC].reshape(RLOC * RES, CZ)).reshape(RLOC, RES, CZ)
        send_bias(recv, which, HT, stage)

        for blk in range(RLOC // 4):
            y = ynorm[blk * 4:blk * 4 + 4, 0:RES, :].reshape(4 * RES, CZ)
            qk = dot(y, w_in[:, 0:2 * CZ]).astype(BF16)
            for t in range(2):
                triqk[t, blk * 4:blk * 4 + 4, 0:RES, :] = qk[:, t * LANES:(t + 1) * LANES].reshape(4, RES, LANES)
        take_bias(recv, HT, stage)
        for j in late:
            mb_start(j)

        for group in range(2):
            first = group * ZGROUP

            def store(u, update):
                result[u] = add_residual(state[u], update[0:RES])
            attend_biased(range(first, first + ZGROUP), 1, lambda u, t: triqk[0, u], lambda u, t: triqk[1, u, 0:RES],
                          lambda u: dot_t(tri_vg[which - 1], ynorm[u]).astype(BF16), bias,
                          lambda u: res_keep[...], w_out[...], store)
            for j in range(RES // 32):
                blk = result[first:first + 8, 32 * j:32 * j + 32, :].reshape(256, CZ)
                send[group, 32 * j:32 * j + 32] = dot(perm_out[...], blk).reshape(32, 8, CZ).astype(BF16)
            start_all(zstage + group, z_src(send, group), z_dst(zrecv, group))
            local_copy(z_src(send, group)(me), z_dst(zrecv, group)(me), slot + group).start()

        for group in range(2):
            local_copy(z_src(send, group)(me), z_dst(zrecv, group)(me), slot + group).wait()
            wait_recv(zstage + group, z_dst(zrecv, group))

        for i in range(RLOC):
            rows = zrecv[:, :, i].astype(F32).reshape(LANES, CZ).astype(BF16)
            moved[i] = dot(compz[...], rows).astype(BF16)

    triangle(z1, z1, w_start_in, 1, w_start_out, stb_recv, STB, (), zs, zr, z2, ZF, NCHUNK)
    triangle(z2, z3, w_end_in, 2, w_end_out, enb_recv, ENB, (), zs2, zr2, z_out, ZB, NCHUNK + 2)

    wait_recv(MB, lambda s: mback.at[pl.ds(s * RLOC, RLOC)])
    keep_mine.wait()

    wait_send(ROWB, lambda d: bias_rows(rowb_recv)(me))
    for q in range(NCHUNK):
        wait_send(MF + q, m_src(q))
    wait_send(MB, lambda d: mdone.at[d])
    for t in range(7):
        rows = c_rows(me if t in (0, 1, 2, 6) else twins[t - 3])
        remote(rows, rows, c_send.at[t], c_pair.at[0], partner).wait_send()
    wait_send(STB, lambda d: bias_rows(stb_recv)(me))
    for group in range(2):
        wait_send(ZF + group, z_src(zs, group))
    wait_send(ENB, lambda d: bias_rows(enb_recv)(me))
    for group in range(2):
        wait_send(ZB + group, z_src(zs2, group))


def finish_kernel(m_home, z_new, m_out, z_out, perm_in):
    @pl.when(pl.program_id(0) == 0)
    def _():
        r, c = iota((256, 256), 0), iota((256, 256), 1)
        perm_in[...] = jnp.where(((r >> 5) == (c & 7)) & ((r & 31) == (c >> 3)), 1.0, 0.0).astype(BF16)
        z_out[...] = z_new[...]

    for j in range(RES // 32):
        blk = m_home[32 * j:32 * j + 32, 0].astype(F32).reshape(256, CM).astype(BF16)
        m_out[:, 32 * j:32 * j + 32, :] = dot(perm_in[...], blk).astype(BF16).reshape(CHUNK, 32, CM)


def solution(mesh):
    rows = P(('data', 'chip', 'dap'))
    in_specs = (rows, rows, P('data'), P('data')) + (P(),) * 13
    vmem = pl.BlockSpec(memory_space=pltpu.VMEM)
    hbm = pl.BlockSpec(memory_space=pl.ANY)

    def per_device(m_blk, z_blk, msa_mask, res_mask, w_row_in, w_row_bias, w_row_out, w_col_in, w_col_out,
                   w_opm_in, w_opm_out, w_start_in, w_start_bias, w_start_out, w_end_in, w_end_bias, w_end_out):
        loaded = [m_blk, w_row_in, w_row_out, w_col_in, w_col_out, w_opm_out, w_start_in, w_start_out, w_end_in, w_end_out]
        scratch = [pltpu.VMEM(x.shape, x.dtype) for x in loaded] + [
            pltpu.VMEM((256, 256), BF16),
            pltpu.VMEM((256, 256), BF16),
            pltpu.VMEM((RES, LANES), BF16),
            pltpu.VMEM((RES, LANES), BF16),
            pltpu.VMEM((LANES, LANES), BF16),
            pltpu.VMEM((SLOC, RES, LANES), F32),
            pltpu.VMEM((RES, SEQ), F32),
            pltpu.VMEM((SEQ, RES), BF16),
            pltpu.VMEM((LANES, LANES), F32),
            pltpu.VMEM((RES, LANES), F32),
            pltpu.VMEM((3, 8, CZ), F32),
            pltpu.VMEM((16, 8, LANES), F32),
            pltpu.VMEM((HM, RES, LANES), F32),
            pltpu.VMEM((NDEV, HM, 16, LANES), BF16),
            pltpu.VMEM((NDEV, HT, 16, LANES), BF16),
            pltpu.VMEM((NDEV, HT, 16, LANES), BF16),
            pltpu.VMEM((2 * CM, CM), BF16),
            pltpu.VMEM((2 * CM, CM), BF16),
            pltpu.VMEM((2, 2 * CZ, CZ), BF16),
            pltpu.VMEM((CHUNK, LANES, CM), BF16),
            pltpu.VMEM((4, CHUNK, LANES, LANES), BF16),
            pltpu.VMEM((2, RLOC, LANES, LANES), BF16),
            pltpu.VMEM((SLOC, RES, CM), BF16),
            pltpu.VMEM((NCHUNK, RES, CHUNK, CM), BF16),
            pltpu.VMEM((NCHUNK, NDEV, RLOC, CHUNK, CM), BF16),
            pltpu.VMEM((NCHUNK, RLOC, CROWS, CM), BF16),
            pltpu.VMEM((NDEV, RLOC, NCHUNK, CHUNK, CM), BF16),
            pltpu.VMEM((RLOC, SEQ, CM), BF16),
            pltpu.VMEM((4, RLOC, SEQ, LANES), BF16),
            pltpu.VMEM((NRES, SEQ, LANES), BF16),
            pltpu.VMEM((NRES, 2, SEQ, LANES), BF16),
            pltpu.VMEM((SEQ, LANES), BF16),
            pltpu.VMEM((RLOC, OPM, SEQ), BF16),
            pltpu.VMEM((RES, OPM, SEQ), BF16),
            pltpu.VMEM((OPM, LANES, SEQ), BF16),
            pltpu.VMEM((RLOC, OPM, OPM, LANES), BF16),
            pltpu.VMEM((OPM, OPM, CZ), BF16),
            pltpu.VMEM((CZ, OPM * OPM), BF16),
            pltpu.VMEM((RLOC, LANES, CZ), BF16),
            pltpu.VMEM((16, RES, CZ), BF16),
            pltpu.VMEM((2, RES, 8, CZ), BF16),
            pltpu.VMEM((2, NDEV, RLOC, 8, CZ), BF16),
            pltpu.VMEM((RLOC, RES, CZ), BF16),
            pltpu.VMEM((16, RES, CZ), BF16),
            pltpu.VMEM((2, RES, 8, CZ), BF16),
            pltpu.VMEM((2, NDEV, RLOC, 8, CZ), BF16),
            pltpu.SemaphoreType.DMA((NSTAGE, NDEV)),
            pltpu.SemaphoreType.DMA((NSTAGE, NDEV)),
            pltpu.SemaphoreType.DMA((NCHUNK + 5,)),
            pltpu.SemaphoreType.DMA((10,)),
            pltpu.SemaphoreType.DMA((7,)),
            pltpu.SemaphoreType.DMA((3, RLOC)),
            pltpu.SemaphoreType.DMA((4,)),
        ]
        m_home, z_new = pl.pallas_call(
            block_kernel,
            name='evoformer_block',
            out_shape=(jax.ShapeDtypeStruct((RES, NCHUNK, CHUNK, CM), BF16), jax.ShapeDtypeStruct(z_blk.shape, BF16)),
            in_specs=[hbm, vmem, vmem, vmem, hbm, vmem, hbm, hbm, hbm, vmem, hbm, hbm, vmem, hbm, hbm, vmem, hbm],
            out_specs=(hbm, vmem),
            scratch_shapes=scratch,
            compiler_params=pltpu.CompilerParams(collective_id=0, has_side_effects=True,
                                                 vmem_limit_bytes=56 * 1024 * 1024),
        )(m_blk, z_blk, msa_mask.T, res_mask.reshape(1, RES), w_row_in, w_row_bias.T, w_row_out, w_col_in, w_col_out,
          w_opm_in.T, w_opm_out, w_start_in, w_start_bias.T, w_start_out, w_end_in, w_end_bias.T, w_end_out)
        whole = pl.BlockSpec((RLOC, RES, CZ), lambda q: (0, 0, 0))
        return pl.pallas_call(
            finish_kernel,
            name='finish',
            grid=(NCHUNK,),
            out_shape=(jax.ShapeDtypeStruct(m_blk.shape, BF16), jax.ShapeDtypeStruct(z_blk.shape, BF16)),
            in_specs=[pl.BlockSpec((RES, 1, CHUNK, CM), lambda q: (0, q, 0, 0)), whole],
            out_specs=(pl.BlockSpec((CHUNK, RES, CM), lambda q: (q, 0, 0)), whole),
            scratch_shapes=[pltpu.VMEM((256, 256), BF16)],
            compiler_params=pltpu.CompilerParams(dimension_semantics=('arbitrary',)),
        )(m_home, z_new)

    return jax.shard_map(per_device, mesh=mesh, in_specs=in_specs, out_specs=(rows, rows), check_vma=False)
```

```python
import functools

import jax
import jax.numpy as jnp
import numpy as np
from jax import lax
from jax.experimental import pallas as pl
from jax.experimental.pallas import tpu as pltpu
from jax.sharding import PartitionSpec as P

BF16 = jnp.bfloat16
F32 = jnp.float32
MESH = pl.DeviceIdType.MESH
NDEV = 8
SEQ, RES, CM, CZ = 256, 96, 256, 128
SLOC, RLOC = SEQ // NDEV, RES // NDEV
HM, HT, HD, OPM = 8, 4, 32, 32
LANES = 128
MASKED = -1e9
SCALE = HD ** -0.5


def bf16_parts(value, n):
    parts = []
    for _ in range(n):
        parts.append(float(np.asarray(value - sum(parts), np.float32).astype(BF16)))
    return parts


MASKED_SCORE = bf16_parts(MASKED / SCALE, 3)

ROWB, MF, MB, STB, ZF, ENB, ZB = 0, 1, 5, 6, 7, 9, 10
NSTAGE = 12
ZGROUP = RLOC // 2
CHUNK = 8
NCHUNK = SLOC // CHUNK
CROWS = NDEV * CHUNK
LAG = 4
NRES = 4


def dot(a, b):
    return jnp.dot(a, b, preferred_element_type=F32)


def dot_t(a, b):
    return lax.dot_general(a, b, (((1,), (1,)), ((), ())), preferred_element_type=F32)


def iota(shape, dim):
    return lax.broadcasted_iota(jnp.int32, shape, dim)


def layer_norm(x):
    values = x.astype(F32)
    centred = values - jnp.mean(values, axis=-1, keepdims=True)
    variance = jnp.mean(centred * centred, axis=-1, keepdims=True)
    return (centred * lax.rsqrt(variance + 1e-5)).astype(BF16)


def add_residual(state, update):
    return (state.astype(F32) + update).astype(BF16)


def head_masks():
    lane = iota((16, LANES), 1)
    return [jnp.where((lane >= h * HD) & (lane < (h + 1) * HD), 1.0, 0.0).astype(BF16) for h in range(LANES // HD)]


def only_head(x, mask):
    return x * jnp.concatenate([mask] * (x.shape[0] // 16), axis=0)


def dot_tl(a, b):
    return lax.dot_general(a, b, (((0,), (0,)), ((), ())), preferred_element_type=F32)


def softmax_keys(logits):
    weights = jnp.exp(logits - jnp.max(logits, axis=0, keepdims=True))
    return (weights * (1.0 / jnp.sum(weights, axis=0, keepdims=True))).astype(BF16)


def pipeline(items, first, middle, last, finish, ahead=1, behind=1):
    count = len(items)
    opened, ready = {}, {}
    for n in range(-ahead, count + behind + 1):
        if n + ahead < count:
            opened[n + ahead] = first(items[n + ahead])
        if 0 <= n < count:
            ready[n] = middle(items[n], opened.pop(n))
        if 0 <= n - behind < count:
            last(items[n - behind], ready.pop(n - behind))
        if 0 <= n - behind - 1 < count:
            finish(items[n - behind - 1])


def attend_biased(rows, tiles, q_of, k_of, vg_of, bias_ref, keep_of, w_out, store):
    masks = head_masks()
    each = len(masks)
    vgs = {}
    mixed = {u: [] for u in rows}

    def first(item):
        u, t = item
        if t == 0:
            vgs[u] = vg_of(u)
        k = k_of(u, t)
        return dot_t(jnp.concatenate([only_head(k, mask) for mask in masks], axis=0), q_of(u, t))

    def middle(item, scores):
        u, t = item
        keep = keep_of(u) != 0.0
        return [softmax_keys(jnp.where(keep, scores[n * RES:(n + 1) * RES] * SCALE + bias_ref[each * t + n], MASKED))
                for n in range(each)]

    def last(item, probs):
        u, t = item
        for n in range(each):
            h = each * t + n
            padded = jnp.concatenate([probs[n], jnp.zeros((LANES - RES, LANES), BF16)], axis=0)
            mixed[u].append(dot(vgs[u][h * HD:(h + 1) * HD], padded))

    def finish(item):
        u, t = item
        if t == tiles - 1:
            gates = jax.nn.sigmoid(vgs[u][tiles * LANES:].astype(F32))
            store(u, dot_tl((jnp.concatenate(mixed[u], axis=0) * gates).astype(BF16), w_out))

    pipeline([(u, t) for u in rows for t in range(tiles)], first, middle, last, finish)


def attend_column(residues, q_of, k_of, aug_of, ones, vg_of, w_out, store):
    masks = head_masks()
    each = len(masks)
    halves = SEQ // LANES
    vgs, keys = {}, {}
    mixed = {(u, half): [] for u in residues for half in range(halves)}

    def first(item):
        u, h, half = item
        if (h, half) == (0, 0):
            vgs[u] = vg_of(u)
        if half == 0:
            keys[u, h] = jnp.concatenate([only_head(k_of(u, h // each), masks[h % each]), aug_of(u)], axis=1)
        q = q_of(u, h // each)[half * LANES:(half + 1) * LANES]
        return dot_t(keys[u, h], jnp.concatenate([q, ones], axis=1))

    def middle(item, scores):
        return softmax_keys(scores * SCALE)

    def last(item, probs):
        u, h, half = item
        mixed[u, half].append(dot(vgs[u][h * HD:(h + 1) * HD], probs))

    def finish(item):
        u, h, half = item
        if (h, half) == (HM - 1, halves - 1):
            gates = jax.nn.sigmoid(vgs[u][CM:].astype(F32))
            out = jnp.concatenate([jnp.concatenate(mixed[u, n], axis=0) for n in range(halves)], axis=1)
            store(u, dot_tl((out * gates).astype(BF16), w_out))

    pipeline([(u, h, half) for u in residues for h in range(HM) for half in range(halves)], first, middle, last, finish, 4, 2)


def block_kernel(m_any, z_ref, mask_ref, res_ref, row_in_any, w_row_bias, row_out_any, col_in_any, col_out_any,
                 w_opm_in, opm_out_any, start_in_any, w_start_bias, start_out_any, end_in_any, w_end_bias, end_out_any,
                 mback, z_out,
                 m_ref, w_row_in, w_row_out, w_col_in, w_col_out, w_opm_out, w_start_in, w_start_out, w_end_in, w_end_out,
                 perm, perm_out, comp, compz, hperm, keep_row, mask_t, mask_s, norm, res_keep, wbt, bcol, bias,
                 rowb_recv, stb_recv, enb_recv, row_vg, col_vg, tri_vg, yrow, rowqk, triqk, m1, msend, mrecv, mcols, mdone,
                 ycol, colqk, caug, ckeep, ones,
                 left, crecv, cbig, outer, w2, w2t, ynorm, z1, zs, zr, z2, z3, zs2, zr2,
                 send_sem, recv_sem, local_sem, load_sem, c_send, c_recv, c_pair):
    data = lax.axis_index('data')
    me = lax.axis_index('chip') * 4 + lax.axis_index('dap')
    core, chip_x, chip_y = lax.rem(me, 2), lax.rem(me // 2, 2), me // 4
    partner = me + 1 - 2 * core
    to_x, to_y = 2 - 4 * chip_x, 4 - 8 * chip_y
    twins = (me + to_x + to_y, me + to_x, me + to_y)

    def device(d):
        return (data, d // 4, lax.rem(d, 4))

    def peer(r):
        return lax.rem(me + r, NDEV)

    def source(r):
        return lax.rem(me + NDEV - r, NDEV)

    def remote(src, dst, send, recv, d):
        return pltpu.make_async_remote_copy(src_ref=src, dst_ref=dst, send_sem=send, recv_sem=recv,
                                            device_id=device(d), device_id_type=MESH)

    def start_all(stage, src_of, dst_of):
        for r in range(1, NDEV):
            d = peer(r)
            remote(src_of(d), dst_of(me), send_sem.at[stage, r], recv_sem.at[stage, r], d).start()

    def wait_recv(stage, dst_of):
        for r in range(1, NDEV):
            dst = dst_of(source(r))
            remote(dst, dst, send_sem.at[stage, r], recv_sem.at[stage, r], peer(r)).wait_recv()

    def wait_send(stage, src_of):
        for r in range(1, NDEV):
            src = src_of(peer(r))
            remote(src, src, send_sem.at[stage, r], recv_sem.at[stage, r], peer(r)).wait_send()

    barrier = pltpu.get_barrier_semaphore()
    for r in range(1, NDEV):
        pl.semaphore_signal(barrier, inc=1, device_id=device(peer(r)), device_id_type=MESH)

    loads = [pltpu.make_async_copy(src, dst, load_sem.at[n]) for n, (src, dst) in enumerate((
        (row_in_any, w_row_in), (m_any, m_ref), (row_out_any, w_row_out), (col_in_any, w_col_in), (opm_out_any, w_opm_out),
        (start_in_any, w_start_in), (end_in_any, w_end_in), (col_out_any, w_col_out), (start_out_any, w_start_out),
        (end_out_any, w_end_out)))]
    for load in loads:
        load.start()

    r0, c0 = iota((256, 256), 0), iota((256, 256), 1)
    perm[...] = jnp.where(((r0 >> 4) == (c0 & 15)) & ((r0 & 15) == (c0 >> 4)), 1.0, 0.0).astype(BF16)
    perm_out[...] = jnp.where(((r0 >> 3) == (c0 & 31)) & ((r0 & 7) == (c0 >> 5)), 1.0, 0.0).astype(BF16)
    r1, c1 = iota((RES, LANES), 0), iota((RES, LANES), 1)
    comp[...] = jnp.where(((c1 & 15) < RLOC) & (r1 == (c1 >> 4) * RLOC + (c1 & 15)), 1.0, 0.0).astype(BF16)
    compz[...] = jnp.where(((c1 & 7) < ZGROUP) & (r1 == ((c1 >> 3) & 7) * RLOC + (c1 >> 6) * ZGROUP + (c1 & 7)),
                           1.0, 0.0).astype(BF16)
    r2, c2 = iota((LANES, LANES), 0), iota((LANES, LANES), 1)
    hperm[...] = jnp.where(((r2 >> 4) == (c2 & 7)) & ((r2 & 15) == (c2 >> 3)), 1.0, 0.0).astype(BF16)
    eye = jnp.where(r2 == c2, 1.0, 0.0).astype(BF16)
    ones[...] = jnp.where(iota((SEQ, LANES), 1) < len(MASKED_SCORE), 1.0, 0.0).astype(BF16)
    bcol[...] = jnp.zeros_like(bcol)
    wbt[...] = jnp.zeros_like(wbt)
    for n, w in enumerate((w_row_bias, w_start_bias, w_end_bias)):
        wbt[n, 0:w.shape[0], :] = w[...].astype(F32)

    def send_bias(recv, which, heads, stage):
        weights = wbt[which].astype(BF16)

        for i in range(RLOC):
            bcol[i] = dot_t(weights, ynorm[i])

        mine = dot(hperm[0:heads * 16, :], bcol[...].reshape(LANES, LANES).astype(BF16)).astype(BF16)
        recv[me] = mine.reshape(heads, 16, LANES)
        start_all(stage, lambda d: recv.at[me], lambda s: recv.at[s])

    def bias_rows(recv):
        return lambda s: recv.at[s]

    def take_bias(recv, heads, stage):
        wait_recv(stage, bias_rows(recv))
        for h in range(heads):
            rows = dot(comp[...], recv[:, h].reshape(LANES, LANES)).astype(BF16)
            bias[h] = dot_t(eye, jnp.concatenate([rows, jnp.zeros((LANES - RES, LANES), BF16)], axis=0))[0:RES]

    ynorm[:, RES:, :] = jnp.zeros((RLOC, LANES - RES, CZ), BF16)

    ynorm[:, 0:RES, :] = layer_norm(z_ref[...].reshape(RLOC * RES, CZ)).reshape(RLOC, RES, CZ)

    pl.semaphore_wait(barrier, NDEV - 1)
    send_bias(rowb_recv, 0, HM, ROWB)

    res_keep[...] = dot((eye[0:RES, 0:RES].astype(F32) * res_ref[...].astype(F32)).astype(BF16),
                        jnp.ones((RES, LANES), BF16))
    seq_order = jnp.where(r0 == ((c0 >> 3) & 7) * SLOC + (c0 >> 6) * CHUNK + (c0 & 7), 1.0, 0.0).astype(BF16)
    seq_rows = jnp.where(c0 == ((r0 >> 3) & 7) * SLOC + (r0 >> 6) * CHUNK + (r0 & 7), 1.0, 0.0).astype(BF16)
    mt = mask_ref[...].astype(F32).astype(BF16)
    mask_t[...] = dot(mt, seq_order)
    mask_s[...] = dot_t(seq_rows, mt).astype(BF16)

    @pl.loop(0, SLOC // 4)
    def _(blk):
        for u in range(4):
            pick = jnp.where(iota((SEQ, LANES), 0) == me * SLOC + blk * 4 + u, 1.0, 0.0).astype(BF16)
            keep_row[blk * 4 + u] = dot(mask_ref[...].astype(F32).astype(BF16), pick)

    for load in loads:
        load.wait()
    row_vg[...] = jnp.transpose(w_row_in[:, 2 * CM:])
    col_vg[...] = jnp.transpose(w_col_in[:, 2 * CM:])
    tri_vg[0] = jnp.transpose(w_start_in[:, 2 * CZ:])
    tri_vg[1] = jnp.transpose(w_end_in[:, 2 * CZ:])
    norm[...] = jnp.zeros_like(norm)
    norm[0:RES, 0:RES] = dot_t(mt, mt)
    w_full = w_opm_out[...].reshape(OPM, OPM, CZ)
    for a in range(2):
        for c in range(2):
            blk = w_full[16 * a:16 * a + 16, 16 * c:16 * c + 16, :].reshape(256, CZ)
            w2[16 * c:16 * c + 16, 16 * a:16 * a + 16, :] = dot(perm[...], blk).astype(BF16).reshape(16, 16, CZ)
    w2t[...] = dot_t(eye, w2[...].reshape(OPM * OPM, CZ)).astype(BF16)
    cbig[:, RES:, :] = jnp.zeros((OPM, LANES - RES, SEQ), BF16)
    yrow[:, RES:, :] = jnp.zeros((CHUNK, LANES - RES, CM), BF16)
    rowqk[:, :, RES:, :] = jnp.zeros((4, CHUNK, LANES - RES, LANES), BF16)
    triqk[:, :, RES:, :] = jnp.zeros((2, RLOC, LANES - RES, LANES), BF16)
    z1[RLOC:, :, :] = jnp.zeros((16 - RLOC, RES, CZ), BF16)
    z3[...] = jnp.zeros_like(z3)

    take_bias(rowb_recv, HM, ROWB)

    def m_src(q):
        return lambda d: msend.at[q, pl.ds(d * RLOC, RLOC)]

    def m_dst(q):
        return lambda s: mrecv.at[q, s]

    def local_copy(src, dst, n):
        return pltpu.make_async_copy(src, dst, local_sem.at[n])

    def row_chunk(q):
        s0 = q * CHUNK
        for part in range(CHUNK // 4):
            here = slice(4 * part, 4 * part + 4)
            y = layer_norm(m_ref[s0 + 4 * part:s0 + 4 * part + 4].reshape(4 * RES, CM))
            yrow[here, 0:RES, :] = y.reshape(4, RES, CM)
            qk = dot(y, w_row_in[:, 0:2 * CM]).astype(BF16)
            for t in range(4):
                rowqk[t, here, 0:RES, :] = qk[:, t * LANES:(t + 1) * LANES].reshape(4, RES, LANES)

        def store(u, update):
            m1[s0 + u] = add_residual(m_ref[s0 + u], update[0:RES])
        attend_biased(range(CHUNK), 2, lambda u, t: rowqk[t, u], lambda u, t: rowqk[2 + t, u, 0:RES],
                      lambda u: dot_t(row_vg[...], yrow[u]).astype(BF16), bias,
                      lambda u: keep_row[s0 + u], w_row_out[...], store)

        for j in range(RES // 32):
            blk = m1[CHUNK * q:CHUNK * q + CHUNK, 32 * j:32 * j + 32, :].reshape(256, CM)
            msend[q, 32 * j:32 * j + 32] = dot(perm_out[...], blk).reshape(32, CHUNK, CM).astype(BF16)
        start_all(MF + q, m_src(q), m_dst(q))
        local_copy(m_src(q)(me), m_dst(q)(me), q).start()

    def column_projection(q):
        local_copy(m_src(q)(me), m_dst(q)(me), q).wait()
        wait_recv(MF + q, m_dst(q))

        for blk in range(RLOC // 4):
            x = jnp.concatenate([mrecv[q, :, blk * 4 + u].astype(F32).reshape(CROWS, CM) for u in range(4)], axis=0)
            for u in range(4):
                mcols[q, blk * 4 + u] = x[u * CROWS:(u + 1) * CROWS].astype(BF16)
            y = layer_norm(x)
            ycol[blk * 4:blk * 4 + 4, CROWS * q:CROWS * q + CROWS, :] = y.reshape(4, CROWS, CM)
            qk = dot(y, w_col_in[:, 0:2 * CM]).astype(BF16)
            for t in range(4):
                colqk[t, blk * 4:blk * 4 + 4, CROWS * q:CROWS * q + CROWS, :] = (
                    qk[:, t * LANES:(t + 1) * LANES].reshape(4, CROWS, LANES))

    row_chunk(0)
    row_chunk(1)
    row_chunk(2)
    column_projection(0)
    row_chunk(3)
    column_projection(1)
    column_projection(2)
    column_projection(3)

    def mb_start(j):
        start_all(MB, lambda d: mdone.at[d, j], lambda s: mback.at[s * RLOC + j])

    def relay(j):
        for t, twin in enumerate(twins):
            row = crecv.at[twin * RLOC + j]
            remote(row, row, c_send.at[t], c_recv.at[t, j], twin).wait_recv()
            remote(row, row, c_send.at[3 + t], c_pair.at[t], partner).start()

    @pl.loop(0, RLOC // NRES)
    def _(pair):
        lane = iota((SEQ, LANES), 1)
        offset = jnp.zeros((SEQ, LANES), F32)
        for n, part in enumerate(MASKED_SCORE):
            offset = jnp.where(lane == n, part, offset)
        for u in range(NRES):
            pick = jnp.where(iota((RES, LANES), 0) == me * RLOC + pair * NRES + u, 1.0, 0.0).astype(BF16)
            keep = dot(mask_s[...], pick)
            caug[u] = ((1.0 - keep) * offset).astype(BF16)
            keep = keep.astype(BF16)
            for t in range(2):
                ckeep[u, t] = colqk[2 + t, pair * NRES + u] * keep

        def store(u, update):
            j = pair * NRES + u
            mask_row = mask_t[pl.ds(me * RLOC + j, 1), :]
            x = add_residual(mcols[:, j].reshape(SEQ, CM), update)
            both = dot_t(w_opm_in[...], layer_norm(x)).astype(BF16).astype(F32) * mask_row
            left[j] = both[0:OPM].astype(BF16)
            crecv[me * RLOC + j] = both[OPM:].astype(BF16)
            done = x.astype(F32).reshape(NCHUNK, NDEV, CHUNK, CM).astype(BF16)
            for d in range(NDEV):
                mdone[d, j] = done[:, d]
            row = crecv.at[me * RLOC + j]
            for t, twin in enumerate(twins):
                remote(row, row, c_send.at[t], c_recv.at[t, j], twin).start()
            remote(row, row, c_send.at[6], c_pair.at[3], partner).start()
            if u < NRES - 1:
                mb_start(j)

        attend_column(range(NRES), lambda u, t: colqk[t, pair * NRES + u], lambda u, t: ckeep[u, t], lambda u: caug[u],
                      ones[0:LANES], lambda u: dot_t(col_vg[...], ycol[pair * NRES + u]).astype(BF16), w_col_out[...], store)
        @pl.when(pair >= LAG // NRES)
        def _():
            for u in range(NRES):
                relay(pair * NRES - LAG + u)

        @pl.when(pair < RLOC // NRES - 1)
        def _():
            mb_start(pair * NRES + NRES - 1)

    for j in range(RLOC - LAG, RLOC):
        relay(j)
    keep_mine = local_copy(mdone.at[me], mback.at[pl.ds(me * RLOC, RLOC)], NCHUNK + 4)
    keep_mine.start()

    def c_rows(s):
        return crecv.at[pl.ds(s * RLOC, RLOC)]

    for t, first in enumerate(twins + (me,)):
        rows = c_rows(first + 1 - 2 * core)
        remote(rows, rows, c_send.at[3 + t], c_pair.at[t], partner).wait_recv()
    mb_start(RLOC - 1)
    for c in range(2):
        for j0 in range(0, RES, 16):
            blk = crecv[j0:j0 + 16, 16 * c:16 * c + 16, :].reshape(256, SEQ)
            cbig[16 * c:16 * c + 16, j0:j0 + 16, :] = dot(perm[...], blk).astype(BF16).reshape(16, 16, SEQ)

    @pl.loop(0, OPM // 8)
    def _(blk):
        for c2 in range(4):
            c = blk * 4 + c2
            prod = dot_t(left[...].reshape(RLOC * OPM, SEQ), cbig[pl.ds(2 * c, 2)].reshape(256, SEQ)).astype(BF16)
            for u in range(2):
                outer[:, 2 * c + u] = prod[:, u * LANES:(u + 1) * LANES].reshape(RLOC, OPM, LANES)

    @pl.loop(0, 2)
    def _(half):
        for u in range(RLOC // 2):
            i = half * (RLOC // 2) + u
            update = dot(w2t[...], outer[i].reshape(OPM * OPM, LANES))
            update = update / (1e-3 + norm[pl.ds(me * RLOC + i, 1), :])
            z1[i] = add_residual(z_ref[i], jnp.transpose(update)[0:RES])

    def z_src(buf, group):
        return lambda d: buf.at[group, pl.ds(d * RLOC, RLOC)]

    def z_dst(buf, group):
        return lambda s: buf.at[group, s]

    def triangle(state, result, w_in, which, w_out, recv, stage, late, send, zrecv, moved, zstage, slot):
        ynorm[:, 0:RES, :] = layer_norm(state[0:RLOC].reshape(RLOC * RES, CZ)).reshape(RLOC, RES, CZ)
        send_bias(recv, which, HT, stage)

        for blk in range(RLOC // 4):
            y = ynorm[blk * 4:blk * 4 + 4, 0:RES, :].reshape(4 * RES, CZ)
            qk = dot(y, w_in[:, 0:2 * CZ]).astype(BF16)
            for t in range(2):
                triqk[t, blk * 4:blk * 4 + 4, 0:RES, :] = qk[:, t * LANES:(t + 1) * LANES].reshape(4, RES, LANES)
        take_bias(recv, HT, stage)
        for j in late:
            mb_start(j)

        for group in range(2):
            first = group * ZGROUP

            def store(u, update):
                result[u] = add_residual(state[u], update[0:RES])
            attend_biased(range(first, first + ZGROUP), 1, lambda u, t: triqk[0, u], lambda u, t: triqk[1, u, 0:RES],
                          lambda u: dot_t(tri_vg[which - 1], ynorm[u]).astype(BF16), bias,
                          lambda u: res_keep[...], w_out[...], store)
            for j in range(RES // 32):
                blk = result[first:first + 8, 32 * j:32 * j + 32, :].reshape(256, CZ)
                send[group, 32 * j:32 * j + 32] = dot(perm_out[...], blk).reshape(32, 8, CZ).astype(BF16)
            start_all(zstage + group, z_src(send, group), z_dst(zrecv, group))
            local_copy(z_src(send, group)(me), z_dst(zrecv, group)(me), slot + group).start()

        for group in range(2):
            local_copy(z_src(send, group)(me), z_dst(zrecv, group)(me), slot + group).wait()
            wait_recv(zstage + group, z_dst(zrecv, group))

        for i in range(RLOC):
            rows = zrecv[:, :, i].astype(F32).reshape(LANES, CZ).astype(BF16)
            moved[i] = dot(compz[...], rows).astype(BF16)

    triangle(z1, z1, w_start_in, 1, w_start_out, stb_recv, STB, (), zs, zr, z2, ZF, NCHUNK)
    triangle(z2, z3, w_end_in, 2, w_end_out, enb_recv, ENB, (), zs2, zr2, z_out, ZB, NCHUNK + 2)

    wait_recv(MB, lambda s: mback.at[pl.ds(s * RLOC, RLOC)])
    keep_mine.wait()

    wait_send(ROWB, lambda d: bias_rows(rowb_recv)(me))
    for q in range(NCHUNK):
        wait_send(MF + q, m_src(q))
    wait_send(MB, lambda d: mdone.at[d])
    for t in range(7):
        rows = c_rows(me if t in (0, 1, 2, 6) else twins[t - 3])
        remote(rows, rows, c_send.at[t], c_pair.at[0], partner).wait_send()
    wait_send(STB, lambda d: bias_rows(stb_recv)(me))
    for group in range(2):
        wait_send(ZF + group, z_src(zs, group))
    wait_send(ENB, lambda d: bias_rows(enb_recv)(me))
    for group in range(2):
        wait_send(ZB + group, z_src(zs2, group))


def finish_kernel(m_home, z_new, m_out, z_out, perm_in):
    @pl.when(pl.program_id(0) == 0)
    def _():
        r, c = iota((256, 256), 0), iota((256, 256), 1)
        perm_in[...] = jnp.where(((r >> 5) == (c & 7)) & ((r & 31) == (c >> 3)), 1.0, 0.0).astype(BF16)
        z_out[...] = z_new[...]

    for j in range(RES // 32):
        blk = m_home[32 * j:32 * j + 32, 0].astype(F32).reshape(256, CM).astype(BF16)
        m_out[:, 32 * j:32 * j + 32, :] = dot(perm_in[...], blk).astype(BF16).reshape(CHUNK, 32, CM)


def solution(mesh):
    rows = P(('data', 'chip', 'dap'))
    in_specs = (rows, rows, P('data'), P('data')) + (P(),) * 13
    vmem = pl.BlockSpec(memory_space=pltpu.VMEM)
    hbm = pl.BlockSpec(memory_space=pl.ANY)

    def per_device(m_blk, z_blk, msa_mask, res_mask, w_row_in, w_row_bias, w_row_out, w_col_in, w_col_out,
                   w_opm_in, w_opm_out, w_start_in, w_start_bias, w_start_out, w_end_in, w_end_bias, w_end_out):
        loaded = [m_blk, w_row_in, w_row_out, w_col_in, w_col_out, w_opm_out, w_start_in, w_start_out, w_end_in, w_end_out]
        scratch = [pltpu.VMEM(x.shape, x.dtype) for x in loaded] + [
            pltpu.VMEM((256, 256), BF16),
            pltpu.VMEM((256, 256), BF16),
            pltpu.VMEM((RES, LANES), BF16),
            pltpu.VMEM((RES, LANES), BF16),
            pltpu.VMEM((LANES, LANES), BF16),
            pltpu.VMEM((SLOC, RES, LANES), F32),
            pltpu.VMEM((RES, SEQ), F32),
            pltpu.VMEM((SEQ, RES), BF16),
            pltpu.VMEM((LANES, LANES), F32),
            pltpu.VMEM((RES, LANES), F32),
            pltpu.VMEM((3, 8, CZ), F32),
            pltpu.VMEM((16, 8, LANES), F32),
            pltpu.VMEM((HM, RES, LANES), F32),
            pltpu.VMEM((NDEV, HM, 16, LANES), BF16),
            pltpu.VMEM((NDEV, HT, 16, LANES), BF16),
            pltpu.VMEM((NDEV, HT, 16, LANES), BF16),
            pltpu.VMEM((2 * CM, CM), BF16),
            pltpu.VMEM((2 * CM, CM), BF16),
            pltpu.VMEM((2, 2 * CZ, CZ), BF16),
            pltpu.VMEM((CHUNK, LANES, CM), BF16),
            pltpu.VMEM((4, CHUNK, LANES, LANES), BF16),
            pltpu.VMEM((2, RLOC, LANES, LANES), BF16),
            pltpu.VMEM((SLOC, RES, CM), BF16),
            pltpu.VMEM((NCHUNK, RES, CHUNK, CM), BF16),
            pltpu.VMEM((NCHUNK, NDEV, RLOC, CHUNK, CM), BF16),
            pltpu.VMEM((NCHUNK, RLOC, CROWS, CM), BF16),
            pltpu.VMEM((NDEV, RLOC, NCHUNK, CHUNK, CM), BF16),
            pltpu.VMEM((RLOC, SEQ, CM), BF16),
            pltpu.VMEM((4, RLOC, SEQ, LANES), BF16),
            pltpu.VMEM((NRES, SEQ, LANES), BF16),
            pltpu.VMEM((NRES, 2, SEQ, LANES), BF16),
            pltpu.VMEM((SEQ, LANES), BF16),
            pltpu.VMEM((RLOC, OPM, SEQ), BF16),
            pltpu.VMEM((RES, OPM, SEQ), BF16),
            pltpu.VMEM((OPM, LANES, SEQ), BF16),
            pltpu.VMEM((RLOC, OPM, OPM, LANES), BF16),
            pltpu.VMEM((OPM, OPM, CZ), BF16),
            pltpu.VMEM((CZ, OPM * OPM), BF16),
            pltpu.VMEM((RLOC, LANES, CZ), BF16),
            pltpu.VMEM((16, RES, CZ), BF16),
            pltpu.VMEM((2, RES, 8, CZ), BF16),
            pltpu.VMEM((2, NDEV, RLOC, 8, CZ), BF16),
            pltpu.VMEM((RLOC, RES, CZ), BF16),
            pltpu.VMEM((16, RES, CZ), BF16),
            pltpu.VMEM((2, RES, 8, CZ), BF16),
            pltpu.VMEM((2, NDEV, RLOC, 8, CZ), BF16),
            pltpu.SemaphoreType.DMA((NSTAGE, NDEV)),
            pltpu.SemaphoreType.DMA((NSTAGE, NDEV)),
            pltpu.SemaphoreType.DMA((NCHUNK + 5,)),
            pltpu.SemaphoreType.DMA((10,)),
            pltpu.SemaphoreType.DMA((7,)),
            pltpu.SemaphoreType.DMA((3, RLOC)),
            pltpu.SemaphoreType.DMA((4,)),
        ]
        m_home, z_new = pl.pallas_call(
            block_kernel,
            name='evoformer_block',
            out_shape=(jax.ShapeDtypeStruct((RES, NCHUNK, CHUNK, CM), BF16), jax.ShapeDtypeStruct(z_blk.shape, BF16)),
            in_specs=[hbm, vmem, vmem, vmem, hbm, vmem, hbm, hbm, hbm, vmem, hbm, hbm, vmem, hbm, hbm, vmem, hbm],
            out_specs=(hbm, vmem),
            scratch_shapes=scratch,
            compiler_params=pltpu.CompilerParams(collective_id=0, has_side_effects=True,
                                                 vmem_limit_bytes=56 * 1024 * 1024),
        )(m_blk, z_blk, msa_mask.T, res_mask.reshape(1, RES), w_row_in, w_row_bias.T, w_row_out, w_col_in, w_col_out,
          w_opm_in.T, w_opm_out, w_start_in, w_start_bias.T, w_start_out, w_end_in, w_end_bias.T, w_end_out)
        whole = pl.BlockSpec((RLOC, RES, CZ), lambda q: (0, 0, 0))
        return pl.pallas_call(
            finish_kernel,
            name='finish',
            grid=(NCHUNK,),
            out_shape=(jax.ShapeDtypeStruct(m_blk.shape, BF16), jax.ShapeDtypeStruct(z_blk.shape, BF16)),
            in_specs=[pl.BlockSpec((RES, 1, CHUNK, CM), lambda q: (0, q, 0, 0)), whole],
            out_specs=(pl.BlockSpec((CHUNK, RES, CM), lambda q: (q, 0, 0)), whole),
            scratch_shapes=[pltpu.VMEM((256, 256), BF16)],
            compiler_params=pltpu.CompilerParams(dimension_semantics=('arbitrary',)),
        )(m_home, z_new)

    return jax.shard_map(per_device, mesh=mesh, in_specs=in_specs, out_specs=(rows, rows), check_vma=False)
```
